128 devices in a mesh: dp: 32 (over x, y, core), group: 4 (over z).
Axes of the slice: x: 4, y: 4, z: 4, core: 2. Of those that a mesh axis runs over, the one named last changes fastest.
Arguments:
- images: bfloat16 [16384, 512], P(('dp', 'group')), may hold values from -1 to 1
- texts: bfloat16 [16384, 512], P(('dp', 'group')), may hold values from -1 to 1
- log_scale: float32 [], replicated, may hold values from 2 to 2.7
Outputs:
- grad_images: bfloat16 [16384, 512], P(('dp', 'group'))
- grad_texts: bfloat16 [16384, 512], P(('dp', 'group'))
- loss: float32 [], replicated
- grad_scale: float32 [], replicated
The draws below stay inside these ranges and needn't reach their ends.
All inputs are finite; a program needn't handle non-finite values.
Results may differ from the reference program's by a relative error of at most 0.0013.
The reference program's roundings to bfloat16 on the way (of `weights_low`) count: a program that leaves them out, or rounds other values in their place, can miss the bound.
Values may be sent and summed in bfloat16 or wider, within the bound.
No kernel may reach another device: no remote copies, remote signals or barrier semaphores. Data moves between devices by JAX's collectives and lax.ppermute only.
A program may use at most 128 MiB of HBM per device.

```python
import jax
import jax.numpy as jnp
from jax import lax

D = 512
B_DEV = 128
N = 16384


def draw_pair(key):
    spread_dims = jnp.exp(jax.random.uniform(jax.random.fold_in(key, 17), (1, D), jnp.float32, -0.693, 0.693))
    spread_dims = spread_dims / jnp.sqrt(jnp.mean(spread_dims * spread_dims))
    base = jnp.clip(0.05 * spread_dims * jax.random.normal(jax.random.fold_in(key, 11), (N, D), jnp.float32), -0.5, 0.5)
    noise = jnp.clip(0.05 * spread_dims * jax.random.normal(jax.random.fold_in(key, 12), (N, D), jnp.float32), -0.5, 0.5)
    paired = 0.3 * base + 0.95 * noise
    common = 0.05 * jax.random.rademacher(jax.random.fold_in(key, 16), (1, D), jnp.float32)
    image_share = jax.random.uniform(jax.random.fold_in(key, 18), (N, 1), jnp.float32, 0.1, 0.4)
    text_share = jax.random.uniform(jax.random.fold_in(key, 19), (N, 1), jnp.float32, 0.1, 0.4)
    base = base + image_share * common
    paired = paired + text_share * common
    return (jnp.clip(base, -1.0, 1.0), jnp.clip(paired, -1.0, 1.0))


def draw_images(key, part):
    return draw_pair(key)[0].astype(jnp.bfloat16)


def draw_texts(key, part):
    return draw_pair(key)[1].astype(jnp.bfloat16)


def setup_inputs(seed: int = 0) -> dict:
    streams_of = jax.random.split(jax.random.key(seed), 4)
    images = draw_images(jax.random.fold_in(streams_of[3], 71), 0)
    texts = draw_texts(jax.random.fold_in(streams_of[3], 71), 0)
    log_scale = jnp.clip(jax.random.uniform(streams_of[2], (), jnp.float32, 2.0, 2.7), 2.0, 2.7)
    return dict(images=images, texts=texts, log_scale=log_scale)


def reference(images, texts, log_scale):
    pair_total = images.shape[0]
    block_rows = B_DEV
    block_count = pair_total // block_rows
    logit_scale = jnp.exp(log_scale)
    columns = jnp.arange(pair_total).astype(jnp.int32)

    def logits_at(block_index):
        first_row = (block_index * block_rows).astype(jnp.int32)
        image_rows = lax.dynamic_slice_in_dim(images, first_row, block_rows, 0)
        logits = logit_scale * jnp.dot(image_rows, texts.T, preferred_element_type=jnp.float32)
        return image_rows, first_row, logits

    def first_pass(carry, block_index):
        col_top, col_sum = carry
        image_rows, first_row, logits = logits_at(block_index)
        row_top = jnp.max(logits, axis=1)
        row_lse = row_top + jnp.log(jnp.sum(jnp.exp(logits - row_top[:, None]), axis=1))
        paired = jnp.diagonal(lax.dynamic_slice_in_dim(logits, first_row, block_rows, 1))
        new_top = jnp.maximum(col_top, jnp.max(logits, axis=0))
        col_sum = col_sum * jnp.exp(col_top - new_top) + jnp.sum(jnp.exp(logits - new_top[None, :]), axis=0)
        return (new_top, col_sum), (row_lse, paired)

    start_carry = (jnp.full((pair_total,), -1e30, jnp.float32), jnp.zeros((pair_total,), jnp.float32))
    indices = jnp.arange(block_count).astype(jnp.int32)
    (col_top, col_sum), (row_lse, paired) = lax.scan(first_pass, start_carry, indices)
    col_lse = col_top + jnp.log(col_sum)

    def second_pass(carry, inputs):
        text_sum, scale_sum = carry
        block_index, block_lse = inputs
        image_rows, first_row, logits = logits_at(block_index)
        own_pairs = (columns[None, :] == (first_row + jnp.arange(block_rows).astype(jnp.int32))[:, None]).astype(jnp.float32)
        grad_block = 0.5 * (jnp.exp(logits - block_lse[:, None]) + jnp.exp(logits - col_lse[None, :])) - own_pairs
        scale_sum = scale_sum + jnp.sum(grad_block * logits)
        weights_low = grad_block.astype(jnp.bfloat16)
        image_grad = logit_scale * jnp.dot(weights_low, texts, preferred_element_type=jnp.float32)
        text_sum = text_sum + jnp.dot(weights_low.T, image_rows, preferred_element_type=jnp.float32)
        return (text_sum, scale_sum), image_grad.astype(jnp.bfloat16)

    start_two = (jnp.zeros(texts.shape, jnp.float32), jnp.zeros((), jnp.float32))
    (text_sum, scale_sum), image_blocks = lax.scan(second_pass, start_two, (indices, row_lse))
    grad_images = image_blocks.reshape(pair_total, images.shape[1])
    grad_texts = (logit_scale * text_sum).astype(jnp.bfloat16)
    loss = (jnp.sum(row_lse) + jnp.sum(col_lse) - 2.0 * jnp.sum(paired)) / (2.0 * pair_total)
    grad_scale = scale_sum / pair_total
    return grad_images, grad_texts, loss, grad_scale
```

```python
import functools

import jax
import jax.numpy as jnp
from jax import lax
from jax.experimental import pallas as pl
from jax.experimental.pallas import tpu as pltpu
from jax.sharding import Mesh
from jax.sharding import PartitionSpec as P

ALL = ("x", "y", "c", "z")
F32, BF16, F16 = jnp.float32, jnp.bfloat16, jnp.float16
LOG2E = 1.4426950408889634
LN2 = 0.6931471805599453
OFFSETS = (1, 3, 2)
ROWS = 128
DOWN = 2.0**-11
STEP = 2.0**8
TINY = 6.2e-5


def turn(value, shift, first):
    pairs = []
    for y in range(4):
        for c in range(2):
            for z in range(4):
                if (c == 0) == first:
                    to = ((y + shift) % 4, c, z)
                else:
                    to = (y, c, (z + shift) % 4)
                pairs.append(((y * 2 + c) * 4 + z, (to[0] * 2 + to[1]) * 4 + to[2]))
    return lax.ppermute(value, ("y", "c", "z"), pairs)


def along_x(value, shift):
    return lax.ppermute(value, "x", [(i, (i + shift) % 4) for i in range(4)])


def other_core(value):
    return lax.ppermute(value, "c", [(0, 1), (1, 0)])


def everyone(value, move):
    got = {0: value}
    for d in OFFSETS:
        got[d] = move(value, d)
    return [got[d] for d in range(4)]


NT = (((1,), (1,)), ((), ()))
TN = (((0,), (0,)), ((), ()))


def call(kernel, outs, *args, smem=(), vmem=16, name=None):
    return pl.pallas_call(
        kernel,
        out_shape=outs,
        in_specs=[
            pl.BlockSpec(memory_space=pltpu.SMEM if i in smem else pltpu.VMEM) for i in range(len(args))
        ],
        out_specs=jax.tree.map(lambda _: pl.BlockSpec(memory_space=pltpu.VMEM), outs),
        compiler_params=pltpu.CompilerParams(vmem_limit_bytes=vmem << 20),
        name=name,
    )(*args)


def out(shape, dtype=F32):
    return pltpu.VMEM(shape, dtype)


def to_lanes(column):
    return [column[128 * k : 128 * (k + 1), :].T[0:1, :] for k in range(4)]


def logits_kernel(s_ref, im_ref, t0_ref, t1_ref, l_ref, rows_ref, cols_ref, lse_scr, mean_scr):
    s2 = s_ref[0, 0]
    for h, t_ref in enumerate((t0_ref, t1_ref)):
        l_ref[:, 512 * h : 512 * (h + 1)] = s2 * lax.dot_general(
            im_ref[...], t_ref[...], NT, preferred_element_type=F32
        )
    col_top = jnp.max(l_ref[...], axis=0, keepdims=True)

    def step(i, carry):
        col_sum, col_mean = carry
        here = pl.ds(pl.multiple_of(i * 32, 32), 32)
        part = l_ref[here, :]
        top = jnp.max(part, axis=1, keepdims=True)
        e = jnp.exp2(part - top)
        total = jnp.sum(e, axis=1, keepdims=True)
        mean = jnp.sum(e * part, axis=1, keepdims=True) / total
        lse_scr[here, :] = jnp.broadcast_to(top + jnp.log2(total), (32, 128))
        mean_scr[here, :] = jnp.broadcast_to(mean, (32, 128))
        e = jnp.exp2(part - col_top)
        f = e * part
        for k in range(4):
            col_sum = col_sum + e[8 * k : 8 * (k + 1), :]
            col_mean = col_mean + f[8 * k : 8 * (k + 1), :]
        return col_sum, col_mean

    zero = jnp.zeros((8, 1024), F32)
    col_sum, col_mean = lax.fori_loop(0, 16, step, (zero, zero))
    cols_ref[0:1, :] = col_top
    cols_ref[1:2, :] = jnp.sum(col_sum, axis=0, keepdims=True)
    cols_ref[2:3, :] = jnp.sum(col_mean, axis=0, keepdims=True)
    for k, (a, b) in enumerate(zip(to_lanes(lse_scr[...]), to_lanes(mean_scr[...]))):
        rows_ref[k : k + 1, :] = a
        rows_ref[4 + k : 5 + k, :] = b


def logits_of(s2, im, t0, t1):
    return pl.pallas_call(
        logits_kernel,
        out_shape=(out((512, 1024)), out((8, 128)), out((3, 1024))),
        in_specs=[pl.BlockSpec(memory_space=pltpu.SMEM)] + [pl.BlockSpec(memory_space=pltpu.VMEM)] * 3,
        out_specs=(pl.BlockSpec(memory_space=pltpu.VMEM),) * 3,
        scratch_shapes=[pltpu.VMEM((512, 128), F32)] * 2,
        compiler_params=pltpu.CompilerParams(vmem_limit_bytes=16 << 20),
        name="logits",
    )(s2, im, t0, t1)


def merge(parts):
    top = functools.reduce(jnp.maximum, [p[0] for p in parts])
    es = [jnp.exp2(p[0] - top) for p in parts]
    total = sum(es)
    mean = sum(e * p[1] for e, p in zip(es, parts)) / total
    return top + jnp.log2(total), mean


def whole(value):
    return jnp.broadcast_to(value, (1, 128))


def peak(ref):
    return jnp.max(jnp.max(jnp.abs(ref[...].astype(F32)), axis=0, keepdims=True), axis=1, keepdims=True)


def start_kernel(l0, r0, r1, r2, r3, c0, c1, c2, c3, i0, i1, i2, i3, t0, t1, row_ref, col_ref):
    for k, r in enumerate((r0, r1, r2, r3)):
        row_ref[4 * k : 4 * k + 4, :] = r[0:4, :]
        row_ref[16 + 4 * k : 20 + 4 * k, :] = r[4:8, :]
    block = l0[0:128, 0:128]
    eye = lax.broadcasted_iota(jnp.int32, (128, 128), 0) == lax.broadcasted_iota(jnp.int32, (128, 128), 1)
    diagonal = jnp.sum(jnp.where(eye, block, 0.0), axis=0, keepdims=True)
    row_ref[32:33, :] = diagonal
    row_ref[33:34, :] = whole(jnp.maximum(peak(t0), peak(t1)))
    row_ref[34:40, :] = jnp.zeros((6, 128), F32)
    cs = (c0, c1, c2, c3)
    top = functools.reduce(jnp.maximum, [c[0:1, :] for c in cs])
    es = [jnp.exp2(c[0:1, :] - top) for c in cs]
    total = sum(e * c[1:2, :] for e, c in zip(es, cs))
    mean = sum(e * c[2:3, :] for e, c in zip(es, cs)) / total
    lse = top + jnp.log2(total)
    for k in range(8):
        col_ref[k : k + 1, :] = lse[:, 128 * k : 128 * (k + 1)]
        col_ref[8 + k : 9 + k, :] = mean[:, 128 * k : 128 * (k + 1)]
    col_ref[16:17, :] = whole(functools.reduce(jnp.maximum, [peak(i) for i in (i0, i1, i2, i3)]))
    col_ref[17:24, :] = jnp.zeros((7, 128), F32)


def rolled(v, d, group):
    if d == 0:
        return v
    n = v.shape[0]
    size = n // group
    quarter = size // 4
    pieces = []
    for g in range(group):
        at = g * size
        pieces += [v[at + size - d * quarter : at + size, :], v[at : at + size - d * quarter, :]]
    return jnp.concatenate(pieces, axis=0)


def middle_kernel(a0, a1, a2, a3, b0, b1, b2, b3, row_ref, col_ref):
    rs = (a0, a1, a2, a3)
    lse, mean = merge([(rolled(r[0:16, :], d, 4), rolled(r[16:32, :], d, 4)) for d, r in enumerate(rs)])
    row_ref[0:16, :] = lse
    row_ref[16:32, :] = mean
    row_ref[32:33, :] = sum(r[32:33, :] for r in rs)
    row_ref[33:34, :] = functools.reduce(jnp.maximum, [r[33:34, :] for r in rs])
    row_ref[34:40, :] = jnp.zeros((6, 128), F32)
    cs = (b0, b1, b2, b3)
    lse, mean = merge([(rolled(c[0:8, :], d, 2), rolled(c[8:16, :], d, 2)) for d, c in enumerate(cs)])
    col_ref[0:8, :] = lse
    col_ref[8:16, :] = mean
    col_ref[16:17, :] = functools.reduce(jnp.maximum, [c[16:17, :] for c in cs])
    col_ref[17:24, :] = jnp.zeros((7, 128), F32)


def pieces_of(value):
    left, pieces = value * DOWN, []
    for _ in range(4):
        head = left.astype(BF16).astype(F32)
        head = jnp.where(jnp.abs(head) < TINY, 0.0, head)
        pieces.append(head)
        left = (left - head) * STEP
    return pieces


def value_of(pieces):
    total = pieces[3]
    for p in (pieces[2], pieces[1], pieces[0]):
        total = p + total * (1.0 / STEP)
    return total * (1.0 / DOWN)


def tail_rows(first, second):
    which = lax.broadcasted_iota(jnp.int32, (16, 128), 0) < 8
    value = jnp.where(which, jnp.broadcast_to(first, (16, 128)), jnp.broadcast_to(second, (16, 128)))
    return pieces_of(value)


def total_of(v):
    return jnp.sum(jnp.sum(v, axis=0, keepdims=True), axis=1, keepdims=True)


def end_kernel(a0, a1, a2, a3, b0, b1, row_ref, col_ref, image_tail, text_tail, scale_ref):
    rs = (a0, a1, a2, a3)
    lse, mean = merge([(rolled(r[0:16, :], d, 1), rolled(r[16:32, :], d, 1)) for d, r in enumerate(rs)])
    row_ref[...] = lse + 1.0
    diagonal = total_of(sum(r[32:33, :] for r in rs)) * LN2
    text_peak = functools.reduce(jnp.maximum, [r[33:34, :] for r in rs])
    for k, v in enumerate(tail_rows(total_of(lse) * LN2 - 2.0 * diagonal, 0.5 * LN2 * total_of(mean) - diagonal)):
        text_tail[:, 128 * k : 128 * (k + 1)] = v
    swapped = jnp.concatenate([b1[4:8, :], b1[0:4, :]], axis=0), jnp.concatenate([b1[12:16, :], b1[8:12, :]], axis=0)
    lse, mean = merge([(b0[0:8, :], b0[8:16, :]), swapped])
    for k in range(8):
        col_ref[:, 128 * k : 128 * (k + 1)] = lse[k : k + 1, :] + 1.0
    image_peak = jnp.maximum(b0[16:17, :], b1[16:17, :])
    for k, v in enumerate(tail_rows(total_of(lse) * LN2, 0.5 * LN2 * total_of(mean))):
        image_tail[:, 128 * k : 128 * (k + 1)] = v
    scale_ref[0:1, :] = 4.0 / jnp.maximum(text_peak, 1e-30)
    scale_ref[1:2, :] = 4.0 / jnp.maximum(image_peak, 1e-30)


def image_kernel(which, l_ref, row_ref, col_ref, scale_ref, t0_ref, t1_ref, w_ref, g_ref):
    for j in range(4):
        at = slice(128 * j, 128 * (j + 1))
        row = row_ref[4 * which + j : 4 * which + j + 1, :]
        row = jnp.broadcast_to(row, (128, 128)).T
        for k in range(8):
            to = slice(128 * k, 128 * (k + 1))
            part = l_ref[at, to]
            w = jnp.exp2(part - row) + jnp.exp2(part - col_ref[:, to])
            if which == 0 and j == 0 and k == 0:
                eye = lax.broadcasted_iota(jnp.int32, (128, 128), 0) == lax.broadcasted_iota(
                    jnp.int32, (128, 128), 1
                )
                w = w - jnp.where(eye, 1.0, 0.0)
            w_ref[at, to] = w.astype(BF16)
    g = jnp.dot(w_ref[:, 0:512], t0_ref[...], preferred_element_type=F32)
    g = g + jnp.dot(w_ref[:, 512:1024], t1_ref[...], preferred_element_type=F32)
    g_ref[...] = g * scale_ref[0:1, 0:1]


def text_kernel(w0, w1, w2, w3, i0, i1, i2, i3, scale_ref, g0_ref, g1_ref):
    for h, g_ref in enumerate((g0_ref, g1_ref)):
        at = slice(512 * h, 512 * (h + 1))
        g = None
        for w, i in zip((w0, w1, w2, w3), (i0, i1, i2, i3)):
            part = lax.dot_general(w[:, at], i[...], TN, preferred_element_type=F32)
            g = part if g is None else g + part
        g_ref[...] = g * scale_ref[1:2, 0:1]


def read_tail(rows):
    parts = [rows[:, 128 * k : 128 * (k + 1)].astype(F32) for k in range(4)]
    value = value_of(parts)
    return value[0, 0], value[8, 0]


def tail_of(values):
    return jnp.concatenate(tail_rows(*[jnp.reshape(v, (1, 1)) for v in values]), axis=1)


def body(images, texts, log_scale):
    pair_total = ROWS * 128
    scale = jnp.exp(log_scale)
    s2 = jnp.reshape(scale * LOG2E, (1, 1))
    line = jnp.concatenate(everyone(images, lambda v, d: turn(v, d, True)), axis=0)
    chunks = everyone(line, lambda v, d: turn(v, d, False))
    t0 = jnp.concatenate(everyone(texts, along_x), axis=0)
    t1 = other_core(t0)
    parts = [logits_of(s2, im, t0, t1) for im in chunks]
    ls = [p[0] for p in parts]
    rows, cols = call(
        start_kernel,
        (out((40, 128)), out((24, 128))),
        ls[0], *[p[1] for p in parts], *[p[2] for p in parts], *chunks, t0, t1,
        name="start",
    )
    rows, cols = call(
        middle_kernel,
        (out((40, 128)), out((24, 128))),
        *everyone(rows, lambda v, d: turn(v, d, True)), *everyone(cols, along_x),
        name="middle",
    )
    row_lse, col_lse, image_tail, text_tail, unit = call(
        end_kernel,
        (out((16, 128)), out((1, 1024)), out((16, 512)), out((16, 512)), out((2, 128))),
        *everyone(rows, lambda v, d: turn(v, d, False)), cols, other_core(cols),
        name="end",
    )
    ws, gs = {}, {}
    for k in (2, 1, 3, 0):
        ws[k], gs[k] = call(
            functools.partial(image_kernel, k),
            (out((512, 1024), BF16), out((512, 512))),
            ls[k], row_lse, col_lse, unit, t0, t1,
            name="image_grad",
        )
    sent = {
        k: turn(jnp.concatenate([gs[k], image_tail], axis=0).astype(F16), (4 - k) % 4, False) for k in (2, 1, 3)
    }
    gt0, gt1 = call(
        text_kernel,
        (out((512, 512)), out((512, 512))),
        *[ws[k] for k in range(4)], *chunks, unit,
        name="text_grad",
    )
    a = read_tail(text_tail)
    swap = other_core(jnp.concatenate([gt1, text_tail], axis=0).astype(F16))
    gt = gt0 + swap[0:512].astype(F32)
    b = read_tail(swap[512:])
    a = (a[0] + b[0], a[1] + b[1])
    tail = tail_of(a)
    moved = [
        along_x(jnp.concatenate([gt[128 * k : 128 * (k + 1)], tail], axis=0).astype(F16), (4 - k) % 4)
        for k in (2, 1, 3)
    ]
    grad_texts = gt[0:128] + sum(m[0:128].astype(F32) for m in moved)
    tails = [read_tail(m[128:]) for m in moved]
    a = tuple(a[i] + sum(t[i] for t in tails) for i in range(2))
    gi = gs[0] + sum(m[0:512].astype(F32) for m in sent.values())
    b = read_tail(image_tail)
    tails = [read_tail(m[512:]) for m in sent.values()]
    b = tuple(b[i] + sum(t[i] for t in tails) for i in range(2))
    tail = tail_of(b)
    moved = [
        turn(jnp.concatenate([gi[128 * k : 128 * (k + 1)], tail], axis=0).astype(F16), (4 - k) % 4, True)
        for k in (2, 1, 3)
    ]
    grad_images = gi[0:128] + sum(m[0:128].astype(F32) for m in moved)
    tails = [read_tail(m[128:]) for m in moved]
    b = tuple(b[i] + sum(t[i] for t in tails) for i in range(2))
    grad_images = (grad_images * (scale / unit[0, 0])).astype(BF16)
    grad_texts = (grad_texts * (scale / unit[1, 0])).astype(BF16)
    return (
        grad_images,
        grad_texts,
        (a[0] + b[0]) / (2.0 * pair_total),
        (a[1] + b[1]) / pair_total,
    )


def solution(mesh):
    split = Mesh(mesh.devices.reshape(4, 4, 2, mesh.shape["group"]), ALL)
    placed = (P(ALL, None), P(ALL, None), P())
    return jax.shard_map(
        body,
        mesh=split,
        in_specs=placed,
        out_specs=(P(ALL, None), P(ALL, None), P(), P()),
        check_vma=False,
    )
```

```python
import functools

import jax
import jax.numpy as jnp
from jax import lax
from jax.experimental import pallas as pl
from jax.experimental.pallas import tpu as pltpu
from jax.sharding import Mesh
from jax.sharding import PartitionSpec as P

ALL = ("x", "y", "c", "z")
F32, BF16, F16 = jnp.float32, jnp.bfloat16, jnp.float16
LOG2E = 1.4426950408889634
LN2 = 0.6931471805599453
OFFSETS = (1, 3, 2)
ROWS = 128
DOWN = 2.0**-11
STEP = 2.0**8
TINY = 6.2e-5


def turn(value, shift, first):
    pairs = []
    for y in range(4):
        for c in range(2):
            for z in range(4):
                if (c == 0) == first:
                    to = ((y + shift) % 4, c, z)
                else:
                    to = (y, c, (z + shift) % 4)
                pairs.append(((y * 2 + c) * 4 + z, (to[0] * 2 + to[1]) * 4 + to[2]))
    return lax.ppermute(value, ("y", "c", "z"), pairs)


def along_x(value, shift):
    return lax.ppermute(value, "x", [(i, (i + shift) % 4) for i in range(4)])


def other_core(value):
    return lax.ppermute(value, "c", [(0, 1), (1, 0)])


def everyone(value, move):
    got = {0: value}
    for d in OFFSETS:
        got[d] = move(value, d)
    return [got[d] for d in range(4)]


NT = (((1,), (1,)), ((), ()))
TN = (((0,), (0,)), ((), ()))


def call(kernel, outs, *args, smem=(), scratch=(), name=None):
    return pl.pallas_call(
        kernel,
        out_shape=outs,
        in_specs=[
            pl.BlockSpec(memory_space=pltpu.SMEM if i in smem else pltpu.VMEM) for i in range(len(args))
        ],
        out_specs=jax.tree.map(lambda _: pl.BlockSpec(memory_space=pltpu.VMEM), outs),
        scratch_shapes=scratch,
        compiler_params=pltpu.CompilerParams(vmem_limit_bytes=16 << 20),
        name=name,
    )(*args)


def out(shape, dtype=F32):
    return pltpu.VMEM(shape, dtype)


def join_kernel(a0, a1, a2, a3, o_ref):
    for k, a in enumerate((a0, a1, a2, a3)):
        o_ref[128 * k : 128 * (k + 1), :] = a[...]


def joined(values, name):
    return call(join_kernel, out((512, 512), BF16), *values, name=name)


def peak(ref):
    tall = jnp.max(jnp.abs(ref[...].astype(F32)), axis=0, keepdims=True)
    return jnp.broadcast_to(jnp.max(tall, axis=1, keepdims=True), (1, 128))


def logits_kernel(first, s_ref, im_ref, t0_ref, t1_ref, l_ref, rows_ref, cols_ref, top_scr, sum_scr, mean_scr):
    s2 = s_ref[0, 0]
    for h, t_ref in enumerate((t0_ref, t1_ref)):
        l_ref[:, 512 * h : 512 * (h + 1)] = s2 * lax.dot_general(
            im_ref[...], t_ref[...], NT, preferred_element_type=F32
        )

    def tops(i, col_tops):
        here = pl.ds(pl.multiple_of(i * 64, 64), 64)
        row_top, new = None, []
        for k in range(8):
            part = l_ref[here, 128 * k : 128 * (k + 1)]
            row_top = part if row_top is None else jnp.maximum(row_top, part)
            new.append(jnp.maximum(col_tops[k], jnp.max(part.reshape(8, 8, 128), axis=0)))
        top_scr[here, :] = row_top
        return tuple(new)

    col_tops = lax.fori_loop(0, 8, tops, tuple(l_ref[0:8, 128 * k : 128 * (k + 1)] for k in range(8)))

    def sums(i, carry):
        here = pl.ds(pl.multiple_of(i * 64, 64), 64)
        row_top = top_scr[here, :]
        row_sum = row_mean = jnp.zeros((64, 128), F32)
        new = []
        for k in range(8):
            part = l_ref[here, 128 * k : 128 * (k + 1)]
            e = jnp.exp2(part - row_top)
            row_sum = row_sum + e
            row_mean = row_mean + e * part
            part = part.reshape(8, 8, 128)
            e = jnp.exp2(part - col_tops[k][None])
            new.append((carry[k][0] + jnp.sum(e, axis=0), carry[k][1] + jnp.sum(e * part, axis=0)))
        sum_scr[here, :] = row_sum
        mean_scr[here, :] = row_mean
        return tuple(new)

    zero = jnp.zeros((8, 128), F32)
    col_sums = lax.fori_loop(0, 8, sums, ((zero, zero),) * 8)
    for k in range(8):
        at = slice(128 * k, 128 * (k + 1))
        top = jnp.max(col_tops[k], axis=0, keepdims=True)
        e = jnp.exp2(col_tops[k] - top)
        cols_ref[0:1, at] = top
        cols_ref[1:2, at] = jnp.sum(e * col_sums[k][0], axis=0, keepdims=True)
        cols_ref[2:3, at] = jnp.sum(e * col_sums[k][1], axis=0, keepdims=True)
    for j in range(4):
        at = slice(128 * j, 128 * (j + 1))
        tops_here = top_scr[at, :].T
        top = jnp.max(tops_here, axis=0, keepdims=True)
        e = jnp.exp2(tops_here - top)
        total = jnp.sum(e * sum_scr[at, :].T, axis=0, keepdims=True)
        rows_ref[j : j + 1, :] = top + jnp.log2(total)
        rows_ref[4 + j : 5 + j, :] = jnp.sum(e * mean_scr[at, :].T, axis=0, keepdims=True) / total
    rows_ref[8:9, :] = peak(im_ref)
    if first:
        rows_ref[9:10, :] = jnp.maximum(peak(t0_ref), peak(t1_ref))
        block = l_ref[0:128, 0:128]
        rows_ref[10:11, :] = jnp.sum(jnp.where(eye(), block, 0.0), axis=0, keepdims=True)


def eye():
    shape = (128, 128)
    return lax.broadcasted_iota(jnp.int32, shape, 0) == lax.broadcasted_iota(jnp.int32, shape, 1)


def logits_of(k, s2, im, t0, t1):
    return call(
        functools.partial(logits_kernel, k == 0),
        (out((512, 1024)), out((16, 128)), out((8, 1024))),
        s2, im, t0, t1,
        smem=(0,),
        scratch=[pltpu.VMEM((512, 128), F32)] * 3,
        name="logits",
    )


def merge(parts):
    top = functools.reduce(jnp.maximum, [p[0] for p in parts])
    es = [jnp.exp2(p[0] - top) for p in parts]
    total = sum(es)
    mean = sum(e * p[1] for e, p in zip(es, parts)) / total
    return top + jnp.log2(total), mean


def greatest(values):
    return functools.reduce(jnp.maximum, values)


def start_kernel(r0, r1, r2, r3, c0, c1, c2, c3, row_ref, col_ref):
    rs, cs = (r0, r1, r2, r3), (c0, c1, c2, c3)
    for k, r in enumerate(rs):
        row_ref[4 * k : 4 * k + 4, :] = r[0:4, :]
        row_ref[16 + 4 * k : 20 + 4 * k, :] = r[4:8, :]
    row_ref[32:33, :] = r0[10:11, :]
    row_ref[33:34, :] = r0[9:10, :]
    row_ref[34:40, :] = jnp.zeros((6, 128), F32)
    top = greatest([c[0:1, :] for c in cs])
    es = [jnp.exp2(c[0:1, :] - top) for c in cs]
    total = sum(e * c[1:2, :] for e, c in zip(es, cs))
    mean = sum(e * c[2:3, :] for e, c in zip(es, cs)) / total
    lse = top + jnp.log2(total)
    for k in range(8):
        col_ref[k : k + 1, :] = lse[:, 128 * k : 128 * (k + 1)]
        col_ref[8 + k : 9 + k, :] = mean[:, 128 * k : 128 * (k + 1)]
    col_ref[16:17, :] = greatest([r[8:9, :] for r in rs])
    col_ref[17:24, :] = jnp.zeros((7, 128), F32)


def rolled(v, d, group):
    if d == 0:
        return v
    n = v.shape[0]
    size = n // group
    quarter = size // 4
    pieces = []
    for g in range(group):
        at = g * size
        pieces += [v[at + size - d * quarter : at + size, :], v[at : at + size - d * quarter, :]]
    return jnp.concatenate(pieces, axis=0)


def middle_kernel(a0, a1, a2, a3, b0, b1, b2, b3, row_ref, col_ref):
    rs = (a0, a1, a2, a3)
    lse, mean = merge([(rolled(r[0:16, :], d, 4), rolled(r[16:32, :], d, 4)) for d, r in enumerate(rs)])
    row_ref[0:16, :] = lse
    row_ref[16:32, :] = mean
    row_ref[32:33, :] = sum(r[32:33, :] for r in rs)
    row_ref[33:34, :] = functools.reduce(jnp.maximum, [r[33:34, :] for r in rs])
    row_ref[34:40, :] = jnp.zeros((6, 128), F32)
    cs = (b0, b1, b2, b3)
    lse, mean = merge([(rolled(c[0:8, :], d, 2), rolled(c[8:16, :], d, 2)) for d, c in enumerate(cs)])
    col_ref[0:8, :] = lse
    col_ref[8:16, :] = mean
    col_ref[16:17, :] = functools.reduce(jnp.maximum, [c[16:17, :] for c in cs])
    col_ref[17:24, :] = jnp.zeros((7, 128), F32)


def pieces_of(value):
    left, pieces = value * DOWN, []
    for _ in range(4):
        head = left.astype(BF16).astype(F32)
        head = jnp.where(jnp.abs(head) < TINY, 0.0, head)
        pieces.append(head)
        left = (left - head) * STEP
    return pieces


def value_of(pieces):
    total = pieces[3]
    for p in (pieces[2], pieces[1], pieces[0]):
        total = p + total * (1.0 / STEP)
    return total * (1.0 / DOWN)


def encoded(first, second):
    lane = lax.broadcasted_iota(jnp.int32, (1, 512), 1) % 256
    value = jnp.where(lane % 64 < 32, first, second)
    row = jnp.zeros((1, 512), F32)
    for p, piece in enumerate(pieces_of(value)):
        row = jnp.where(lane // 64 == p, piece, row)
    return row


def tail(row, at, half):
    shape = (8, 512)
    here = lax.broadcasted_iota(jnp.int32, shape, 0) == at
    if half is not None:
        here = here & (lax.broadcasted_iota(jnp.int32, shape, 1) // 256 == half)
    return jnp.where(here, jnp.broadcast_to(row, shape), 0.0)


def total_of(v):
    return jnp.sum(jnp.sum(v, axis=0, keepdims=True), axis=1, keepdims=True)


def end_kernel(s_ref, a0, a1, a2, a3, b0, b1, row_ref, col_ref, codes_ref, unit_ref, back_ref):
    rs = (a0, a1, a2, a3)
    lse, mean = merge([(rolled(r[0:16, :], d, 1), rolled(r[16:32, :], d, 1)) for d, r in enumerate(rs)])
    row_ref[...] = lse + 1.0
    diagonal = total_of(sum(r[32:33, :] for r in rs)) * LN2
    text_peak = greatest([r[33:34, :] for r in rs])
    codes_ref[1:2, :] = encoded(total_of(lse) * LN2 - 2.0 * diagonal, 0.5 * LN2 * total_of(mean) - diagonal)
    swapped = [jnp.concatenate([b1[k + 4 : k + 8, :], b1[k : k + 4, :]], axis=0) for k in (0, 8)]
    lse, mean = merge([(b0[0:8, :], b0[8:16, :]), swapped])
    for k in range(8):
        col_ref[:, 128 * k : 128 * (k + 1)] = lse[k : k + 1, :] + 1.0
    image_peak = jnp.maximum(b0[16:17, :], b1[16:17, :])
    codes_ref[0:1, :] = encoded(total_of(lse) * LN2, 0.5 * LN2 * total_of(mean))
    scale = s_ref[0, 0] * LN2
    for k, top in enumerate((text_peak, image_peak)):
        unit = 4.0 / jnp.maximum(top, 1e-30)
        unit_ref[k : k + 1, :] = unit
        back = scale / unit
        back_ref[k : k + 1, :] = jnp.concatenate([back] * 4, axis=1)


def image_kernel(which, l_ref, row_ref, col_ref, unit_ref, codes_ref, t0_ref, t1_ref, w_ref, g_ref):
    for j in range(4):
        at = slice(128 * j, 128 * (j + 1))
        row = row_ref[4 * which + j : 4 * which + j + 1, :]
        row = jnp.broadcast_to(row, (128, 128)).T
        for k in range(8):
            to = slice(128 * k, 128 * (k + 1))
            part = l_ref[at, to]
            w = jnp.exp2(part - row) + jnp.exp2(part - col_ref[:, to])
            if which == 0 and j == 0 and k == 0:
                w = w - jnp.where(eye(), 1.0, 0.0)
            w_ref[at, to] = w.astype(BF16)
    g = jnp.dot(w_ref[:, 0:512], t0_ref[...], preferred_element_type=F32)
    g = g + jnp.dot(w_ref[:, 512:1024], t1_ref[...], preferred_element_type=F32)
    g = g * unit_ref[0:1, 0:1]
    for k in range(4):
        g_ref[136 * k : 136 * k + 128, :] = g[128 * k : 128 * (k + 1), :]
        g_ref[136 * k + 128 : 136 * (k + 1), :] = tail(codes_ref[0:1, :], 4 * (k % 2) + which, k // 2)


def text_kernel(w0, w1, w2, w3, i0, i1, i2, i3, unit_ref, codes_ref, g0_ref, g1_ref):
    for h, g_ref in enumerate((g0_ref, g1_ref)):
        at = slice(512 * h, 512 * (h + 1))
        g = None
        for w, i in zip((w0, w1, w2, w3), (i0, i1, i2, i3)):
            part = lax.dot_general(w[:, at], i[...], TN, preferred_element_type=F32)
            g = part if g is None else g + part
        g = g * unit_ref[1:2, 0:1]
        for k in range(4):
            g_ref[136 * k : 136 * k + 128, :] = g[128 * k : 128 * (k + 1), :]
            g_ref[136 * k + 128 : 136 * (k + 1), :] = tail(codes_ref[1:2, :], 2 * k + h, 0)


def decode_kernel(i_ref, t_ref, loss_ref, grad_ref):
    rows = jnp.sum(i_ref[...] + t_ref[...], axis=0, keepdims=True)
    rows = rows[:, 0:256] + rows[:, 256:512]
    pair_total = ROWS * 128
    for v, (ref, count) in enumerate(((loss_ref, 2.0 * pair_total), (grad_ref, float(pair_total)))):
        ref[...] = value_of([rows[:, 64 * p + 32 * v : 64 * p + 32 * v + 1] for p in range(4)]) / count


def group(value, k):
    return value[136 * k : 136 * (k + 1)]


def body(images, texts, log_scale):
    s2 = jnp.reshape(jnp.exp(log_scale) * LOG2E, (1, 1))
    with jax.named_scope("line"):
        line = everyone(images, lambda v, d: turn(v, d, True))
    line = joined(line, "join_images")
    with jax.named_scope("plane"):
        chunks = everyone(line, lambda v, d: turn(v, d, False))
    with jax.named_scope("texts_x"):
        t0 = everyone(texts, along_x)
    t0 = joined(t0, "join_texts")
    with jax.named_scope("texts_c"):
        t1 = other_core(t0)
    parts = [None] * 4
    for k in (0, 1, 3, 2):
        with jax.named_scope(f"logits_{k}"):
            parts[k] = logits_of(k, s2, chunks[k], t0, t1)
    ls = [p[0] for p in parts]
    rows, cols = call(
        start_kernel,
        (out((40, 128)), out((24, 128))),
        *[p[1] for p in parts], *[p[2] for p in parts],
        name="start",
    )
    with jax.named_scope("rows_1"):
        rows = everyone(rows, lambda v, d: turn(v, d, True))
    with jax.named_scope("cols_1"):
        cols = everyone(cols, along_x)
    rows, cols = call(middle_kernel, (out((40, 128)), out((24, 128))), *rows, *cols, name="middle")
    with jax.named_scope("rows_2"):
        rows = everyone(rows, lambda v, d: turn(v, d, False))
    with jax.named_scope("cols_2"):
        cols = [cols, other_core(cols)]
    row_lse, col_lse, codes, unit, back = call(
        end_kernel,
        (out((16, 128)), out((1, 1024)), out((2, 512)), out((2, 128)), out((2, 512))),
        s2, *rows, *cols,
        smem=(0,),
        name="end",
    )
    ws, gs, sent = {}, {}, {}
    for k in (2, 1, 3, 0):
        with jax.named_scope(f"image_grad_{k}"):
            ws[k], gs[k] = call(
                functools.partial(image_kernel, k),
                (out((512, 1024), BF16), out((544, 512))),
                ls[k], row_lse, col_lse, unit, codes, t0, t1,
                name="image_grad",
            )
        if k:
            with jax.named_scope(f"images_back_{k}"):
                sent[k] = turn(gs[k].astype(F16), 4 - k, False)
    with jax.named_scope("text_grad"):
        g0, g1 = call(
            text_kernel,
            (out((544, 512)), out((544, 512))),
            *[ws[k] for k in range(4)], *chunks, unit, codes,
            name="text_grad",
        )
    with jax.named_scope("texts_back_c"):
        swap = other_core(g1.astype(F16))
    with jax.named_scope("texts_back_x"):
        moved = [along_x((group(g0, k) + group(swap, k).astype(F32)).astype(F16), 4 - k) for k in (2, 1, 3)]
        gt = group(g0, 0) + sum(m.astype(F32) for m in [group(swap, 0)] + moved)
    with jax.named_scope("images_back_2"):
        sums = [group(gs[0], k) + sum(group(m, k).astype(F32) for m in sent.values()) for k in range(4)]
        moved = [turn(sums[k].astype(F16), 4 - k, True) for k in (2, 1, 3)]
        gi = sums[0] + sum(m.astype(F32) for m in moved)
    loss, grad_scale = call(decode_kernel, (out((1, 1)), out((1, 1))), gi[128:], gt[128:], name="decode")
    grad_images = (gi[0:128] * back[0:1, :]).astype(BF16)
    grad_texts = (gt[0:128] * back[1:2, :]).astype(BF16)
    return grad_images, grad_texts, jnp.reshape(loss, ()), jnp.reshape(grad_scale, ())


def solution(mesh):
    split = Mesh(mesh.devices.reshape(4, 4, 2, mesh.shape["group"]), ALL)
    placed = (P(ALL, None), P(ALL, None), P())
    return jax.shard_map(
        body,
        mesh=split,
        in_specs=placed,
        out_specs=(P(ALL, None), P(ALL, None), P(), P()),
        check_vma=False,
    )
```

```python
import functools

import jax
import jax.numpy as jnp
from jax import lax
from jax.experimental import pallas as pl
from jax.experimental.pallas import tpu as pltpu
from jax.sharding import Mesh
from jax.sharding import PartitionSpec as P


ALL = ("x", "y", "c", "z")
F32, BF16, F16 = jnp.float32, jnp.bfloat16, jnp.float16
LOG2E = 1.4426950408889634
LN2 = 0.6931471805599453
OFFSETS = (1, 3, 2)
ROWS = 128
DOWN = 2.0**-11
STEP = 2.0**8
TINY = 6.2e-5


def turn(value, shift, first):
    pairs = []
    for y in range(4):
        for c in range(2):
            for z in range(4):
                if (c == 0) == first:
                    to = ((y + shift) % 4, c, z)
                else:
                    to = (y, c, (z + shift) % 4)
                pairs.append(((y * 2 + c) * 4 + z, (to[0] * 2 + to[1]) * 4 + to[2]))
    return lax.ppermute(value, ("y", "c", "z"), pairs)


def along_x(value, shift):
    return lax.ppermute(value, "x", [(i, (i + shift) % 4) for i in range(4)])


def other_core(value):
    return lax.ppermute(value, "c", [(0, 1), (1, 0)])


def everyone(value, move):
    got = {0: value}
    for d in OFFSETS:
        got[d] = move(value, d)
    return [got[d] for d in range(4)]


LINES = [[(y * 2) * 4 + z for y in range(4)] for z in range(4)] + [
    [(y * 2 + 1) * 4 + z for z in range(4)] for y in range(4)
]
NT = (((1,), (1,)), ((), ()))
TN = (((0,), (0,)), ((), ()))


def call(kernel, outs, *args, smem=(), scratch=()):
    return pl.pallas_call(
        kernel,
        out_shape=outs,
        in_specs=[
            pl.BlockSpec(memory_space=pltpu.SMEM if i in smem else pltpu.VMEM) for i in range(len(args))
        ],
        out_specs=jax.tree.map(lambda _: pl.BlockSpec(memory_space=pltpu.VMEM), outs),
        scratch_shapes=scratch,
        compiler_params=pltpu.CompilerParams(vmem_limit_bytes=16 << 20),
    )(*args)


def out(shape, dtype=F32):
    return pltpu.VMEM(shape, dtype)


def places():
    y, z, on_y = lax.axis_index("y"), lax.axis_index("z"), lax.axis_index("c") == 0
    return jnp.where(on_y, y, z), jnp.where(on_y, z, y), lax.axis_index("x")


def turn_kernel(axis, a_ref, o_ref):
    here = places()[axis]
    for d in range(4):
        at = pl.multiple_of(lax.rem(here - d + 4, 4) * 128, 128)
        o_ref[128 * d : 128 * (d + 1), :] = a_ref[pl.ds(at, 128), :]


def join_kernel(a0, a1, a2, a3, o_ref):
    for k, a in enumerate((a0, a1, a2, a3)):
        o_ref[128 * k : 128 * (k + 1), :] = a[...]


def lined_up(value):
    copies = jnp.broadcast_to(value[None], (4, ROWS, value.shape[1]))
    got = lax.all_to_all(copies, ("y", "c", "z"), 0, 0, axis_index_groups=LINES, tiled=True)
    return call(functools.partial(turn_kernel, 0), out((512, 512), BF16), got.reshape(512, -1))


def peak(ref):
    tall = jnp.max(jnp.abs(ref[...].astype(F32)), axis=0, keepdims=True)
    return jnp.broadcast_to(jnp.max(tall, axis=1, keepdims=True), (1, 128))


def logits_kernel(first, s_ref, im_ref, t0_ref, t1_ref, l_ref, rows_ref, cols_ref, top_scr, sum_scr, mean_scr):
    s2 = s_ref[0, 0]
    for h, t_ref in enumerate((t0_ref, t1_ref)):
        l_ref[:, 512 * h : 512 * (h + 1)] = s2 * lax.dot_general(
            im_ref[...], t_ref[...], NT, preferred_element_type=F32
        )

    def tops(i, col_tops):
        here = pl.ds(pl.multiple_of(i * 64, 64), 64)
        row_top, new = None, []
        for k in range(8):
            part = l_ref[here, 128 * k : 128 * (k + 1)]
            row_top = part if row_top is None else jnp.maximum(row_top, part)
            new.append(jnp.maximum(col_tops[k], jnp.max(part.reshape(8, 8, 128), axis=0)))
        top_scr[here, :] = row_top
        return tuple(new)

    col_tops = lax.fori_loop(0, 8, tops, tuple(l_ref[0:8, 128 * k : 128 * (k + 1)] for k in range(8)))

    def sums(i, carry):
        here = pl.ds(pl.multiple_of(i * 64, 64), 64)
        row_top = top_scr[here, :]
        row_sum = row_mean = jnp.zeros((64, 128), F32)
        new = []
        for k in range(8):
            part = l_ref[here, 128 * k : 128 * (k + 1)]
            e = jnp.exp2(part - row_top)
            row_sum = row_sum + e
            row_mean = row_mean + e * part
            part = part.reshape(8, 8, 128)
            e = jnp.exp2(part - col_tops[k][None])
            new.append((carry[k][0] + jnp.sum(e, axis=0), carry[k][1] + jnp.sum(e * part, axis=0)))
        sum_scr[here, :] = row_sum
        mean_scr[here, :] = row_mean
        return tuple(new)

    zero = jnp.zeros((8, 128), F32)
    col_sums = lax.fori_loop(0, 8, sums, ((zero, zero),) * 8)
    for k in range(8):
        at = slice(128 * k, 128 * (k + 1))
        top = jnp.max(col_tops[k], axis=0, keepdims=True)
        e = jnp.exp2(col_tops[k] - top)
        cols_ref[0:1, at] = top
        cols_ref[1:2, at] = jnp.sum(e * col_sums[k][0], axis=0, keepdims=True)
        cols_ref[2:3, at] = jnp.sum(e * col_sums[k][1], axis=0, keepdims=True)
    for j in range(4):
        at = slice(128 * j, 128 * (j + 1))
        tops_here = top_scr[at, :].T
        top = jnp.max(tops_here, axis=0, keepdims=True)
        e = jnp.exp2(tops_here - top)
        total = jnp.sum(e * sum_scr[at, :].T, axis=0, keepdims=True)
        rows_ref[j : j + 1, :] = top + jnp.log2(total)
        rows_ref[4 + j : 5 + j, :] = jnp.sum(e * mean_scr[at, :].T, axis=0, keepdims=True) / total
    rows_ref[8:9, :] = peak(im_ref)
    if first:
        rows_ref[9:10, :] = jnp.maximum(peak(t0_ref), peak(t1_ref))
        block = l_ref[0:128, 0:128]
        rows_ref[10:11, :] = jnp.sum(jnp.where(eye(), block, 0.0), axis=0, keepdims=True)


def eye():
    shape = (128, 128)
    return lax.broadcasted_iota(jnp.int32, shape, 0) == lax.broadcasted_iota(jnp.int32, shape, 1)


def logits_of(k, s2, im, t0, t1):
    return call(
        functools.partial(logits_kernel, k == 0),
        (out((512, 1024)), out((16, 128)), out((8, 1024))),
        s2, im, t0, t1,
        smem=(0,),
        scratch=[pltpu.VMEM((512, 128), F32)] * 3,
    )


def merge(parts):
    top = functools.reduce(jnp.maximum, [p[0] for p in parts])
    es = [jnp.exp2(p[0] - top) for p in parts]
    total = sum(es)
    mean = sum(e * p[1] for e, p in zip(es, parts)) / total
    return top + jnp.log2(total), mean


def greatest(values):
    return functools.reduce(jnp.maximum, values)


def row_at(back_second, back_first):
    first, second, _ = places()
    return lax.rem(second - back_second + 4, 4) * 4 + lax.rem(first - back_first + 4, 4)


def start_kernel(r0, r1, r2, r3, c0, c1, c2, c3, all_ref, col_ref, scr):
    rs, cs = (r0, r1, r2, r3), (c0, c1, c2, c3)
    for k, r in enumerate(rs):
        for j in range(4):
            at = row_at(k, j)
            scr[pl.ds(at, 1), :] = r[j : j + 1, :]
            scr[pl.ds(16 + at, 1), :] = r[4 + j : 5 + j, :]
    scr[32:33, :] = r0[10:11, :]
    scr[33:34, :] = r0[9:10, :]
    scr[34:40, :] = jnp.zeros((6, 128), F32)
    message = scr[...]
    for k in range(16):
        all_ref[40 * k : 40 * (k + 1), :] = message
    top = greatest([c[0:1, :] for c in cs])
    es = [jnp.exp2(c[0:1, :] - top) for c in cs]
    total = sum(e * c[1:2, :] for e, c in zip(es, cs))
    mean = sum(e * c[2:3, :] for e, c in zip(es, cs)) / total
    lse = top + jnp.log2(total)
    for k in range(8):
        col_ref[k : k + 1, :] = lse[:, 128 * k : 128 * (k + 1)]
        col_ref[8 + k : 9 + k, :] = mean[:, 128 * k : 128 * (k + 1)]
    col_ref[16:17, :] = greatest([r[8:9, :] for r in rs])
    col_ref[17:24, :] = jnp.zeros((7, 128), F32)


def rolled(v, d, group):
    if d == 0:
        return v
    n = v.shape[0]
    size = n // group
    quarter = size // 4
    pieces = []
    for g in range(group):
        at = g * size
        pieces += [v[at + size - d * quarter : at + size, :], v[at : at + size - d * quarter, :]]
    return jnp.concatenate(pieces, axis=0)


def middle_kernel(b0, b1, col_ref):
    swapped = [jnp.concatenate([b1[k + 4 : k + 8, :], b1[k : k + 4, :]], axis=0) for k in (0, 8)]
    lse, mean = merge([(b0[0:8, :], b0[8:16, :]), swapped])
    col_ref[0:8, :] = lse
    col_ref[8:16, :] = mean
    col_ref[16:24, :] = jnp.maximum(b0[16:24, :], b1[16:24, :])


def pieces_of(value):
    left, pieces = value * DOWN, []
    for _ in range(4):
        head = left.astype(BF16).astype(F32)
        head = jnp.where(jnp.abs(head) < TINY, 0.0, head)
        pieces.append(head)
        left = (left - head) * STEP
    return pieces


def value_of(pieces):
    total = pieces[3]
    for p in (pieces[2], pieces[1], pieces[0]):
        total = p + total * (1.0 / STEP)
    return total * (1.0 / DOWN)


def encoded(first, second):
    lane = lax.broadcasted_iota(jnp.int32, (1, 512), 1) % 256
    value = jnp.where(lane % 64 < 32, first, second)
    row = jnp.zeros((1, 512), F32)
    for p, piece in enumerate(pieces_of(value)):
        row = jnp.where(lane // 64 == p, piece, row)
    return row


def tail(row, at, half):
    shape = (8, 512)
    here = lax.broadcasted_iota(jnp.int32, shape, 0) == at
    if half is not None:
        here = here & (lax.broadcasted_iota(jnp.int32, shape, 1) // 256 == half)
    return jnp.where(here, jnp.broadcast_to(row, shape), 0.0)


def total_of(v):
    return jnp.sum(jnp.sum(v, axis=0, keepdims=True), axis=1, keepdims=True)


def end_kernel(s_ref, a_ref, b0, b1, b2, b3, row_ref, col_ref, codes_ref, unit_ref, back_ref, scr):
    rs = [a_ref[40 * k : 40 * (k + 1), :] for k in range(16)]
    lse, mean = merge([(r[0:16, :], r[16:32, :]) for r in rs])
    scr[...] = lse + 1.0
    for k in range(4):
        for j in range(4):
            row_ref[4 * k + j : 4 * k + j + 1, :] = scr[pl.ds(row_at(k, j), 1), :]
    diagonal = total_of(sum(r[32:33, :] for r in rs)) * LN2
    text_peak = greatest([r[33:34, :] for r in rs])
    codes_ref[1:2, :] = encoded(total_of(lse) * LN2 - 2.0 * diagonal, 0.5 * LN2 * total_of(mean) - diagonal)
    cs = (b0, b1, b2, b3)
    lse, mean = merge([(rolled(c[0:8, :], d, 2), rolled(c[8:16, :], d, 2)) for d, c in enumerate(cs)])
    for k in range(8):
        col_ref[:, 128 * k : 128 * (k + 1)] = lse[k : k + 1, :] + 1.0
    image_peak = greatest([c[16:17, :] for c in cs])
    codes_ref[0:1, :] = encoded(total_of(lse) * LN2, 0.5 * LN2 * total_of(mean))
    scale = s_ref[0, 0] * LN2
    for k, top in enumerate((text_peak, image_peak)):
        unit = 4.0 / jnp.maximum(top, 1e-30)
        unit_ref[k : k + 1, :] = unit
        back = scale / unit
        back_ref[k : k + 1, :] = jnp.concatenate([back] * 4, axis=1)


def image_kernel(which, l_ref, row_ref, col_ref, unit_ref, codes_ref, t0_ref, t1_ref, w_ref, g_ref):
    for j in range(4):
        at = slice(128 * j, 128 * (j + 1))
        row = row_ref[4 * which + j : 4 * which + j + 1, :]
        row = jnp.broadcast_to(row, (128, 128)).T
        for k in range(8):
            to = slice(128 * k, 128 * (k + 1))
            part = l_ref[at, to]
            w = jnp.exp2(part - row) + jnp.exp2(part - col_ref[:, to])
            if which == 0 and j == 0 and k == 0:
                w = w - jnp.where(eye(), 1.0, 0.0)
            w_ref[at, to] = w.astype(BF16)
    g = jnp.dot(w_ref[:, 0:512], t0_ref[...], preferred_element_type=F32)
    g = g + jnp.dot(w_ref[:, 512:1024], t1_ref[...], preferred_element_type=F32)
    g = g * unit_ref[0:1, 0:1]
    for k in range(4):
        g_ref[136 * k : 136 * k + 128, :] = g[128 * k : 128 * (k + 1), :]
        g_ref[136 * k + 128 : 136 * (k + 1), :] = tail(codes_ref[0:1, :], 4 * (k % 2) + which, k // 2)


def text_kernel(w0, w1, w2, w3, i0, i1, i2, i3, unit_ref, codes_ref, g0_ref, g1_ref):
    for h, g_ref in enumerate((g0_ref, g1_ref)):
        at = slice(512 * h, 512 * (h + 1))
        g = None
        for w, i in zip((w0, w1, w2, w3), (i0, i1, i2, i3)):
            part = lax.dot_general(w[:, at], i[...], TN, preferred_element_type=F32)
            g = part if g is None else g + part
        g = g * unit_ref[1:2, 0:1]
        for k in range(4):
            g_ref[136 * k : 136 * k + 128, :] = g[128 * k : 128 * (k + 1), :]
            g_ref[136 * k + 128 : 136 * (k + 1), :] = tail(codes_ref[1:2, :], 2 * k + h, 0)


def decode_kernel(i_ref, t_ref, loss_ref, grad_ref):
    rows = jnp.sum(i_ref[...] + t_ref[...], axis=0, keepdims=True)
    rows = rows[:, 0:256] + rows[:, 256:512]
    pair_total = ROWS * 128
    for v, (ref, count) in enumerate(((loss_ref, 2.0 * pair_total), (grad_ref, float(pair_total)))):
        ref[...] = value_of([rows[:, 64 * p + 32 * v : 64 * p + 32 * v + 1] for p in range(4)]) / count


def group(value, k):
    return value[136 * k : 136 * (k + 1)]


def program(images, texts, log_scale):
    s2 = jnp.reshape(jnp.exp(log_scale) * LOG2E, (1, 1))
    line = lined_up(images)
    chunks = everyone(line, lambda v, d: turn(v, d, False))
    t0 = call(join_kernel, out((512, 512), BF16), *everyone(texts, along_x))
    t1 = other_core(t0)
    parts = [None] * 4
    for k in (0, 1, 3, 2):
        parts[k] = logits_of(k, s2, chunks[k], t0, t1)
    ls = [p[0] for p in parts]
    rows, cols = call(
        start_kernel,
        (out((640, 128)), out((24, 128))),
        *[p[1] for p in parts], *[p[2] for p in parts],
        scratch=[pltpu.VMEM((40, 128), F32)],
    )
    rows = lax.all_to_all(rows.reshape(16, 40, 128), ("y", "z"), 0, 0, tiled=True).reshape(640, 128)
    other = other_core(cols)
    cols = call(middle_kernel, out((24, 128)), cols, other)
    cols = everyone(cols, along_x)
    row_lse, col_lse, codes, unit, back = call(
        end_kernel,
        (out((16, 128)), out((1, 1024)), out((2, 512)), out((2, 128)), out((2, 512))),
        s2, rows, *cols,
        smem=(0,),
        scratch=[pltpu.VMEM((16, 128), F32)],
    )
    ws, gs, sent = {}, {}, {}
    for k in (2, 1, 3, 0):
        ws[k], gs[k] = call(
            functools.partial(image_kernel, k),
            (out((512, 1024), BF16), out((544, 512))),
            ls[k], row_lse, col_lse, unit, codes, t0, t1,
        )
        if k:
            sent[k] = turn(gs[k].astype(F16), 4 - k, False)
    g0, g1 = call(
        text_kernel,
        (out((544, 512)), out((544, 512))),
        *[ws[k] for k in range(4)], *chunks, unit, codes,
    )
    swap = other_core(g1.astype(F16))
    moved = []
    for k in (2, 1, 3):
        moved.append(along_x((group(g0, k) + group(swap, k).astype(F32)).astype(F16), 4 - k))
    gt = group(g0, 0) + sum(m.astype(F32) for m in [group(swap, 0)] + moved)
    sums = [group(gs[0], k) + sum(group(m, k).astype(F32) for m in sent.values()) for k in range(4)]
    moved = []
    for k in (2, 1, 3):
        moved.append(turn(sums[k].astype(F16), 4 - k, True))
    gi = sums[0] + sum(m.astype(F32) for m in moved)
    loss, grad_scale = call(decode_kernel, (out((1, 1)), out((1, 1))), gi[128:], gt[128:])
    grad_images = (gi[0:128] * back[0:1, :]).astype(BF16)
    grad_texts = (gt[0:128] * back[1:2, :]).astype(BF16)
    return grad_images, grad_texts, jnp.reshape(loss, ()), jnp.reshape(grad_scale, ())


def solution(mesh):
    split = Mesh(mesh.devices.reshape(4, 4, 2, mesh.shape["group"]), ALL)
    placed = (P(ALL, None), P(ALL, None), P())
    return jax.shard_map(
        program,
        mesh=split,
        in_specs=placed,
        out_specs=(P(ALL, None), P(ALL, None), P(), P()),
        check_vma=False,
    )
```

```python
import functools

import jax
import jax.numpy as jnp
from jax import lax
from jax.experimental import pallas as pl
from jax.experimental.pallas import tpu as pltpu
from jax.sharding import Mesh
from jax.sharding import PartitionSpec as P


ALL = ("x", "y", "c", "z")
F32, BF16, F16 = jnp.float32, jnp.bfloat16, jnp.float16
LOG2E = 1.4426950408889634
LN2 = 0.6931471805599453
OFFSETS = (1, 3, 2)
ROWS = 128
DOWN = 2.0**-11
STEP = 2.0**8
TINY = 6.2e-5


def turn(value, shift, first):
    pairs = []
    for y in range(4):
        for c in range(2):
            for z in range(4):
                if (c == 0) == first:
                    to = ((y + shift) % 4, c, z)
                else:
                    to = (y, c, (z + shift) % 4)
                pairs.append(((y * 2 + c) * 4 + z, (to[0] * 2 + to[1]) * 4 + to[2]))
    return lax.ppermute(value, ("y", "c", "z"), pairs)


def along_x(value, shift):
    return lax.ppermute(value, "x", [(i, (i + shift) % 4) for i in range(4)])


def other_core(value):
    return lax.ppermute(value, "c", [(0, 1), (1, 0)])


def everyone(value, move):
    got = {0: value}
    for d in OFFSETS:
        got[d] = move(value, d)
    return [got[d] for d in range(4)]


NT = (((1,), (1,)), ((), ()))
TN = (((0,), (0,)), ((), ()))


def call(kernel, outs, *args, smem=(), scratch=()):
    return pl.pallas_call(
        kernel,
        out_shape=outs,
        in_specs=[
            pl.BlockSpec(memory_space=pltpu.SMEM if i in smem else pltpu.VMEM) for i in range(len(args))
        ],
        out_specs=jax.tree.map(lambda _: pl.BlockSpec(memory_space=pltpu.VMEM), outs),
        scratch_shapes=scratch,
        compiler_params=pltpu.CompilerParams(vmem_limit_bytes=16 << 20),
    )(*args)


def out(shape, dtype=F32):
    return pltpu.VMEM(shape, dtype)


def join_kernel(a0, a1, a2, a3, o_ref):
    for k, a in enumerate((a0, a1, a2, a3)):
        o_ref[128 * k : 128 * (k + 1), :] = a[...]


def joined(values):
    return call(join_kernel, out((512, 512), BF16), *values)


def peak(ref):
    tall = jnp.max(jnp.abs(ref[...].astype(F32)), axis=0, keepdims=True)
    return jnp.broadcast_to(jnp.max(tall, axis=1, keepdims=True), (1, 128))


def logits_kernel(first, s_ref, im_ref, t0_ref, t1_ref, l_ref, rows_ref, cols_ref, top_scr, sum_scr, mean_scr):
    s2 = s_ref[0, 0]
    for h, t_ref in enumerate((t0_ref, t1_ref)):
        l_ref[:, 512 * h : 512 * (h + 1)] = s2 * lax.dot_general(
            im_ref[...], t_ref[...], NT, preferred_element_type=F32
        )

    def tops(i, col_tops):
        here = pl.ds(pl.multiple_of(i * 64, 64), 64)
        row_top, new = None, []
        for k in range(8):
            part = l_ref[here, 128 * k : 128 * (k + 1)]
            row_top = part if row_top is None else jnp.maximum(row_top, part)
            new.append(jnp.maximum(col_tops[k], jnp.max(part.reshape(8, 8, 128), axis=0)))
        top_scr[here, :] = row_top
        return tuple(new)

    col_tops = lax.fori_loop(0, 8, tops, tuple(l_ref[0:8, 128 * k : 128 * (k + 1)] for k in range(8)))

    def sums(i, carry):
        here = pl.ds(pl.multiple_of(i * 64, 64), 64)
        row_top = top_scr[here, :]
        row_sum = row_mean = jnp.zeros((64, 128), F32)
        new = []
        for k in range(8):
            part = l_ref[here, 128 * k : 128 * (k + 1)]
            e = jnp.exp2(part - row_top)
            row_sum = row_sum + e
            row_mean = row_mean + e * part
            part = part.reshape(8, 8, 128)
            e = jnp.exp2(part - col_tops[k][None])
            new.append((carry[k][0] + jnp.sum(e, axis=0), carry[k][1] + jnp.sum(e * part, axis=0)))
        sum_scr[here, :] = row_sum
        mean_scr[here, :] = row_mean
        return tuple(new)

    zero = jnp.zeros((8, 128), F32)
    col_sums = lax.fori_loop(0, 8, sums, ((zero, zero),) * 8)
    for k in range(8):
        at = slice(128 * k, 128 * (k + 1))
        top = jnp.max(col_tops[k], axis=0, keepdims=True)
        e = jnp.exp2(col_tops[k] - top)
        cols_ref[0:1, at] = top
        cols_ref[1:2, at] = jnp.sum(e * col_sums[k][0], axis=0, keepdims=True)
        cols_ref[2:3, at] = jnp.sum(e * col_sums[k][1], axis=0, keepdims=True)
    for j in range(4):
        at = slice(128 * j, 128 * (j + 1))
        tops_here = top_scr[at, :].T
        top = jnp.max(tops_here, axis=0, keepdims=True)
        e = jnp.exp2(tops_here - top)
        total = jnp.sum(e * sum_scr[at, :].T, axis=0, keepdims=True)
        rows_ref[j : j + 1, :] = top + jnp.log2(total)
        rows_ref[4 + j : 5 + j, :] = jnp.sum(e * mean_scr[at, :].T, axis=0, keepdims=True) / total
    rows_ref[8:9, :] = peak(im_ref)
    if first:
        rows_ref[9:10, :] = jnp.maximum(peak(t0_ref), peak(t1_ref))
        block = l_ref[0:128, 0:128]
        rows_ref[10:11, :] = jnp.sum(jnp.where(eye(), block, 0.0), axis=0, keepdims=True)


def eye():
    shape = (128, 128)
    return lax.broadcasted_iota(jnp.int32, shape, 0) == lax.broadcasted_iota(jnp.int32, shape, 1)


def logits_of(k, s2, im, t0, t1):
    return call(
        functools.partial(logits_kernel, k == 0),
        (out((512, 1024)), out((16, 128)), out((8, 1024))),
        s2, im, t0, t1,
        smem=(0,),
        scratch=[pltpu.VMEM((512, 128), F32)] * 3,
    )


def merge(parts):
    top = functools.reduce(jnp.maximum, [p[0] for p in parts])
    es = [jnp.exp2(p[0] - top) for p in parts]
    total = sum(es)
    mean = sum(e * p[1] for e, p in zip(es, parts)) / total
    return top + jnp.log2(total), mean


def greatest(values):
    return functools.reduce(jnp.maximum, values)


def start_kernel(r0, r1, r2, r3, c0, c1, c2, c3, row_ref, col_ref):
    rs, cs = (r0, r1, r2, r3), (c0, c1, c2, c3)
    for k, r in enumerate(rs):
        row_ref[4 * k : 4 * k + 4, :] = r[0:4, :]
        row_ref[16 + 4 * k : 20 + 4 * k, :] = r[4:8, :]
    row_ref[32:33, :] = r0[10:11, :]
    row_ref[33:34, :] = r0[9:10, :]
    row_ref[34:40, :] = jnp.zeros((6, 128), F32)
    top = greatest([c[0:1, :] for c in cs])
    es = [jnp.exp2(c[0:1, :] - top) for c in cs]
    total = sum(e * c[1:2, :] for e, c in zip(es, cs))
    mean = sum(e * c[2:3, :] for e, c in zip(es, cs)) / total
    lse = top + jnp.log2(total)
    for k in range(8):
        col_ref[k : k + 1, :] = lse[:, 128 * k : 128 * (k + 1)]
        col_ref[8 + k : 9 + k, :] = mean[:, 128 * k : 128 * (k + 1)]
    col_ref[16:17, :] = greatest([r[8:9, :] for r in rs])
    col_ref[17:24, :] = jnp.zeros((7, 128), F32)


def rolled(v, d, group):
    if d == 0:
        return v
    n = v.shape[0]
    size = n // group
    quarter = size // 4
    pieces = []
    for g in range(group):
        at = g * size
        pieces += [v[at + size - d * quarter : at + size, :], v[at : at + size - d * quarter, :]]
    return jnp.concatenate(pieces, axis=0)


def middle_kernel(a0, a1, a2, a3, b0, b1, b2, b3, row_ref, col_ref):
    rs = (a0, a1, a2, a3)
    lse, mean = merge([(rolled(r[0:16, :], d, 4), rolled(r[16:32, :], d, 4)) for d, r in enumerate(rs)])
    row_ref[0:16, :] = lse
    row_ref[16:32, :] = mean
    row_ref[32:33, :] = sum(r[32:33, :] for r in rs)
    row_ref[33:34, :] = functools.reduce(jnp.maximum, [r[33:34, :] for r in rs])
    row_ref[34:40, :] = jnp.zeros((6, 128), F32)
    cs = (b0, b1, b2, b3)
    lse, mean = merge([(rolled(c[0:8, :], d, 2), rolled(c[8:16, :], d, 2)) for d, c in enumerate(cs)])
    col_ref[0:8, :] = lse
    col_ref[8:16, :] = mean
    col_ref[16:17, :] = functools.reduce(jnp.maximum, [c[16:17, :] for c in cs])
    col_ref[17:24, :] = jnp.zeros((7, 128), F32)


def pieces_of(value):
    left, pieces = value * DOWN, []
    for _ in range(4):
        head = left.astype(BF16).astype(F32)
        head = jnp.where(jnp.abs(head) < TINY, 0.0, head)
        pieces.append(head)
        left = (left - head) * STEP
    return pieces


def value_of(pieces):
    total = pieces[3]
    for p in (pieces[2], pieces[1], pieces[0]):
        total = p + total * (1.0 / STEP)
    return total * (1.0 / DOWN)


def encoded(first, second):
    lane = lax.broadcasted_iota(jnp.int32, (1, 512), 1) % 256
    value = jnp.where(lane % 64 < 32, first, second)
    row = jnp.zeros((1, 512), F32)
    for p, piece in enumerate(pieces_of(value)):
        row = jnp.where(lane // 64 == p, piece, row)
    return row


def tail(row, at, half):
    shape = (8, 512)
    here = lax.broadcasted_iota(jnp.int32, shape, 0) == at
    if half is not None:
        here = here & (lax.broadcasted_iota(jnp.int32, shape, 1) // 256 == half)
    return jnp.where(here, jnp.broadcast_to(row, shape), 0.0)


def total_of(v):
    return jnp.sum(jnp.sum(v, axis=0, keepdims=True), axis=1, keepdims=True)


def end_kernel(s_ref, a0, a1, a2, a3, b0, b1, row_ref, col_ref, codes_ref, unit_ref, back_ref):
    rs = (a0, a1, a2, a3)
    lse, mean = merge([(rolled(r[0:16, :], d, 1), rolled(r[16:32, :], d, 1)) for d, r in enumerate(rs)])
    row_ref[...] = lse + 1.0
    diagonal = total_of(sum(r[32:33, :] for r in rs)) * LN2
    text_peak = greatest([r[33:34, :] for r in rs])
    codes_ref[1:2, :] = encoded(total_of(lse) * LN2 - 2.0 * diagonal, 0.5 * LN2 * total_of(mean) - diagonal)
    swapped = [jnp.concatenate([b1[k + 4 : k + 8, :], b1[k : k + 4, :]], axis=0) for k in (0, 8)]
    lse, mean = merge([(b0[0:8, :], b0[8:16, :]), swapped])
    for k in range(8):
        col_ref[:, 128 * k : 128 * (k + 1)] = lse[k : k + 1, :] + 1.0
    image_peak = jnp.maximum(b0[16:17, :], b1[16:17, :])
    codes_ref[0:1, :] = encoded(total_of(lse) * LN2, 0.5 * LN2 * total_of(mean))
    scale = s_ref[0, 0] * LN2
    for k, top in enumerate((text_peak, image_peak)):
        unit = 4.0 / jnp.maximum(top, 1e-30)
        unit_ref[k : k + 1, :] = unit
        back = scale / unit
        back_ref[k : k + 1, :] = jnp.concatenate([back] * 4, axis=1)


def image_kernel(which, l_ref, row_ref, col_ref, unit_ref, codes_ref, t0_ref, t1_ref, w_ref, g_ref):
    for j in range(4):
        at = slice(128 * j, 128 * (j + 1))
        row = row_ref[4 * which + j : 4 * which + j + 1, :]
        row = jnp.broadcast_to(row, (128, 128)).T
        for k in range(8):
            to = slice(128 * k, 128 * (k + 1))
            part = l_ref[at, to]
            w = jnp.exp2(part - row) + jnp.exp2(part - col_ref[:, to])
            if which == 0 and j == 0 and k == 0:
                w = w - jnp.where(eye(), 1.0, 0.0)
            w_ref[at, to] = w.astype(BF16)
    g = jnp.dot(w_ref[:, 0:512], t0_ref[...], preferred_element_type=F32)
    g = g + jnp.dot(w_ref[:, 512:1024], t1_ref[...], preferred_element_type=F32)
    g = g * unit_ref[0:1, 0:1]
    for k in range(4):
        g_ref[136 * k : 136 * k + 128, :] = g[128 * k : 128 * (k + 1), :]
        g_ref[136 * k + 128 : 136 * (k + 1), :] = tail(codes_ref[0:1, :], 4 * (k % 2) + which, k // 2)


def text_kernel(w0, w1, w2, w3, i0, i1, i2, i3, unit_ref, codes_ref, g0_ref, g1_ref):
    for h, g_ref in enumerate((g0_ref, g1_ref)):
        at = slice(512 * h, 512 * (h + 1))
        g = None
        for w, i in zip((w0, w1, w2, w3), (i0, i1, i2, i3)):
            part = lax.dot_general(w[:, at], i[...], TN, preferred_element_type=F32)
            g = part if g is None else g + part
        g = g * unit_ref[1:2, 0:1]
        for k in range(4):
            g_ref[136 * k : 136 * k + 128, :] = g[128 * k : 128 * (k + 1), :]
            g_ref[136 * k + 128 : 136 * (k + 1), :] = tail(codes_ref[1:2, :], 2 * k + h, 0)


def decode_kernel(i_ref, t_ref, loss_ref, grad_ref):
    rows = jnp.sum(i_ref[...] + t_ref[...], axis=0, keepdims=True)
    rows = rows[:, 0:256] + rows[:, 256:512]
    pair_total = ROWS * 128
    for v, (ref, count) in enumerate(((loss_ref, 2.0 * pair_total), (grad_ref, float(pair_total)))):
        ref[...] = value_of([rows[:, 64 * p + 32 * v : 64 * p + 32 * v + 1] for p in range(4)]) / count


def group(value, k):
    return value[136 * k : 136 * (k + 1)]


def program(images, texts, log_scale):
    s2 = jnp.reshape(jnp.exp(log_scale) * LOG2E, (1, 1))
    line = everyone(images, lambda v, d: turn(v, d, True))
    line = joined(line)
    chunks = everyone(line, lambda v, d: turn(v, d, False))
    t0 = everyone(texts, along_x)
    t0 = joined(t0)
    t1 = other_core(t0)
    parts = [None] * 4
    for k in (0, 1, 3, 2):
        parts[k] = logits_of(k, s2, chunks[k], t0, t1)
    ls = [p[0] for p in parts]
    rows, cols = call(
        start_kernel,
        (out((40, 128)), out((24, 128))),
        *[p[1] for p in parts], *[p[2] for p in parts],
    )
    rows = everyone(rows, lambda v, d: turn(v, d, True))
    cols = everyone(cols, along_x)
    rows, cols = call(middle_kernel, (out((40, 128)), out((24, 128))), *rows, *cols)
    rows = everyone(rows, lambda v, d: turn(v, d, False))
    cols = [cols, other_core(cols)]
    row_lse, col_lse, codes, unit, back = call(
        end_kernel,
        (out((16, 128)), out((1, 1024)), out((2, 512)), out((2, 128)), out((2, 512))),
        s2, *rows, *cols,
        smem=(0,),
    )
    ws, gs, sent = {}, {}, {}
    for k in (2, 1, 3, 0):
        ws[k], gs[k] = call(
            functools.partial(image_kernel, k),
            (out((512, 1024), BF16), out((544, 512))),
            ls[k], row_lse, col_lse, unit, codes, t0, t1,
        )
        if k:
            sent[k] = turn(gs[k].astype(F16), 4 - k, False)
    g0, g1 = call(
        text_kernel,
        (out((544, 512)), out((544, 512))),
        *[ws[k] for k in range(4)], *chunks, unit, codes,
    )
    swap = other_core(g1.astype(F16))
    moved = []
    for k in (2, 1, 3):
        moved.append(along_x((group(g0, k) + group(swap, k).astype(F32)).astype(F16), 4 - k))
    gt = group(g0, 0) + sum(m.astype(F32) for m in [group(swap, 0)] + moved)
    sums = [group(gs[0], k) + sum(group(m, k).astype(F32) for m in sent.values()) for k in range(4)]
    moved = []
    for k in (2, 1, 3):
        moved.append(turn(sums[k].astype(F16), 4 - k, True))
    gi = sums[0] + sum(m.astype(F32) for m in moved)
    loss, grad_scale = call(decode_kernel, (out((1, 1)), out((1, 1))), gi[128:], gt[128:])
    grad_images = (gi[0:128] * back[0:1, :]).astype(BF16)
    grad_texts = (gt[0:128] * back[1:2, :]).astype(BF16)
    return grad_images, grad_texts, jnp.reshape(loss, ()), jnp.reshape(grad_scale, ())


def solution(mesh):
    split = Mesh(mesh.devices.reshape(4, 4, 2, mesh.shape["group"]), ALL)
    placed = (P(ALL, None), P(ALL, None), P())
    return jax.shard_map(
        program,
        mesh=split,
        in_specs=placed,
        out_specs=(P(ALL, None), P(ALL, None), P(), P()),
        check_vma=False,
    )
```

```python
import functools

import jax
import jax.numpy as jnp
from jax import lax
from jax.experimental import pallas as pl
from jax.experimental.pallas import tpu as pltpu
from jax.sharding import Mesh
from jax.sharding import PartitionSpec as P


ALL = ("x", "y", "c", "z")
F32, BF16, F16 = jnp.float32, jnp.bfloat16, jnp.float16
LOG2E = 1.4426950408889634
LN2 = 0.6931471805599453
OFFSETS = (1, 3, 2)
ROWS = 128
DOWN = 2.0**-11
STEP = 2.0**8
TINY = 6.2e-5


def turn(value, shift, first):
    pairs = []
    for y in range(4):
        for c in range(2):
            for z in range(4):
                if (c == 0) == first:
                    to = ((y + shift) % 4, c, z)
                else:
                    to = (y, c, (z + shift) % 4)
                pairs.append(((y * 2 + c) * 4 + z, (to[0] * 2 + to[1]) * 4 + to[2]))
    return lax.ppermute(value, ("y", "c", "z"), pairs)


def along_x(value, shift):
    return lax.ppermute(value, "x", [(i, (i + shift) % 4) for i in range(4)])


def other_core(value):
    return lax.ppermute(value, "c", [(0, 1), (1, 0)])


def everyone(value, move):
    got = {0: value}
    for d in OFFSETS:
        got[d] = move(value, d)
    return [got[d] for d in range(4)]


NT = (((1,), (1,)), ((), ()))
TN = (((0,), (0,)), ((), ()))


def call(kernel, outs, *args, smem=(), scratch=()):
    return pl.pallas_call(
        kernel,
        out_shape=outs,
        in_specs=[
            pl.BlockSpec(memory_space=pltpu.SMEM if i in smem else pltpu.VMEM) for i in range(len(args))
        ],
        out_specs=jax.tree.map(lambda _: pl.BlockSpec(memory_space=pltpu.VMEM), outs),
        scratch_shapes=scratch,
        compiler_params=pltpu.CompilerParams(vmem_limit_bytes=16 << 20),
    )(*args)


def out(shape, dtype=F32):
    return pltpu.VMEM(shape, dtype)


def join_kernel(a0, a1, a2, a3, o_ref):
    for k, a in enumerate((a0, a1, a2, a3)):
        o_ref[128 * k : 128 * (k + 1), :] = a[...]


def joined(values):
    return call(join_kernel, out((512, 512), BF16), *values)


def places():
    y, z, on_y = lax.axis_index("y"), lax.axis_index("z"), lax.axis_index("c") == 0
    return jnp.where(on_y, y, z), jnp.where(on_y, z, y), lax.axis_index("x")


def peak(ref):
    tall = jnp.max(jnp.abs(ref[...].astype(F32)), axis=0, keepdims=True)
    return jnp.broadcast_to(jnp.max(tall, axis=1, keepdims=True), (1, 128))


def logits_into(l_ref, s2, im_ref, t_refs):
    for h, t_ref in enumerate(t_refs):
        l_ref[:, 512 * h : 512 * (h + 1)] = s2 * lax.dot_general(
            im_ref[...], t_ref[...], NT, preferred_element_type=F32
        )


def logits_kernel(first, s_ref, im_ref, t0_ref, t1_ref, rows_ref, cols_ref, l_ref, top_scr, sum_scr, mean_scr):
    s2 = s_ref[0, 0]
    logits_into(l_ref, s2, im_ref, (t0_ref, t1_ref))

    def tops(i, col_tops):
        here = pl.ds(pl.multiple_of(i * 64, 64), 64)
        row_top, new = None, []
        for k in range(8):
            part = l_ref[here, 128 * k : 128 * (k + 1)]
            row_top = part if row_top is None else jnp.maximum(row_top, part)
            new.append(jnp.maximum(col_tops[k], jnp.max(part.reshape(8, 8, 128), axis=0)))
        top_scr[here, :] = row_top
        return tuple(new)

    col_tops = lax.fori_loop(0, 8, tops, tuple(l_ref[0:8, 128 * k : 128 * (k + 1)] for k in range(8)))

    def sums(i, carry):
        here = pl.ds(pl.multiple_of(i * 64, 64), 64)
        row_top = top_scr[here, :]
        row_sum = row_mean = jnp.zeros((64, 128), F32)
        new = []
        for k in range(8):
            part = l_ref[here, 128 * k : 128 * (k + 1)]
            e = jnp.exp2(part - row_top)
            row_sum = row_sum + e
            row_mean = row_mean + e * part
            part = part.reshape(8, 8, 128)
            e = jnp.exp2(part - col_tops[k][None])
            new.append((carry[k][0] + jnp.sum(e, axis=0), carry[k][1] + jnp.sum(e * part, axis=0)))
        sum_scr[here, :] = row_sum
        mean_scr[here, :] = row_mean
        return tuple(new)

    zero = jnp.zeros((8, 128), F32)
    col_sums = lax.fori_loop(0, 8, sums, ((zero, zero),) * 8)
    for k in range(8):
        at = slice(128 * k, 128 * (k + 1))
        top = jnp.max(col_tops[k], axis=0, keepdims=True)
        e = jnp.exp2(col_tops[k] - top)
        cols_ref[0:1, at] = top
        cols_ref[1:2, at] = jnp.sum(e * col_sums[k][0], axis=0, keepdims=True)
        cols_ref[2:3, at] = jnp.sum(e * col_sums[k][1], axis=0, keepdims=True)
    for j in range(4):
        at = slice(128 * j, 128 * (j + 1))
        tops_here = top_scr[at, :].T
        top = jnp.max(tops_here, axis=0, keepdims=True)
        e = jnp.exp2(tops_here - top)
        total = jnp.sum(e * sum_scr[at, :].T, axis=0, keepdims=True)
        rows_ref[j : j + 1, :] = top + jnp.log2(total)
        rows_ref[4 + j : 5 + j, :] = jnp.sum(e * mean_scr[at, :].T, axis=0, keepdims=True) / total
    rows_ref[8:9, :] = peak(im_ref)
    if first:
        rows_ref[9:10, :] = jnp.maximum(peak(t0_ref), peak(t1_ref))
        block = l_ref[0:128, 0:128]
        rows_ref[10:11, :] = jnp.sum(jnp.where(eye(), block, 0.0), axis=0, keepdims=True)


def eye():
    shape = (128, 128)
    return lax.broadcasted_iota(jnp.int32, shape, 0) == lax.broadcasted_iota(jnp.int32, shape, 1)


def logits_of(k, s2, im, t0, t1):
    return call(
        functools.partial(logits_kernel, k == 0),
        (out((16, 128)), out((8, 1024))),
        s2, im, t0, t1,
        smem=(0,),
        scratch=[pltpu.VMEM((512, 1024), F32)] + [pltpu.VMEM((512, 128), F32)] * 3,
    )


def merge(parts):
    top = functools.reduce(jnp.maximum, [p[0] for p in parts])
    es = [jnp.exp2(p[0] - top) for p in parts]
    total = sum(es)
    mean = sum(e * p[1] for e, p in zip(es, parts)) / total
    return top + jnp.log2(total), mean


def greatest(values):
    return functools.reduce(jnp.maximum, values)


def row_at(back_second, back_first):
    first, second, _ = places()
    return lax.rem(second - back_second + 4, 4) * 4 + lax.rem(first - back_first + 4, 4)


def start_kernel(r0, r1, r2, r3, c0, c1, c2, c3, all_ref, col_ref, scr):
    rs, cs = (r0, r1, r2, r3), (c0, c1, c2, c3)
    for k, r in enumerate(rs):
        for j in range(4):
            at = row_at(k, j)
            scr[pl.ds(at, 1), :] = r[j : j + 1, :]
            scr[pl.ds(16 + at, 1), :] = r[4 + j : 5 + j, :]
    scr[32:33, :] = r0[10:11, :]
    scr[33:34, :] = r0[9:10, :]
    scr[34:40, :] = jnp.zeros((6, 128), F32)
    message = scr[...]
    for k in range(16):
        all_ref[40 * k : 40 * (k + 1), :] = message
    top = greatest([c[0:1, :] for c in cs])
    es = [jnp.exp2(c[0:1, :] - top) for c in cs]
    total = sum(e * c[1:2, :] for e, c in zip(es, cs))
    mean = sum(e * c[2:3, :] for e, c in zip(es, cs)) / total
    lse = top + jnp.log2(total)
    for k in range(8):
        col_ref[k : k + 1, :] = lse[:, 128 * k : 128 * (k + 1)]
        col_ref[8 + k : 9 + k, :] = mean[:, 128 * k : 128 * (k + 1)]
    col_ref[16:17, :] = greatest([r[8:9, :] for r in rs])
    col_ref[17:24, :] = jnp.zeros((7, 128), F32)


def rolled(v, d, group):
    if d == 0:
        return v
    n = v.shape[0]
    size = n // group
    quarter = size // 4
    pieces = []
    for g in range(group):
        at = g * size
        pieces += [v[at + size - d * quarter : at + size, :], v[at : at + size - d * quarter, :]]
    return jnp.concatenate(pieces, axis=0)


def middle_kernel(b0, b1, b2, b3, col_ref):
    cs = (b0, b1, b2, b3)
    lse, mean = merge([(rolled(c[0:8, :], d, 2), rolled(c[8:16, :], d, 2)) for d, c in enumerate(cs)])
    col_ref[0:8, :] = lse
    col_ref[8:16, :] = mean
    col_ref[16:24, :] = greatest([c[16:24, :] for c in cs])


def pieces_of(value):
    left, pieces = value * DOWN, []
    for _ in range(4):
        head = left.astype(BF16).astype(F32)
        head = jnp.where(jnp.abs(head) < TINY, 0.0, head)
        pieces.append(head)
        left = (left - head) * STEP
    return pieces


def value_of(pieces):
    total = pieces[3]
    for p in (pieces[2], pieces[1], pieces[0]):
        total = p + total * (1.0 / STEP)
    return total * (1.0 / DOWN)


def encoded(first, second):
    lane = lax.broadcasted_iota(jnp.int32, (1, 512), 1) % 256
    value = jnp.where(lane % 64 < 32, first, second)
    row = jnp.zeros((1, 512), F32)
    for p, piece in enumerate(pieces_of(value)):
        row = jnp.where(lane // 64 == p, piece, row)
    return row


def tail(row, at, half):
    shape = (8, 512)
    here = lax.broadcasted_iota(jnp.int32, shape, 0) == at
    if half is not None:
        here = here & (lax.broadcasted_iota(jnp.int32, shape, 1) // 256 == half)
    return jnp.where(here, jnp.broadcast_to(row, shape), 0.0)


def total_of(v):
    return jnp.sum(jnp.sum(v, axis=0, keepdims=True), axis=1, keepdims=True)


def end_kernel(s_ref, a_ref, b0, b1, row_ref, col_ref, codes_ref, unit_ref, back_ref, scr):
    rs = [a_ref[40 * k : 40 * (k + 1), :] for k in range(16)]
    lse, mean = merge([(r[0:16, :], r[16:32, :]) for r in rs])
    scr[...] = lse + 1.0
    for k in range(4):
        for j in range(4):
            row_ref[4 * k + j : 4 * k + j + 1, :] = scr[pl.ds(row_at(k, j), 1), :]
    diagonal = total_of(sum(r[32:33, :] for r in rs)) * LN2
    text_peak = greatest([r[33:34, :] for r in rs])
    codes_ref[1:2, :] = encoded(total_of(lse) * LN2 - 2.0 * diagonal, 0.5 * LN2 * total_of(mean) - diagonal)
    swapped = [jnp.concatenate([b1[k + 4 : k + 8, :], b1[k : k + 4, :]], axis=0) for k in (0, 8)]
    lse, mean = merge([(b0[0:8, :], b0[8:16, :]), swapped])
    for k in range(8):
        col_ref[:, 128 * k : 128 * (k + 1)] = lse[k : k + 1, :] + 1.0
    image_peak = jnp.maximum(b0[16:17, :], b1[16:17, :])
    codes_ref[0:1, :] = encoded(total_of(lse) * LN2, 0.5 * LN2 * total_of(mean))
    scale = s_ref[0, 0] * LN2
    for k, top in enumerate((text_peak, image_peak)):
        unit = 4.0 / jnp.maximum(top, 1e-30)
        unit_ref[k : k + 1, :] = unit
        back = scale / unit
        back_ref[k : k + 1, :] = jnp.concatenate([back] * 4, axis=1)


def image_kernel(which, s_ref, im_ref, row_ref, col_ref, unit_ref, codes_ref, t0_ref, t1_ref, w_ref, g_ref, l_ref):
    logits_into(l_ref, s_ref[0, 0], im_ref, (t0_ref, t1_ref))
    for j in range(4):
        at = slice(128 * j, 128 * (j + 1))
        row = row_ref[4 * which + j : 4 * which + j + 1, :]
        row = jnp.broadcast_to(row, (128, 128)).T
        for k in range(8):
            to = slice(128 * k, 128 * (k + 1))
            part = l_ref[at, to]
            w = jnp.exp2(part - row) + jnp.exp2(part - col_ref[:, to])
            if which == 0 and j == 0 and k == 0:
                w = w - jnp.where(eye(), 1.0, 0.0)
            w_ref[at, to] = w.astype(BF16)
    g = jnp.dot(w_ref[:, 0:512], t0_ref[...], preferred_element_type=F32)
    g = g + jnp.dot(w_ref[:, 512:1024], t1_ref[...], preferred_element_type=F32)
    g = g * unit_ref[0:1, 0:1]
    for k in range(4):
        g_ref[136 * k : 136 * k + 128, :] = g[128 * k : 128 * (k + 1), :]
        g_ref[136 * k + 128 : 136 * (k + 1), :] = tail(codes_ref[0:1, :], 4 * (k % 2) + which, k // 2)


def text_kernel(w0, w1, w2, w3, i0, i1, i2, i3, unit_ref, codes_ref, g0_ref, g1_ref):
    for h, g_ref in enumerate((g0_ref, g1_ref)):
        at = slice(512 * h, 512 * (h + 1))
        g = None
        for w, i in zip((w0, w1, w2, w3), (i0, i1, i2, i3)):
            part = lax.dot_general(w[:, at], i[...], TN, preferred_element_type=F32)
            g = part if g is None else g + part
        g = g * unit_ref[1:2, 0:1]
        for k in range(4):
            g_ref[136 * k : 136 * k + 128, :] = g[128 * k : 128 * (k + 1), :]
            g_ref[136 * k + 128 : 136 * (k + 1), :] = tail(codes_ref[1:2, :], 2 * k + h, 0)


def decode_kernel(i_ref, t_ref, loss_ref, grad_ref):
    rows = jnp.sum(i_ref[...] + t_ref[...], axis=0, keepdims=True)
    rows = rows[:, 0:256] + rows[:, 256:512]
    pair_total = ROWS * 128
    for v, (ref, count) in enumerate(((loss_ref, 2.0 * pair_total), (grad_ref, float(pair_total)))):
        ref[...] = value_of([rows[:, 64 * p + 32 * v : 64 * p + 32 * v + 1] for p in range(4)]) / count


def group(value, k):
    return value[136 * k : 136 * (k + 1)]


def program(images, texts, log_scale):
    s2 = jnp.reshape(jnp.exp(log_scale) * LOG2E, (1, 1))
    line = everyone(images, lambda v, d: turn(v, d, True))
    line = joined(line)
    chunks = everyone(line, lambda v, d: turn(v, d, False))
    t0 = everyone(texts, along_x)
    t0 = joined(t0)
    t1 = other_core(t0)
    parts = [None] * 4
    for k in (0, 1, 3, 2):
        parts[k] = logits_of(k, s2, chunks[k], t0, t1)
    rows, cols = call(
        start_kernel,
        (jax.ShapeDtypeStruct((640, 128), F32), out((24, 128))),
        *[p[0] for p in parts], *[p[1] for p in parts],
        scratch=[pltpu.VMEM((40, 128), F32)],
    )
    cols = everyone(cols, along_x)
    rows = lax.all_to_all(rows.reshape(16, 40, 128), ("y", "z"), 0, 0, tiled=True).reshape(640, 128)
    cols = call(middle_kernel, out((24, 128)), *cols)
    cols = [cols, other_core(cols)]
    row_lse, col_lse, codes, unit, back = call(
        end_kernel,
        (out((16, 128)), out((1, 1024)), out((2, 512)), out((2, 128)), out((2, 512))),
        s2, rows, *cols,
        smem=(0,),
        scratch=[pltpu.VMEM((16, 128), F32)],
    )
    ws, gs, sent = {}, {}, {}
    for k in (2, 1, 3, 0):
        ws[k], gs[k] = call(
            functools.partial(image_kernel, k),
            (out((512, 1024), BF16), out((544, 512))),
            s2, chunks[k], row_lse, col_lse, unit, codes, t0, t1,
            smem=(0,),
            scratch=[pltpu.VMEM((512, 1024), F32)],
        )
        if k:
            sent[k] = turn(gs[k].astype(F16), 4 - k, False)
    g0, g1 = call(
        text_kernel,
        (out((544, 512)), out((544, 512))),
        *[ws[k] for k in range(4)], *chunks, unit, codes,
    )
    swap = other_core(g1.astype(F16))
    moved = []
    for k in (2, 1, 3):
        moved.append(along_x((group(g0, k) + group(swap, k).astype(F32)).astype(F16), 4 - k))
    gt = group(g0, 0) + sum(m.astype(F32) for m in [group(swap, 0)] + moved)
    sums = [group(gs[0], k) + sum(group(m, k).astype(F32) for m in sent.values()) for k in range(4)]
    moved = []
    for k in (2, 1, 3):
        moved.append(turn(sums[k].astype(F16), 4 - k, True))
    gi = sums[0] + sum(m.astype(F32) for m in moved)
    loss, grad_scale = call(decode_kernel, (out((1, 1)), out((1, 1))), gi[128:], gt[128:])
    grad_images = (gi[0:128] * back[0:1, :]).astype(BF16)
    grad_texts = (gt[0:128] * back[1:2, :]).astype(BF16)
    return grad_images, grad_texts, jnp.reshape(loss, ()), jnp.reshape(grad_scale, ())


def solution(mesh):
    split = Mesh(mesh.devices.reshape(4, 4, 2, mesh.shape["group"]), ALL)
    placed = (P(ALL, None), P(ALL, None), P())
    return jax.shard_map(
        program,
        mesh=split,
        in_specs=placed,
        out_specs=(P(ALL, None), P(ALL, None), P(), P()),
        check_vma=False,
    )
```

```python
import functools

import jax
import jax.numpy as jnp
from jax import lax
from jax.experimental import pallas as pl
from jax.experimental.pallas import tpu as pltpu
from jax.sharding import Mesh
from jax.sharding import PartitionSpec as P


ALL = ("x", "y", "c", "z")
F32, BF16, F16 = jnp.float32, jnp.bfloat16, jnp.float16
LOG2E = 1.4426950408889634
LN2 = 0.6931471805599453
OFFSETS = (1, 3, 2)
ROWS = 128
DOWN = 2.0**-11
STEP = 2.0**8
TINY = 6.2e-5


def turn(value, shift, first):
    pairs = []
    for y in range(4):
        for c in range(2):
            for z in range(4):
                if (c == 0) == first:
                    to = ((y + shift) % 4, c, z)
                else:
                    to = (y, c, (z + shift) % 4)
                pairs.append(((y * 2 + c) * 4 + z, (to[0] * 2 + to[1]) * 4 + to[2]))
    return lax.ppermute(value, ("y", "c", "z"), pairs)


def along_x(value, shift):
    return lax.ppermute(value, "x", [(i, (i + shift) % 4) for i in range(4)])


def other_core(value):
    return lax.ppermute(value, "c", [(0, 1), (1, 0)])


def everyone(value, move):
    got = {0: value}
    for d in OFFSETS:
        got[d] = move(value, d)
    return [got[d] for d in range(4)]


NT = (((1,), (1,)), ((), ()))
TN = (((0,), (0,)), ((), ()))


def call(kernel, outs, *args, smem=(), scratch=()):
    return pl.pallas_call(
        kernel,
        out_shape=outs,
        in_specs=[
            pl.BlockSpec(memory_space=pltpu.SMEM if i in smem else pltpu.VMEM) for i in range(len(args))
        ],
        out_specs=jax.tree.map(lambda _: pl.BlockSpec(memory_space=pltpu.VMEM), outs),
        scratch_shapes=scratch,
        compiler_params=pltpu.CompilerParams(vmem_limit_bytes=16 << 20),
    )(*args)


def out(shape, dtype=F32):
    return pltpu.VMEM(shape, dtype)


def hold_kernel(a_ref, o_ref):
    o_ref[...] = a_ref[...]


def held(value):
    return call(hold_kernel, out((ROWS, 512), BF16), value)


def join_kernel(a0, a1, a2, a3, o_ref):
    for k, a in enumerate((a0, a1, a2, a3)):
        o_ref[128 * k : 128 * (k + 1), :] = a[...]


def joined(values):
    return call(join_kernel, out((512, 512), BF16), *values)


def places():
    y, z, on_y = lax.axis_index("y"), lax.axis_index("z"), lax.axis_index("c") == 0
    return jnp.where(on_y, y, z), jnp.where(on_y, z, y), lax.axis_index("x")


def peak(ref):
    tall = jnp.max(jnp.abs(ref[...].astype(F32)), axis=0, keepdims=True)
    return jnp.broadcast_to(jnp.max(tall, axis=1, keepdims=True), (1, 128))


def logits_into(l_ref, s2, im_ref, t_refs):
    for h, t_ref in enumerate(t_refs):
        l_ref[:, 512 * h : 512 * (h + 1)] = s2 * lax.dot_general(
            im_ref[...], t_ref[...], NT, preferred_element_type=F32
        )


def logits_kernel(first, s_ref, im_ref, t0_ref, t1_ref, rows_ref, cols_ref, l_ref, top_scr, sum_scr, mean_scr):
    s2 = s_ref[0, 0]
    logits_into(l_ref, s2, im_ref, (t0_ref, t1_ref))

    def tops(i, col_tops):
        here = pl.ds(pl.multiple_of(i * 64, 64), 64)
        row_top, new = None, []
        for k in range(8):
            part = l_ref[here, 128 * k : 128 * (k + 1)]
            row_top = part if row_top is None else jnp.maximum(row_top, part)
            new.append(jnp.maximum(col_tops[k], jnp.max(part.reshape(8, 8, 128), axis=0)))
        top_scr[here, :] = row_top
        return tuple(new)

    col_tops = lax.fori_loop(
        0, 8, tops, tuple(l_ref[0:8, 128 * k : 128 * (k + 1)] for k in range(8)), unroll=True
    )

    def sums(i, carry):
        here = pl.ds(pl.multiple_of(i * 64, 64), 64)
        row_top = top_scr[here, :]
        row_sum = row_mean = jnp.zeros((64, 128), F32)
        new = []
        for k in range(8):
            part = l_ref[here, 128 * k : 128 * (k + 1)]
            e = jnp.exp2(part - row_top)
            row_sum = row_sum + e
            row_mean = row_mean + e * part
            part = part.reshape(8, 8, 128)
            e = jnp.exp2(part - col_tops[k][None])
            new.append((carry[k][0] + jnp.sum(e, axis=0), carry[k][1] + jnp.sum(e * part, axis=0)))
        sum_scr[here, :] = row_sum
        mean_scr[here, :] = row_mean
        return tuple(new)

    zero = jnp.zeros((8, 128), F32)
    col_sums = lax.fori_loop(0, 8, sums, ((zero, zero),) * 8, unroll=True)
    for k in range(8):
        at = slice(128 * k, 128 * (k + 1))
        top = jnp.max(col_tops[k], axis=0, keepdims=True)
        e = jnp.exp2(col_tops[k] - top)
        cols_ref[0:1, at] = top
        cols_ref[1:2, at] = jnp.sum(e * col_sums[k][0], axis=0, keepdims=True)
        cols_ref[2:3, at] = jnp.sum(e * col_sums[k][1], axis=0, keepdims=True)
    for j in range(4):
        at = slice(128 * j, 128 * (j + 1))
        tops_here = top_scr[at, :].T
        top = jnp.max(tops_here, axis=0, keepdims=True)
        e = jnp.exp2(tops_here - top)
        total = jnp.sum(e * sum_scr[at, :].T, axis=0, keepdims=True)
        rows_ref[j : j + 1, :] = top + jnp.log2(total)
        rows_ref[4 + j : 5 + j, :] = jnp.sum(e * mean_scr[at, :].T, axis=0, keepdims=True) / total
    rows_ref[8:9, :] = peak(im_ref)
    if first:
        rows_ref[9:10, :] = jnp.maximum(peak(t0_ref), peak(t1_ref))
        block = l_ref[0:128, 0:128]
        rows_ref[10:11, :] = jnp.sum(jnp.where(eye(), block, 0.0), axis=0, keepdims=True)


def eye():
    shape = (128, 128)
    return lax.broadcasted_iota(jnp.int32, shape, 0) == lax.broadcasted_iota(jnp.int32, shape, 1)


def logits_of(k, s2, im, t0, t1):
    return call(
        functools.partial(logits_kernel, k == 0),
        (out((16, 128)), out((8, 1024))),
        s2, im, t0, t1,
        smem=(0,),
        scratch=[pltpu.VMEM((512, 1024), F32)] + [pltpu.VMEM((512, 128), F32)] * 3,
    )


def merge(parts):
    top = functools.reduce(jnp.maximum, [p[0] for p in parts])
    es = [jnp.exp2(p[0] - top) for p in parts]
    total = sum(es)
    mean = sum(e * p[1] for e, p in zip(es, parts)) / total
    return top + jnp.log2(total), mean


def greatest(values):
    return functools.reduce(jnp.maximum, values)


def row_at(back_second, back_first):
    first, second, _ = places()
    return lax.rem(second - back_second + 4, 4) * 4 + lax.rem(first - back_first + 4, 4)


def row_kernel(r0, r1, r2, r3, all_ref, scr):
    for k, r in enumerate((r0, r1, r2, r3)):
        for j in range(4):
            at = row_at(k, j)
            scr[pl.ds(at, 1), :] = r[j : j + 1, :]
            scr[pl.ds(16 + at, 1), :] = r[4 + j : 5 + j, :]
    scr[32:33, :] = r0[10:11, :]
    scr[33:34, :] = r0[9:10, :]
    scr[34:40, :] = jnp.zeros((6, 128), F32)
    message = scr[...]
    for k in range(16):
        all_ref[40 * k : 40 * (k + 1), :] = message


def col_kernel(r0, r1, r2, r3, c0, c1, c2, c3, col_ref):
    rs, cs = (r0, r1, r2, r3), (c0, c1, c2, c3)
    top = greatest([c[0:1, :] for c in cs])
    es = [jnp.exp2(c[0:1, :] - top) for c in cs]
    total = sum(e * c[1:2, :] for e, c in zip(es, cs))
    mean = sum(e * c[2:3, :] for e, c in zip(es, cs)) / total
    lse = top + jnp.log2(total)
    for k in range(8):
        col_ref[k : k + 1, :] = lse[:, 128 * k : 128 * (k + 1)]
        col_ref[8 + k : 9 + k, :] = mean[:, 128 * k : 128 * (k + 1)]
    col_ref[16:17, :] = greatest([r[8:9, :] for r in rs])
    col_ref[17:24, :] = jnp.zeros((7, 128), F32)


def rolled(v, d, group):
    if d == 0:
        return v
    n = v.shape[0]
    size = n // group
    quarter = size // 4
    pieces = []
    for g in range(group):
        at = g * size
        pieces += [v[at + size - d * quarter : at + size, :], v[at : at + size - d * quarter, :]]
    return jnp.concatenate(pieces, axis=0)


def middle_kernel(b0, b1, b2, b3, col_ref):
    cs = (b0, b1, b2, b3)
    lse, mean = merge([(rolled(c[0:8, :], d, 2), rolled(c[8:16, :], d, 2)) for d, c in enumerate(cs)])
    col_ref[0:8, :] = lse
    col_ref[8:16, :] = mean
    col_ref[16:24, :] = greatest([c[16:24, :] for c in cs])


def pieces_of(value):
    left, pieces = value * DOWN, []
    for _ in range(4):
        head = left.astype(BF16).astype(F32)
        head = jnp.where(jnp.abs(head) < TINY, 0.0, head)
        pieces.append(head)
        left = (left - head) * STEP
    return pieces


def value_of(pieces):
    total = pieces[3]
    for p in (pieces[2], pieces[1], pieces[0]):
        total = p + total * (1.0 / STEP)
    return total * (1.0 / DOWN)


def encoded(first, second):
    lane = lax.broadcasted_iota(jnp.int32, (1, 512), 1) % 256
    value = jnp.where(lane % 64 < 32, first, second)
    row = jnp.zeros((1, 512), F32)
    for p, piece in enumerate(pieces_of(value)):
        row = jnp.where(lane // 64 == p, piece, row)
    return row


def tail(row, at, half):
    shape = (8, 512)
    here = lax.broadcasted_iota(jnp.int32, shape, 0) == at
    if half is not None:
        here = here & (lax.broadcasted_iota(jnp.int32, shape, 1) // 256 == half)
    return jnp.where(here, jnp.broadcast_to(row, shape), 0.0)


def total_of(v):
    return jnp.sum(jnp.sum(v, axis=0, keepdims=True), axis=1, keepdims=True)


def end_kernel(s_ref, a_ref, b0, b1, row_ref, col_ref, codes_ref, unit_ref, back_ref, scr):
    rs = [a_ref[40 * k : 40 * (k + 1), :] for k in range(16)]
    lse, mean = merge([(r[0:16, :], r[16:32, :]) for r in rs])
    scr[...] = lse + 1.0
    for k in range(4):
        for j in range(4):
            row_ref[4 * k + j : 4 * k + j + 1, :] = scr[pl.ds(row_at(k, j), 1), :]
    diagonal = total_of(sum(r[32:33, :] for r in rs)) * LN2
    text_peak = greatest([r[33:34, :] for r in rs])
    codes_ref[1:2, :] = encoded(total_of(lse) * LN2 - 2.0 * diagonal, 0.5 * LN2 * total_of(mean) - diagonal)
    swapped = [jnp.concatenate([b1[k + 4 : k + 8, :], b1[k : k + 4, :]], axis=0) for k in (0, 8)]
    lse, mean = merge([(b0[0:8, :], b0[8:16, :]), swapped])
    for k in range(8):
        col_ref[:, 128 * k : 128 * (k + 1)] = lse[k : k + 1, :] + 1.0
    image_peak = jnp.maximum(b0[16:17, :], b1[16:17, :])
    codes_ref[0:1, :] = encoded(total_of(lse) * LN2, 0.5 * LN2 * total_of(mean))
    scale = s_ref[0, 0] * LN2
    for k, top in enumerate((text_peak, image_peak)):
        unit = 4.0 / jnp.maximum(top, 1e-30)
        unit_ref[k : k + 1, :] = unit
        back = scale / unit
        back_ref[k : k + 1, :] = jnp.concatenate([back] * 4, axis=1)


def image_kernel(which, s_ref, im_ref, row_ref, col_ref, unit_ref, codes_ref, t0_ref, t1_ref, w_ref, g_ref, l_ref):
    logits_into(l_ref, s_ref[0, 0], im_ref, (t0_ref, t1_ref))
    for j in range(4):
        at = slice(128 * j, 128 * (j + 1))
        row = row_ref[4 * which + j : 4 * which + j + 1, :]
        row = jnp.broadcast_to(row, (128, 128)).T
        for k in range(8):
            to = slice(128 * k, 128 * (k + 1))
            part = l_ref[at, to]
            w = jnp.exp2(part - row) + jnp.exp2(part - col_ref[:, to])
            if which == 0 and j == 0 and k == 0:
                w = w - jnp.where(eye(), 1.0, 0.0)
            w_ref[at, to] = w.astype(BF16)
    g = jnp.dot(w_ref[:, 0:512], t0_ref[...], preferred_element_type=F32)
    g = g + jnp.dot(w_ref[:, 512:1024], t1_ref[...], preferred_element_type=F32)
    g = g * unit_ref[0:1, 0:1]
    for k in range(4):
        g_ref[136 * k : 136 * k + 128, :] = g[128 * k : 128 * (k + 1), :]
        g_ref[136 * k + 128 : 136 * (k + 1), :] = tail(codes_ref[0:1, :], 4 * (k % 2) + which, k // 2)


def text_kernel(h, w0, w1, w2, w3, i0, i1, i2, i3, unit_ref, codes_ref, g_ref):
    at = slice(512 * h, 512 * (h + 1))
    g = None
    for w, i in zip((w0, w1, w2, w3), (i0, i1, i2, i3)):
        part = lax.dot_general(w[:, at], i[...], TN, preferred_element_type=F32)
        g = part if g is None else g + part
    g = g * unit_ref[1:2, 0:1]
    for k in range(4):
        g_ref[136 * k : 136 * k + 128, :] = g[128 * k : 128 * (k + 1), :]
        g_ref[136 * k + 128 : 136 * (k + 1), :] = tail(codes_ref[1:2, :], 2 * k + h, 0)


def texts_end_kernel(g_ref, back_ref, o_ref, tail_ref):
    o_ref[...] = (g_ref[0:128, :] * back_ref[1:2, :]).astype(BF16)
    tail_ref[...] = g_ref[128:136, :]


def images_end_kernel(g_ref, t_ref, back_ref, o_ref, loss_ref, grad_ref):
    o_ref[...] = (g_ref[0:128, :] * back_ref[0:1, :]).astype(BF16)
    rows = jnp.sum(g_ref[128:136, :] + t_ref[...], axis=0, keepdims=True)
    rows = rows[:, 0:256] + rows[:, 256:512]
    pair_total = ROWS * 128
    for v, (ref, count) in enumerate(((loss_ref, 2.0 * pair_total), (grad_ref, float(pair_total)))):
        ref[...] = value_of([rows[:, 64 * p + 32 * v : 64 * p + 32 * v + 1] for p in range(4)]) / count


def group(value, k):
    return value[136 * k : 136 * (k + 1)]


def program(images, texts, log_scale):
    s2 = jnp.reshape(jnp.exp(log_scale) * LOG2E, (1, 1))
    line = [held(images)] + everyone(images, lambda v, d: turn(v, d, True))[1:]
    line = joined(line)
    chunks = everyone(line, lambda v, d: turn(v, d, False))
    t0 = [held(texts)] + everyone(texts, along_x)[1:]
    t0 = joined(t0)
    t1 = other_core(t0)
    parts = [None] * 4
    for k in (0, 1, 3, 2):
        parts[k] = logits_of(k, s2, chunks[k], t0, t1)
    cols = call(col_kernel, out((24, 128)), *[p[0] for p in parts], *[p[1] for p in parts])
    rows = call(
        row_kernel, jax.ShapeDtypeStruct((640, 128), F32), *[p[0] for p in parts], scratch=[pltpu.VMEM((40, 128), F32)]
    )
    cols = everyone(cols, along_x)
    rows = lax.all_to_all(rows.reshape(16, 40, 128), ("y", "z"), 0, 0, tiled=True).reshape(640, 128)
    cols = call(middle_kernel, out((24, 128)), *cols)
    cols = [cols, other_core(cols)]
    row_lse, col_lse, codes, unit, back = call(
        end_kernel,
        (out((16, 128)), out((1, 1024)), out((2, 512)), out((2, 128)), out((2, 512))),
        s2, rows, *cols,
        smem=(0,),
        scratch=[pltpu.VMEM((16, 128), F32)],
    )
    ws, gs, sent = {}, {}, {}
    for k in (2, 1, 3, 0):
        ws[k], gs[k] = call(
            functools.partial(image_kernel, k),
            (out((512, 1024), BF16), out((544, 512))),
            s2, chunks[k], row_lse, col_lse, unit, codes, t0, t1,
            smem=(0,),
            scratch=[pltpu.VMEM((512, 1024), F32)],
        )
        if k:
            sent[k] = turn(gs[k].astype(F16), 4 - k, False)
    g0, g1 = [
        call(
            functools.partial(text_kernel, h),
            out((544, 512)),
            *[ws[k] for k in range(4)], *chunks, unit, codes,
        )
        for h in range(2)
    ]
    swap = other_core(g1.astype(F16))
    moved = []
    for k in (2, 1, 3):
        moved.append(along_x((group(g0, k) + group(swap, k).astype(F32)).astype(F16), 4 - k))
    gt = group(g0, 0) + sum(m.astype(F32) for m in [group(swap, 0)] + moved)
    sums = [group(gs[0], k) + sum(group(m, k).astype(F32) for m in sent.values()) for k in range(4)]
    moved = []
    for k in (2, 1, 3):
        moved.append(turn(sums[k].astype(F16), 4 - k, True))
    gi = sums[0] + sum(m.astype(F32) for m in moved)
    grad_texts, gt_tail = call(
        texts_end_kernel,
        (jax.ShapeDtypeStruct((ROWS, 512), BF16), out((8, 512))),
        gt, back,
    )
    grad_images, loss, grad_scale = call(
        images_end_kernel,
        (jax.ShapeDtypeStruct((ROWS, 512), BF16),) + (jax.ShapeDtypeStruct((1, 1), F32),) * 2,
        gi, gt_tail, back,
    )
    return grad_images, grad_texts, jnp.reshape(loss, ()), jnp.reshape(grad_scale, ())


def solution(mesh):
    split = Mesh(mesh.devices.reshape(4, 4, 2, mesh.shape["group"]), ALL)
    placed = (P(ALL, None), P(ALL, None), P())
    return jax.shard_map(
        program,
        mesh=split,
        in_specs=placed,
        out_specs=(P(ALL, None), P(ALL, None), P(), P()),
        check_vma=False,
    )
```

```python
import functools

import jax
import jax.numpy as jnp
from jax import lax
from jax.experimental import pallas as pl
from jax.experimental.pallas import tpu as pltpu
from jax.sharding import Mesh
from jax.sharding import PartitionSpec as P


ALL = ("x", "y", "c", "z")
F32, BF16, F16 = jnp.float32, jnp.bfloat16, jnp.float16
LOG2E = 1.4426950408889634
LN2 = 0.6931471805599453
OFFSETS = (1, 3, 2)
ROWS = 128
DOWN = 2.0**-11
STEP = 2.0**8
TINY = 6.2e-5


def turn(value, shift, first):
    pairs = []
    for y in range(4):
        for c in range(2):
            for z in range(4):
                if (c == 0) == first:
                    to = ((y + shift) % 4, c, z)
                else:
                    to = (y, c, (z + shift) % 4)
                pairs.append(((y * 2 + c) * 4 + z, (to[0] * 2 + to[1]) * 4 + to[2]))
    return lax.ppermute(value, ("y", "c", "z"), pairs)


def along_x(value, shift):
    return lax.ppermute(value, "x", [(i, (i + shift) % 4) for i in range(4)])


def other_core(value):
    return lax.ppermute(value, "c", [(0, 1), (1, 0)])


def everyone(value, move):
    got = {0: value}
    for d in OFFSETS:
        got[d] = move(value, d)
    return [got[d] for d in range(4)]


NT = (((1,), (1,)), ((), ()))
TN = (((0,), (0,)), ((), ()))


def call(kernel, outs, *args, smem=(), scratch=()):
    return pl.pallas_call(
        kernel,
        out_shape=outs,
        in_specs=[
            pl.BlockSpec(memory_space=pltpu.SMEM if i in smem else pltpu.VMEM) for i in range(len(args))
        ],
        out_specs=jax.tree.map(lambda _: pl.BlockSpec(memory_space=pltpu.VMEM), outs),
        scratch_shapes=scratch,
        compiler_params=pltpu.CompilerParams(vmem_limit_bytes=16 << 20),
    )(*args)


def out(shape, dtype=F32):
    return pltpu.VMEM(shape, dtype)


def hold_kernel(a_ref, b_ref, a_out, b_out, sems):
    copies = [
        pltpu.make_async_copy(ref, o_ref, sems.at[k])
        for k, (ref, o_ref) in enumerate(((a_ref, a_out), (b_ref, b_out)))
    ]
    for copy in copies:
        copy.start()
    for copy in copies:
        copy.wait()


def held(a, b):
    return pl.pallas_call(
        hold_kernel,
        out_shape=(out(a.shape, BF16), out(b.shape, BF16)),
        in_specs=[pl.BlockSpec(memory_space=pl.ANY)] * 2,
        out_specs=(pl.BlockSpec(memory_space=pltpu.VMEM),) * 2,
        scratch_shapes=[pltpu.SemaphoreType.DMA((2,))],
        name="hold",
    )(a, b)


def join_kernel(*refs):
    o_ref, at = refs[-1], 0
    for a in refs[:-1]:
        o_ref[at : at + a.shape[0], :] = a[...]
        at += a.shape[0]


def joined(values):
    return call(join_kernel, out((512, 512), BF16), *values)


def places():
    y, z, on_y = lax.axis_index("y"), lax.axis_index("z"), lax.axis_index("c") == 0
    return jnp.where(on_y, y, z), jnp.where(on_y, z, y), lax.axis_index("x")


def peak(ref):
    tall = jnp.max(jnp.abs(ref[...].astype(F32)), axis=0, keepdims=True)
    return jnp.broadcast_to(jnp.max(tall, axis=1, keepdims=True), (1, 128))


def logits_into(l_ref, s2, im_ref, t_refs):
    for h, t_ref in enumerate(t_refs):
        l_ref[:, 512 * h : 512 * (h + 1)] = s2 * lax.dot_general(
            im_ref[...], t_ref[...], NT, preferred_element_type=F32
        )


def logits_kernel(first, s_ref, im_ref, t0_ref, t1_ref, rows_ref, cols_ref, l_ref, top_scr, sum_scr, mean_scr):
    s2 = s_ref[0, 0]
    logits_into(l_ref, s2, im_ref, (t0_ref, t1_ref))

    def tops(i, col_tops):
        here = pl.ds(pl.multiple_of(i * 64, 64), 64)
        row_top, new = None, []
        for k in range(8):
            part = l_ref[here, 128 * k : 128 * (k + 1)]
            row_top = part if row_top is None else jnp.maximum(row_top, part)
            new.append(jnp.maximum(col_tops[k], jnp.max(part.reshape(8, 8, 128), axis=0)))
        top_scr[here, :] = row_top
        return tuple(new)

    col_tops = lax.fori_loop(
        0, 8, tops, tuple(l_ref[0:8, 128 * k : 128 * (k + 1)] for k in range(8)), unroll=True
    )

    def sums(i, carry):
        here = pl.ds(pl.multiple_of(i * 64, 64), 64)
        row_top = top_scr[here, :]
        row_sum = row_mean = jnp.zeros((64, 128), F32)
        new = []
        for k in range(8):
            part = l_ref[here, 128 * k : 128 * (k + 1)]
            e = jnp.exp2(part - row_top)
            row_sum = row_sum + e
            row_mean = row_mean + e * part
            part = part.reshape(8, 8, 128)
            e = jnp.exp2(part - col_tops[k][None])
            new.append((carry[k][0] + jnp.sum(e, axis=0), carry[k][1] + jnp.sum(e * part, axis=0)))
        sum_scr[here, :] = row_sum
        mean_scr[here, :] = row_mean
        return tuple(new)

    zero = jnp.zeros((8, 128), F32)
    col_sums = lax.fori_loop(0, 8, sums, ((zero, zero),) * 8, unroll=True)
    for k in range(8):
        at = slice(128 * k, 128 * (k + 1))
        top = jnp.max(col_tops[k], axis=0, keepdims=True)
        e = jnp.exp2(col_tops[k] - top)
        cols_ref[0:1, at] = top
        cols_ref[1:2, at] = jnp.sum(e * col_sums[k][0], axis=0, keepdims=True)
        cols_ref[2:3, at] = jnp.sum(e * col_sums[k][1], axis=0, keepdims=True)
    for j in range(4):
        at = slice(128 * j, 128 * (j + 1))
        tops_here = top_scr[at, :].T
        top = jnp.max(tops_here, axis=0, keepdims=True)
        e = jnp.exp2(tops_here - top)
        total = jnp.sum(e * sum_scr[at, :].T, axis=0, keepdims=True)
        rows_ref[j : j + 1, :] = top + jnp.log2(total)
        rows_ref[4 + j : 5 + j, :] = jnp.sum(e * mean_scr[at, :].T, axis=0, keepdims=True) / total
    rows_ref[8:9, :] = peak(im_ref)
    if first:
        rows_ref[9:10, :] = jnp.maximum(peak(t0_ref), peak(t1_ref))
        block = l_ref[0:128, 0:128]
        rows_ref[10:11, :] = jnp.sum(jnp.where(eye(), block, 0.0), axis=0, keepdims=True)


def eye():
    shape = (128, 128)
    return lax.broadcasted_iota(jnp.int32, shape, 0) == lax.broadcasted_iota(jnp.int32, shape, 1)


def logits_of(k, s2, im, t0, t1):
    return call(
        functools.partial(logits_kernel, k == 0),
        (out((16, 128)), out((8, 1024))),
        s2, im, t0, t1,
        smem=(0,),
        scratch=[pltpu.VMEM((512, 1024), F32)] + [pltpu.VMEM((512, 128), F32)] * 3,
    )


def merge(parts):
    top = functools.reduce(jnp.maximum, [p[0] for p in parts])
    es = [jnp.exp2(p[0] - top) for p in parts]
    total = sum(es)
    mean = sum(e * p[1] for e, p in zip(es, parts)) / total
    return top + jnp.log2(total), mean


def greatest(values):
    return functools.reduce(jnp.maximum, values)


def row_at(back_second, back_first):
    first, second, _ = places()
    return lax.rem(second - back_second + 4, 4) * 4 + lax.rem(first - back_first + 4, 4)


def row_kernel(r0, r1, r2, r3, all_ref, scr):
    for k, r in enumerate((r0, r1, r2, r3)):
        for j in range(4):
            at = row_at(k, j)
            scr[pl.ds(at, 1), :] = r[j : j + 1, :]
            scr[pl.ds(16 + at, 1), :] = r[4 + j : 5 + j, :]
    scr[32:33, :] = r0[10:11, :]
    scr[33:34, :] = r0[9:10, :]
    scr[34:40, :] = jnp.zeros((6, 128), F32)
    message = scr[...]
    for k in range(16):
        all_ref[40 * k : 40 * (k + 1), :] = message


def col_kernel(r0, r1, r2, r3, c0, c1, c2, c3, col_ref):
    rs, cs = (r0, r1, r2, r3), (c0, c1, c2, c3)
    top = greatest([c[0:1, :] for c in cs])
    es = [jnp.exp2(c[0:1, :] - top) for c in cs]
    total = sum(e * c[1:2, :] for e, c in zip(es, cs))
    mean = sum(e * c[2:3, :] for e, c in zip(es, cs)) / total
    lse = top + jnp.log2(total)
    for k in range(8):
        col_ref[k : k + 1, :] = lse[:, 128 * k : 128 * (k + 1)]
        col_ref[8 + k : 9 + k, :] = mean[:, 128 * k : 128 * (k + 1)]
    col_ref[16:17, :] = greatest([r[8:9, :] for r in rs])
    col_ref[17:24, :] = jnp.zeros((7, 128), F32)


def rolled(v, d, group):
    if d == 0:
        return v
    n = v.shape[0]
    size = n // group
    quarter = size // 4
    pieces = []
    for g in range(group):
        at = g * size
        pieces += [v[at + size - d * quarter : at + size, :], v[at : at + size - d * quarter, :]]
    return jnp.concatenate(pieces, axis=0)


def middle_kernel(b0, b1, b2, b3, col_ref):
    cs = (b0, b1, b2, b3)
    lse, mean = merge([(rolled(c[0:8, :], d, 2), rolled(c[8:16, :], d, 2)) for d, c in enumerate(cs)])
    col_ref[0:8, :] = lse
    col_ref[8:16, :] = mean
    col_ref[16:24, :] = greatest([c[16:24, :] for c in cs])


def pieces_of(value):
    left, pieces = value * DOWN, []
    for _ in range(4):
        head = left.astype(BF16).astype(F32)
        head = jnp.where(jnp.abs(head) < TINY, 0.0, head)
        pieces.append(head)
        left = (left - head) * STEP
    return pieces


def value_of(pieces):
    total = pieces[3]
    for p in (pieces[2], pieces[1], pieces[0]):
        total = p + total * (1.0 / STEP)
    return total * (1.0 / DOWN)


def encoded(first, second):
    lane = lax.broadcasted_iota(jnp.int32, (1, 512), 1) % 256
    value = jnp.where(lane % 64 < 32, first, second)
    row = jnp.zeros((1, 512), F32)
    for p, piece in enumerate(pieces_of(value)):
        row = jnp.where(lane // 64 == p, piece, row)
    return row


def tail(row, at, half):
    shape = (8, 512)
    here = lax.broadcasted_iota(jnp.int32, shape, 0) == at
    if half is not None:
        here = here & (lax.broadcasted_iota(jnp.int32, shape, 1) // 256 == half)
    return jnp.where(here, jnp.broadcast_to(row, shape), 0.0)


def total_of(v):
    return jnp.sum(jnp.sum(v, axis=0, keepdims=True), axis=1, keepdims=True)


def end_kernel(s_ref, a_ref, b0, b1, row_ref, col_ref, codes_ref, unit_ref, back_ref, scr):
    rs = [a_ref[40 * k : 40 * (k + 1), :] for k in range(16)]
    lse, mean = merge([(r[0:16, :], r[16:32, :]) for r in rs])
    scr[...] = lse + 1.0
    for k in range(4):
        for j in range(4):
            row_ref[4 * k + j : 4 * k + j + 1, :] = scr[pl.ds(row_at(k, j), 1), :]
    diagonal = total_of(sum(r[32:33, :] for r in rs)) * LN2
    text_peak = greatest([r[33:34, :] for r in rs])
    codes_ref[1:2, :] = encoded(total_of(lse) * LN2 - 2.0 * diagonal, 0.5 * LN2 * total_of(mean) - diagonal)
    swapped = [jnp.concatenate([b1[k + 4 : k + 8, :], b1[k : k + 4, :]], axis=0) for k in (0, 8)]
    lse, mean = merge([(b0[0:8, :], b0[8:16, :]), swapped])
    for k in range(8):
        col_ref[:, 128 * k : 128 * (k + 1)] = lse[k : k + 1, :] + 1.0
    image_peak = jnp.maximum(b0[16:17, :], b1[16:17, :])
    codes_ref[0:1, :] = encoded(total_of(lse) * LN2, 0.5 * LN2 * total_of(mean))
    scale = s_ref[0, 0] * LN2
    for k, top in enumerate((text_peak, image_peak)):
        unit = 4.0 / jnp.maximum(top, 1e-30)
        unit_ref[k : k + 1, :] = unit
        back = scale / unit
        back_ref[k : k + 1, :] = jnp.concatenate([back] * 4, axis=1)


def image_kernel(which, s_ref, im_ref, row_ref, col_ref, unit_ref, codes_ref, t0_ref, t1_ref, w_ref, g_ref, l_ref):
    logits_into(l_ref, s_ref[0, 0], im_ref, (t0_ref, t1_ref))
    for j in range(4):
        at = slice(128 * j, 128 * (j + 1))
        row = row_ref[4 * which + j : 4 * which + j + 1, :]
        row = jnp.broadcast_to(row, (128, 128)).T
        for k in range(8):
            to = slice(128 * k, 128 * (k + 1))
            part = l_ref[at, to]
            w = jnp.exp2(part - row) + jnp.exp2(part - col_ref[:, to])
            if which == 0 and j == 0 and k == 0:
                w = w - jnp.where(eye(), 1.0, 0.0)
            w_ref[at, to] = w.astype(BF16)
    g = jnp.dot(w_ref[:, 0:512], t0_ref[...], preferred_element_type=F32)
    g = g + jnp.dot(w_ref[:, 512:1024], t1_ref[...], preferred_element_type=F32)
    g = g * unit_ref[0:1, 0:1]
    for k in range(4):
        g_ref[136 * k : 136 * k + 128, :] = g[128 * k : 128 * (k + 1), :]
        g_ref[136 * k + 128 : 136 * (k + 1), :] = tail(codes_ref[0:1, :], 4 * (k % 2) + which, k // 2)


def text_kernel(h, w0, w1, w2, w3, i0, i1, i2, i3, unit_ref, codes_ref, g_ref):
    at = slice(512 * h, 512 * (h + 1))
    g = None
    for w, i in zip((w0, w1, w2, w3), (i0, i1, i2, i3)):
        part = lax.dot_general(w[:, at], i[...], TN, preferred_element_type=F32)
        g = part if g is None else g + part
    g = g * unit_ref[1:2, 0:1]
    for k in range(4):
        g_ref[136 * k : 136 * k + 128, :] = g[128 * k : 128 * (k + 1), :]
        g_ref[136 * k + 128 : 136 * (k + 1), :] = tail(codes_ref[1:2, :], 2 * k + h, 0)


def texts_end_kernel(g_ref, back_ref, o_ref, tail_ref):
    o_ref[...] = (g_ref[0:128, :] * back_ref[1:2, :]).astype(BF16)
    tail_ref[...] = g_ref[128:136, :]


def images_end_kernel(g_ref, t_ref, back_ref, o_ref, loss_ref, grad_ref):
    o_ref[...] = (g_ref[0:128, :] * back_ref[0:1, :]).astype(BF16)
    rows = jnp.sum(g_ref[128:136, :] + t_ref[...], axis=0, keepdims=True)
    rows = rows[:, 0:256] + rows[:, 256:512]
    pair_total = ROWS * 128
    for v, (ref, count) in enumerate(((loss_ref, 2.0 * pair_total), (grad_ref, float(pair_total)))):
        ref[...] = value_of([rows[:, 64 * p + 32 * v : 64 * p + 32 * v + 1] for p in range(4)]) / count


def group(value, k):
    return value[136 * k : 136 * (k + 1)]


def program(images, texts, log_scale):
    s2 = jnp.reshape(jnp.exp(log_scale) * LOG2E, (1, 1))
    own_images, own_texts = held(images, texts)
    line = [own_images] + everyone(images, lambda v, d: turn(v, d, True))[1:]
    line = joined(line)
    chunks = [line, None, None, None]
    for d in (1, 3):
        chunks[d] = turn(line, d, False)
    halves = []
    for d, part in ((1, chunks[1][0:256]), (3, chunks[3][256:512])):
        halves.append(turn(part, d, False))
    chunks[2] = joined(halves)
    t0 = [own_texts] + everyone(texts, along_x)[1:]
    t0 = joined(t0)
    t1 = other_core(t0)
    parts = [None] * 4
    for k in (0, 1, 3, 2):
        parts[k] = logits_of(k, s2, chunks[k], t0, t1)
    cols = call(col_kernel, out((24, 128)), *[p[0] for p in parts], *[p[1] for p in parts])
    rows = call(
        row_kernel, jax.ShapeDtypeStruct((640, 128), F32), *[p[0] for p in parts], scratch=[pltpu.VMEM((40, 128), F32)]
    )
    cols = everyone(cols, along_x)
    rows = lax.all_to_all(rows.reshape(16, 40, 128), ("y", "z"), 0, 0, tiled=True).reshape(640, 128)
    cols = call(middle_kernel, out((24, 128)), *cols)
    cols = [cols, other_core(cols)]
    row_lse, col_lse, codes, unit, back = call(
        end_kernel,
        (out((16, 128)), out((1, 1024)), out((2, 512)), out((2, 128)), out((2, 512))),
        s2, rows, *cols,
        smem=(0,),
        scratch=[pltpu.VMEM((16, 128), F32)],
    )
    ws, gs, sent = {}, {}, {}
    for k in (2, 1, 3, 0):
        ws[k], gs[k] = call(
            functools.partial(image_kernel, k),
            (out((512, 1024), BF16), out((544, 512))),
            s2, chunks[k], row_lse, col_lse, unit, codes, t0, t1,
            smem=(0,),
            scratch=[pltpu.VMEM((512, 1024), F32)],
        )
        if k == 2:
            for d, part in ((3, gs[k][0:272]), (1, gs[k][272:544])):
                sent[d] = turn(part.astype(F16), d, False).astype(F32)
        elif k:
            mine = [gs[k][0:272], gs[k][272:544]]
            mine[k // 2] = mine[k // 2] + sent.pop(4 - k)
            mine = jnp.concatenate([m.astype(F16) for m in mine], axis=0)
            sent[k + 4] = turn(mine, 4 - k, False)
    g0, g1 = [
        call(
            functools.partial(text_kernel, h),
            out((544, 512)),
            *[ws[k] for k in range(4)], *chunks, unit, codes,
        )
        for h in range(2)
    ]
    swap = other_core(g1.astype(F16))
    moved = []
    for k in (2, 1, 3):
        moved.append(along_x((group(g0, k) + group(swap, k).astype(F32)).astype(F16), 4 - k))
    gt = group(g0, 0) + sum(m.astype(F32) for m in [group(swap, 0)] + moved)
    sums = [group(gs[0], k) + sum(group(m, k).astype(F32) for m in sent.values()) for k in range(4)]
    moved = []
    for k in (2, 1, 3):
        moved.append(turn(sums[k].astype(F16), 4 - k, True))
    gi = sums[0] + sum(m.astype(F32) for m in moved)
    grad_texts, gt_tail = call(
        texts_end_kernel,
        (jax.ShapeDtypeStruct((ROWS, 512), BF16), out((8, 512))),
        gt, back,
    )
    grad_images, loss, grad_scale = call(
        images_end_kernel,
        (jax.ShapeDtypeStruct((ROWS, 512), BF16),) + (jax.ShapeDtypeStruct((1, 1), F32),) * 2,
        gi, gt_tail, back,
    )
    return grad_images, grad_texts, jnp.reshape(loss, ()), jnp.reshape(grad_scale, ())


def solution(mesh):
    split = Mesh(mesh.devices.reshape(4, 4, 2, mesh.shape["group"]), ALL)
    placed = (P(ALL, None), P(ALL, None), P())
    return jax.shard_map(
        program,
        mesh=split,
        in_specs=placed,
        out_specs=(P(ALL, None), P(ALL, None), P(), P()),
        check_vma=False,
    )
```

```python
import functools

import jax
import jax.numpy as jnp
from jax import lax
from jax.experimental import pallas as pl
from jax.experimental.pallas import tpu as pltpu
from jax.sharding import Mesh
from jax.sharding import PartitionSpec as P


ALL = ("x", "y", "c", "z")
F32, BF16, F16 = jnp.float32, jnp.bfloat16, jnp.float16
LOG2E = 1.4426950408889634
LN2 = 0.6931471805599453
OFFSETS = (1, 3, 2)
ROWS = 128
DOWN = 2.0**-11
STEP = 2.0**8
TINY = 6.2e-5


def turn(value, shift, first):
    pairs = []
    for y in range(4):
        for c in range(2):
            for z in range(4):
                if (c == 0) == first:
                    to = ((y + shift) % 4, c, z)
                else:
                    to = (y, c, (z + shift) % 4)
                pairs.append(((y * 2 + c) * 4 + z, (to[0] * 2 + to[1]) * 4 + to[2]))
    return lax.ppermute(value, ("y", "c", "z"), pairs)


def along_x(value, shift):
    return lax.ppermute(value, "x", [(i, (i + shift) % 4) for i in range(4)])


def other_core(value):
    return lax.ppermute(value, "c", [(0, 1), (1, 0)])


def everyone(value, move):
    got = {0: value}
    for d in OFFSETS:
        got[d] = move(value, d)
    return [got[d] for d in range(4)]


NT = (((1,), (1,)), ((), ()))
TN = (((0,), (0,)), ((), ()))


def call(kernel, outs, *args, smem=(), scratch=()):
    return pl.pallas_call(
        kernel,
        out_shape=outs,
        in_specs=[
            pl.BlockSpec(memory_space=pltpu.SMEM if i in smem else pltpu.VMEM) for i in range(len(args))
        ],
        out_specs=jax.tree.map(lambda _: pl.BlockSpec(memory_space=pltpu.VMEM), outs),
        scratch_shapes=scratch,
        compiler_params=pltpu.CompilerParams(vmem_limit_bytes=16 << 20),
    )(*args)


def out(shape, dtype=F32):
    return pltpu.VMEM(shape, dtype)


def hold_kernel(a_ref, b_ref, a_out, b_out, sems):
    copies = [
        pltpu.make_async_copy(ref, o_ref, sems.at[k])
        for k, (ref, o_ref) in enumerate(((a_ref, a_out), (b_ref, b_out)))
    ]
    for copy in copies:
        copy.start()
    for copy in copies:
        copy.wait()


def held(a, b):
    return pl.pallas_call(
        hold_kernel,
        out_shape=(out(a.shape, BF16), out(b.shape, BF16)),
        in_specs=[pl.BlockSpec(memory_space=pl.ANY)] * 2,
        out_specs=(pl.BlockSpec(memory_space=pltpu.VMEM),) * 2,
        scratch_shapes=[pltpu.SemaphoreType.DMA((2,))],
        name="hold",
    )(a, b)


def join_kernel(a0, a1, a2, a3, o_ref):
    for k, a in enumerate((a0, a1, a2, a3)):
        o_ref[128 * k : 128 * (k + 1), :] = a[...]


def joined(values):
    return call(join_kernel, out((512, 512), BF16), *values)


def places():
    y, z, on_y = lax.axis_index("y"), lax.axis_index("z"), lax.axis_index("c") == 0
    return jnp.where(on_y, y, z), jnp.where(on_y, z, y), lax.axis_index("x")


def peak(ref):
    tall = jnp.max(jnp.abs(ref[...].astype(F32)), axis=0, keepdims=True)
    return jnp.broadcast_to(jnp.max(tall, axis=1, keepdims=True), (1, 128))


def logits_into(l_ref, s2, im_ref, t_refs):
    for h, t_ref in enumerate(t_refs):
        l_ref[:, 512 * h : 512 * (h + 1)] = s2 * lax.dot_general(
            im_ref[...], t_ref[...], NT, preferred_element_type=F32
        )


def logits_kernel(first, s_ref, im_ref, t0_ref, t1_ref, rows_ref, cols_ref, l_ref, top_scr, sum_scr, mean_scr):
    s2 = s_ref[0, 0]
    logits_into(l_ref, s2, im_ref, (t0_ref, t1_ref))

    def tops(i, col_tops):
        here = pl.ds(pl.multiple_of(i * 64, 64), 64)
        row_top, new = None, []
        for k in range(8):
            part = l_ref[here, 128 * k : 128 * (k + 1)]
            row_top = part if row_top is None else jnp.maximum(row_top, part)
            new.append(jnp.maximum(col_tops[k], jnp.max(part.reshape(8, 8, 128), axis=0)))
        top_scr[here, :] = row_top
        return tuple(new)

    col_tops = lax.fori_loop(
        0, 8, tops, tuple(l_ref[0:8, 128 * k : 128 * (k + 1)] for k in range(8)), unroll=True
    )

    def sums(i, carry):
        here = pl.ds(pl.multiple_of(i * 64, 64), 64)
        row_top = top_scr[here, :]
        row_sum = row_mean = jnp.zeros((64, 128), F32)
        new = []
        for k in range(8):
            part = l_ref[here, 128 * k : 128 * (k + 1)]
            e = jnp.exp2(part - row_top)
            row_sum = row_sum + e
            row_mean = row_mean + e * part
            part = part.reshape(8, 8, 128)
            e = jnp.exp2(part - col_tops[k][None])
            new.append((carry[k][0] + jnp.sum(e, axis=0), carry[k][1] + jnp.sum(e * part, axis=0)))
        sum_scr[here, :] = row_sum
        mean_scr[here, :] = row_mean
        return tuple(new)

    zero = jnp.zeros((8, 128), F32)
    col_sums = lax.fori_loop(0, 8, sums, ((zero, zero),) * 8, unroll=True)
    for k in range(8):
        at = slice(128 * k, 128 * (k + 1))
        top = jnp.max(col_tops[k], axis=0, keepdims=True)
        e = jnp.exp2(col_tops[k] - top)
        cols_ref[0:1, at] = top
        cols_ref[1:2, at] = jnp.sum(e * col_sums[k][0], axis=0, keepdims=True)
        cols_ref[2:3, at] = jnp.sum(e * col_sums[k][1], axis=0, keepdims=True)
    for j in range(4):
        at = slice(128 * j, 128 * (j + 1))
        tops_here = top_scr[at, :].T
        top = jnp.max(tops_here, axis=0, keepdims=True)
        e = jnp.exp2(tops_here - top)
        total = jnp.sum(e * sum_scr[at, :].T, axis=0, keepdims=True)
        rows_ref[j : j + 1, :] = top + jnp.log2(total)
        rows_ref[4 + j : 5 + j, :] = jnp.sum(e * mean_scr[at, :].T, axis=0, keepdims=True) / total
    rows_ref[8:9, :] = peak(im_ref)
    if first:
        rows_ref[9:10, :] = jnp.maximum(peak(t0_ref), peak(t1_ref))
        block = l_ref[0:128, 0:128]
        rows_ref[10:11, :] = jnp.sum(jnp.where(eye(), block, 0.0), axis=0, keepdims=True)


def eye():
    shape = (128, 128)
    return lax.broadcasted_iota(jnp.int32, shape, 0) == lax.broadcasted_iota(jnp.int32, shape, 1)


def logits_of(k, s2, im, t0, t1):
    return call(
        functools.partial(logits_kernel, k == 0),
        (out((16, 128)), out((8, 1024))),
        s2, im, t0, t1,
        smem=(0,),
        scratch=[pltpu.VMEM((512, 1024), F32)] + [pltpu.VMEM((512, 128), F32)] * 3,
    )


def merge(parts):
    top = functools.reduce(jnp.maximum, [p[0] for p in parts])
    es = [jnp.exp2(p[0] - top) for p in parts]
    total = sum(es)
    mean = sum(e * p[1] for e, p in zip(es, parts)) / total
    return top + jnp.log2(total), mean


def greatest(values):
    return functools.reduce(jnp.maximum, values)


def row_at(back_second, back_first):
    first, second, _ = places()
    return lax.rem(second - back_second + 4, 4) * 4 + lax.rem(first - back_first + 4, 4)


def row_kernel(r0, r1, r2, r3, all_ref, scr):
    for k, r in enumerate((r0, r1, r2, r3)):
        for j in range(4):
            at = row_at(k, j)
            scr[pl.ds(at, 1), :] = r[j : j + 1, :]
            scr[pl.ds(16 + at, 1), :] = r[4 + j : 5 + j, :]
    scr[32:33, :] = r0[10:11, :]
    scr[33:34, :] = r0[9:10, :]
    scr[34:40, :] = jnp.zeros((6, 128), F32)
    message = scr[...]
    for k in range(16):
        all_ref[40 * k : 40 * (k + 1), :] = message


def col_kernel(r0, r1, r2, r3, c0, c1, c2, c3, col_ref):
    rs, cs = (r0, r1, r2, r3), (c0, c1, c2, c3)
    top = greatest([c[0:1, :] for c in cs])
    es = [jnp.exp2(c[0:1, :] - top) for c in cs]
    total = sum(e * c[1:2, :] for e, c in zip(es, cs))
    mean = sum(e * c[2:3, :] for e, c in zip(es, cs)) / total
    lse = top + jnp.log2(total)
    for k in range(8):
        col_ref[k : k + 1, :] = lse[:, 128 * k : 128 * (k + 1)]
        col_ref[8 + k : 9 + k, :] = mean[:, 128 * k : 128 * (k + 1)]
    col_ref[16:17, :] = greatest([r[8:9, :] for r in rs])
    col_ref[17:24, :] = jnp.zeros((7, 128), F32)


def rolled(v, d, group):
    if d == 0:
        return v
    n = v.shape[0]
    size = n // group
    quarter = size // 4
    pieces = []
    for g in range(group):
        at = g * size
        pieces += [v[at + size - d * quarter : at + size, :], v[at : at + size - d * quarter, :]]
    return jnp.concatenate(pieces, axis=0)


def middle_kernel(b0, b1, b2, b3, col_ref):
    cs = (b0, b1, b2, b3)
    lse, mean = merge([(rolled(c[0:8, :], d, 2), rolled(c[8:16, :], d, 2)) for d, c in enumerate(cs)])
    col_ref[0:8, :] = lse
    col_ref[8:16, :] = mean
    col_ref[16:24, :] = greatest([c[16:24, :] for c in cs])


def pieces_of(value):
    left, pieces = value * DOWN, []
    for _ in range(4):
        head = left.astype(BF16).astype(F32)
        head = jnp.where(jnp.abs(head) < TINY, 0.0, head)
        pieces.append(head)
        left = (left - head) * STEP
    return pieces


def value_of(pieces):
    total = pieces[3]
    for p in (pieces[2], pieces[1], pieces[0]):
        total = p + total * (1.0 / STEP)
    return total * (1.0 / DOWN)


def encoded(first, second):
    lane = lax.broadcasted_iota(jnp.int32, (1, 512), 1) % 256
    value = jnp.where(lane % 64 < 32, first, second)
    row = jnp.zeros((1, 512), F32)
    for p, piece in enumerate(pieces_of(value)):
        row = jnp.where(lane // 64 == p, piece, row)
    return row


def tail(row, at, half):
    shape = (8, 512)
    here = lax.broadcasted_iota(jnp.int32, shape, 0) == at
    if half is not None:
        here = here & (lax.broadcasted_iota(jnp.int32, shape, 1) // 256 == half)
    return jnp.where(here, jnp.broadcast_to(row, shape), 0.0)


def total_of(v):
    return jnp.sum(jnp.sum(v, axis=0, keepdims=True), axis=1, keepdims=True)


def end_kernel(s_ref, a_ref, b0, b1, row_ref, col_ref, codes_ref, unit_ref, back_ref, scr):
    rs = [a_ref[40 * k : 40 * (k + 1), :] for k in range(16)]
    lse, mean = merge([(r[0:16, :], r[16:32, :]) for r in rs])
    scr[...] = lse + 1.0
    for k in range(4):
        for j in range(4):
            row_ref[4 * k + j : 4 * k + j + 1, :] = scr[pl.ds(row_at(k, j), 1), :]
    diagonal = total_of(sum(r[32:33, :] for r in rs)) * LN2
    text_peak = greatest([r[33:34, :] for r in rs])
    codes_ref[1:2, :] = encoded(total_of(lse) * LN2 - 2.0 * diagonal, 0.5 * LN2 * total_of(mean) - diagonal)
    swapped = [jnp.concatenate([b1[k + 4 : k + 8, :], b1[k : k + 4, :]], axis=0) for k in (0, 8)]
    lse, mean = merge([(b0[0:8, :], b0[8:16, :]), swapped])
    for k in range(8):
        col_ref[:, 128 * k : 128 * (k + 1)] = lse[k : k + 1, :] + 1.0
    image_peak = jnp.maximum(b0[16:17, :], b1[16:17, :])
    codes_ref[0:1, :] = encoded(total_of(lse) * LN2, 0.5 * LN2 * total_of(mean))
    scale = s_ref[0, 0] * LN2
    for k, top in enumerate((text_peak, image_peak)):
        unit = 4.0 / jnp.maximum(top, 1e-30)
        unit_ref[k : k + 1, :] = unit
        back = scale / unit
        back_ref[k : k + 1, :] = jnp.concatenate([back] * 4, axis=1)


def image_kernel(which, s_ref, im_ref, row_ref, col_ref, unit_ref, codes_ref, t0_ref, t1_ref, w_ref, g_ref, l_ref):
    logits_into(l_ref, s_ref[0, 0], im_ref, (t0_ref, t1_ref))
    for j in range(4):
        at = slice(128 * j, 128 * (j + 1))
        row = row_ref[4 * which + j : 4 * which + j + 1, :]
        row = jnp.broadcast_to(row, (128, 128)).T
        for k in range(8):
            to = slice(128 * k, 128 * (k + 1))
            part = l_ref[at, to]
            w = jnp.exp2(part - row) + jnp.exp2(part - col_ref[:, to])
            if which == 0 and j == 0 and k == 0:
                w = w - jnp.where(eye(), 1.0, 0.0)
            w_ref[at, to] = w.astype(BF16)
    g = jnp.dot(w_ref[:, 0:512], t0_ref[...], preferred_element_type=F32)
    g = g + jnp.dot(w_ref[:, 512:1024], t1_ref[...], preferred_element_type=F32)
    g = g * unit_ref[0:1, 0:1]
    for k in range(4):
        g_ref[136 * k : 136 * k + 128, :] = g[128 * k : 128 * (k + 1), :]
        g_ref[136 * k + 128 : 136 * (k + 1), :] = tail(codes_ref[0:1, :], 4 * (k % 2) + which, k // 2)


def text_kernel(h, w0, w1, w2, w3, i0, i1, i2, i3, unit_ref, codes_ref, g_ref):
    at = slice(512 * h, 512 * (h + 1))
    g = None
    for w, i in zip((w0, w1, w2, w3), (i0, i1, i2, i3)):
        part = lax.dot_general(w[:, at], i[...], TN, preferred_element_type=F32)
        g = part if g is None else g + part
    g = g * unit_ref[1:2, 0:1]
    for k in range(4):
        g_ref[136 * k : 136 * k + 128, :] = g[128 * k : 128 * (k + 1), :]
        g_ref[136 * k + 128 : 136 * (k + 1), :] = tail(codes_ref[1:2, :], 2 * k + h, 0)


def texts_end_kernel(g_ref, back_ref, o_ref, tail_ref):
    o_ref[...] = (g_ref[0:128, :] * back_ref[1:2, :]).astype(BF16)
    tail_ref[...] = g_ref[128:136, :]


def images_end_kernel(g_ref, t_ref, back_ref, o_ref, loss_ref, grad_ref):
    o_ref[...] = (g_ref[0:128, :] * back_ref[0:1, :]).astype(BF16)
    rows = jnp.sum(g_ref[128:136, :] + t_ref[...], axis=0, keepdims=True)
    rows = rows[:, 0:256] + rows[:, 256:512]
    pair_total = ROWS * 128
    for v, (ref, count) in enumerate(((loss_ref, 2.0 * pair_total), (grad_ref, float(pair_total)))):
        ref[...] = value_of([rows[:, 64 * p + 32 * v : 64 * p + 32 * v + 1] for p in range(4)]) / count


def group(value, k):
    return value[136 * k : 136 * (k + 1)]


def program(images, texts, log_scale):
    s2 = jnp.reshape(jnp.exp(log_scale) * LOG2E, (1, 1))
    own_images, own_texts = held(images, texts)
    line = [own_images] + everyone(images, lambda v, d: turn(v, d, True))[1:]
    line = joined(line)
    chunks = everyone(line, lambda v, d: turn(v, d, False))
    t0 = [own_texts] + everyone(texts, along_x)[1:]
    t0 = joined(t0)
    t1 = other_core(t0)
    parts = [None] * 4
    for k in (0, 1, 3, 2):
        parts[k] = logits_of(k, s2, chunks[k], t0, t1)
    cols = call(col_kernel, out((24, 128)), *[p[0] for p in parts], *[p[1] for p in parts])
    rows = call(
        row_kernel, jax.ShapeDtypeStruct((640, 128), F32), *[p[0] for p in parts], scratch=[pltpu.VMEM((40, 128), F32)]
    )
    cols = everyone(cols, along_x)
    rows = lax.all_to_all(rows.reshape(16, 40, 128), ("y", "z"), 0, 0, tiled=True).reshape(640, 128)
    cols = call(middle_kernel, out((24, 128)), *cols)
    cols = [cols, other_core(cols)]
    row_lse, col_lse, codes, unit, back = call(
        end_kernel,
        (out((16, 128)), out((1, 1024)), out((2, 512)), out((2, 128)), out((2, 512))),
        s2, rows, *cols,
        smem=(0,),
        scratch=[pltpu.VMEM((16, 128), F32)],
    )
    ws, gs, sent = {}, {}, {}
    for k in (2, 1, 3, 0):
        ws[k], gs[k] = call(
            functools.partial(image_kernel, k),
            (out((512, 1024), BF16), out((544, 512))),
            s2, chunks[k], row_lse, col_lse, unit, codes, t0, t1,
            smem=(0,),
            scratch=[pltpu.VMEM((512, 1024), F32)],
        )
        if k:
            sent[k] = turn(gs[k].astype(F16), 4 - k, False)
    g0, g1 = [
        call(
            functools.partial(text_kernel, h),
            out((544, 512)),
            *[ws[k] for k in range(4)], *chunks, unit, codes,
        )
        for h in range(2)
    ]
    swap = other_core(g1.astype(F16))
    moved = []
    for k in (2, 1, 3):
        moved.append(along_x((group(g0, k) + group(swap, k).astype(F32)).astype(F16), 4 - k))
    gt = group(g0, 0) + sum(m.astype(F32) for m in [group(swap, 0)] + moved)
    sums = [group(gs[0], k) + sum(group(m, k).astype(F32) for m in sent.values()) for k in range(4)]
    moved = []
    for k in (2, 1, 3):
        moved.append(turn(sums[k].astype(F16), 4 - k, True))
    gi = sums[0] + sum(m.astype(F32) for m in moved)
    grad_texts, gt_tail = call(
        texts_end_kernel,
        (jax.ShapeDtypeStruct((ROWS, 512), BF16), out((8, 512))),
        gt, back,
    )
    grad_images, loss, grad_scale = call(
        images_end_kernel,
        (jax.ShapeDtypeStruct((ROWS, 512), BF16),) + (jax.ShapeDtypeStruct((1, 1), F32),) * 2,
        gi, gt_tail, back,
    )
    return grad_images, grad_texts, jnp.reshape(loss, ()), jnp.reshape(grad_scale, ())


def solution(mesh):
    split = Mesh(mesh.devices.reshape(4, 4, 2, mesh.shape["group"]), ALL)
    placed = (P(ALL, None), P(ALL, None), P())
    return jax.shard_map(
        program,
        mesh=split,
        in_specs=placed,
        out_specs=(P(ALL, None), P(ALL, None), P(), P()),
        check_vma=False,
    )
```

```python
import functools

import jax
import jax.numpy as jnp
from jax import lax
from jax.experimental import pallas as pl
from jax.experimental.pallas import tpu as pltpu
from jax.sharding import Mesh
from jax.sharding import PartitionSpec as P


ALL = ("x", "y", "c", "z")
F32, BF16, F16 = jnp.float32, jnp.bfloat16, jnp.float16
LOG2E = 1.4426950408889634
LN2 = 0.6931471805599453
OFFSETS = (1, 3, 2)
ROWS = 128
DOWN = 2.0**-11
STEP = 2.0**8
TINY = 6.2e-5


def turn(value, shift, first):
    pairs = []
    for y in range(4):
        for c in range(2):
            for z in range(4):
                if (c == 0) == first:
                    to = ((y + shift) % 4, c, z)
                else:
                    to = (y, c, (z + shift) % 4)
                pairs.append(((y * 2 + c) * 4 + z, (to[0] * 2 + to[1]) * 4 + to[2]))
    return lax.ppermute(value, ("y", "c", "z"), pairs)


def along_x(value, shift):
    return lax.ppermute(value, "x", [(i, (i + shift) % 4) for i in range(4)])


def other_core(value):
    return lax.ppermute(value, "c", [(0, 1), (1, 0)])


def everyone(value, move):
    got = {0: value}
    for d in OFFSETS:
        got[d] = move(value, d)
    return [got[d] for d in range(4)]


NT = (((1,), (1,)), ((), ()))
TN = (((0,), (0,)), ((), ()))


def call(kernel, outs, *args, smem=(), scratch=()):
    return pl.pallas_call(
        kernel,
        out_shape=outs,
        in_specs=[
            pl.BlockSpec(memory_space=pltpu.SMEM if i in smem else pltpu.VMEM) for i in range(len(args))
        ],
        out_specs=jax.tree.map(lambda _: pl.BlockSpec(memory_space=pltpu.VMEM), outs),
        scratch_shapes=scratch,
        compiler_params=pltpu.CompilerParams(vmem_limit_bytes=16 << 20),
    )(*args)


def out(shape, dtype=F32):
    return pltpu.VMEM(shape, dtype)


def hold_kernel(a_ref, o_ref):
    o_ref[...] = a_ref[...]


def held(value):
    return call(hold_kernel, out((ROWS, 512), BF16), value)


def join_kernel(a0, a1, a2, a3, o_ref):
    for k, a in enumerate((a0, a1, a2, a3)):
        o_ref[128 * k : 128 * (k + 1), :] = a[...]


def joined(values):
    return call(join_kernel, out((512, 512), BF16), *values)


def places():
    y, z, on_y = lax.axis_index("y"), lax.axis_index("z"), lax.axis_index("c") == 0
    return jnp.where(on_y, y, z), jnp.where(on_y, z, y), lax.axis_index("x")


def peak(ref):
    tall = jnp.max(jnp.abs(ref[...].astype(F32)), axis=0, keepdims=True)
    return jnp.broadcast_to(jnp.max(tall, axis=1, keepdims=True), (1, 128))


def logits_into(l_ref, s2, im_ref, t_refs):
    for h, t_ref in enumerate(t_refs):
        l_ref[:, 512 * h : 512 * (h + 1)] = s2 * lax.dot_general(
            im_ref[...], t_ref[...], NT, preferred_element_type=F32
        )


def logits_kernel(k, *refs):
    first, keep = k == 0, k != 2
    s_ref, im_ref, t0_ref, t1_ref, rows_ref, cols_ref = refs[:6]
    l_ref, top_scr, sum_scr, mean_scr = refs[7:11] if keep else refs[6:10]
    logits_into(l_ref, s_ref[0, 0], im_ref, (t0_ref, t1_ref))
    if keep:
        copy = pltpu.make_async_copy(l_ref, refs[6], refs[11])
        copy.start()

    def tops(i, col_tops):
        here = pl.ds(pl.multiple_of(i * 64, 64), 64)
        row_top, new = None, []
        for k in range(8):
            part = l_ref[here, 128 * k : 128 * (k + 1)]
            row_top = part if row_top is None else jnp.maximum(row_top, part)
            new.append(jnp.maximum(col_tops[k], jnp.max(part.reshape(8, 8, 128), axis=0)))
        top_scr[here, :] = row_top
        return tuple(new)

    col_tops = lax.fori_loop(
        0, 8, tops, tuple(l_ref[0:8, 128 * k : 128 * (k + 1)] for k in range(8)), unroll=True
    )

    def sums(i, carry):
        here = pl.ds(pl.multiple_of(i * 64, 64), 64)
        row_top = top_scr[here, :]
        row_sum = row_mean = jnp.zeros((64, 128), F32)
        new = []
        for k in range(8):
            part = l_ref[here, 128 * k : 128 * (k + 1)]
            e = jnp.exp2(part - row_top)
            row_sum = row_sum + e
            row_mean = row_mean + e * part
            part = part.reshape(8, 8, 128)
            e = jnp.exp2(part - col_tops[k][None])
            new.append((carry[k][0] + jnp.sum(e, axis=0), carry[k][1] + jnp.sum(e * part, axis=0)))
        sum_scr[here, :] = row_sum
        mean_scr[here, :] = row_mean
        return tuple(new)

    zero = jnp.zeros((8, 128), F32)
    col_sums = lax.fori_loop(0, 8, sums, ((zero, zero),) * 8, unroll=True)
    for k in range(8):
        at = slice(128 * k, 128 * (k + 1))
        top = jnp.max(col_tops[k], axis=0, keepdims=True)
        e = jnp.exp2(col_tops[k] - top)
        cols_ref[0:1, at] = top
        cols_ref[1:2, at] = jnp.sum(e * col_sums[k][0], axis=0, keepdims=True)
        cols_ref[2:3, at] = jnp.sum(e * col_sums[k][1], axis=0, keepdims=True)
    for j in range(4):
        at = slice(128 * j, 128 * (j + 1))
        tops_here = top_scr[at, :].T
        top = jnp.max(tops_here, axis=0, keepdims=True)
        e = jnp.exp2(tops_here - top)
        total = jnp.sum(e * sum_scr[at, :].T, axis=0, keepdims=True)
        rows_ref[j : j + 1, :] = top + jnp.log2(total)
        rows_ref[4 + j : 5 + j, :] = jnp.sum(e * mean_scr[at, :].T, axis=0, keepdims=True) / total
    rows_ref[8:9, :] = peak(im_ref)
    if first:
        rows_ref[9:10, :] = jnp.maximum(peak(t0_ref), peak(t1_ref))
        block = l_ref[0:128, 0:128]
        rows_ref[10:11, :] = jnp.sum(jnp.where(eye(), block, 0.0), axis=0, keepdims=True)
    if keep:
        copy.wait()


def eye():
    shape = (128, 128)
    return lax.broadcasted_iota(jnp.int32, shape, 0) == lax.broadcasted_iota(jnp.int32, shape, 1)


def logits_of(k, s2, im, t0, t1):
    keep = k != 2
    vmem = pl.BlockSpec(memory_space=pltpu.VMEM)
    got = pl.pallas_call(
        functools.partial(logits_kernel, k),
        out_shape=(out((16, 128)), out((8, 1024))) + ((pltpu.HBM((512, 1024), F32),) if keep else ()),
        in_specs=[pl.BlockSpec(memory_space=pltpu.SMEM)] + [vmem] * 3,
        out_specs=(vmem, vmem) + ((pl.BlockSpec(memory_space=pltpu.HBM),) if keep else ()),
        scratch_shapes=[pltpu.VMEM((512, 1024), F32)]
        + [pltpu.VMEM((512, 128), F32)] * 3
        + ([pltpu.SemaphoreType.DMA] if keep else []),
        compiler_params=pltpu.CompilerParams(vmem_limit_bytes=16 << 20),
        name="logits",
    )(s2, im, t0, t1)
    return got if keep else (*got, im)


def merge(parts):
    top = functools.reduce(jnp.maximum, [p[0] for p in parts])
    es = [jnp.exp2(p[0] - top) for p in parts]
    total = sum(es)
    mean = sum(e * p[1] for e, p in zip(es, parts)) / total
    return top + jnp.log2(total), mean


def greatest(values):
    return functools.reduce(jnp.maximum, values)


def row_at(back_second, back_first):
    first, second, _ = places()
    return lax.rem(second - back_second + 4, 4) * 4 + lax.rem(first - back_first + 4, 4)


def row_kernel(r0, r1, r2, r3, all_ref, scr):
    for k, r in enumerate((r0, r1, r2, r3)):
        for j in range(4):
            at = row_at(k, j)
            scr[pl.ds(at, 1), :] = r[j : j + 1, :]
            scr[pl.ds(16 + at, 1), :] = r[4 + j : 5 + j, :]
    scr[32:33, :] = r0[10:11, :]
    scr[33:34, :] = r0[9:10, :]
    scr[34:40, :] = jnp.zeros((6, 128), F32)
    message = scr[...]
    for k in range(16):
        all_ref[40 * k : 40 * (k + 1), :] = message


def col_kernel(r0, r1, r2, r3, c0, c1, c2, c3, col_ref):
    rs, cs = (r0, r1, r2, r3), (c0, c1, c2, c3)
    top = greatest([c[0:1, :] for c in cs])
    es = [jnp.exp2(c[0:1, :] - top) for c in cs]
    total = sum(e * c[1:2, :] for e, c in zip(es, cs))
    mean = sum(e * c[2:3, :] for e, c in zip(es, cs)) / total
    lse = top + jnp.log2(total)
    for k in range(8):
        col_ref[k : k + 1, :] = lse[:, 128 * k : 128 * (k + 1)]
        col_ref[8 + k : 9 + k, :] = mean[:, 128 * k : 128 * (k + 1)]
    col_ref[16:17, :] = greatest([r[8:9, :] for r in rs])
    col_ref[17:24, :] = jnp.zeros((7, 128), F32)


def rolled(v, d, group):
    if d == 0:
        return v
    n = v.shape[0]
    size = n // group
    quarter = size // 4
    pieces = []
    for g in range(group):
        at = g * size
        pieces += [v[at + size - d * quarter : at + size, :], v[at : at + size - d * quarter, :]]
    return jnp.concatenate(pieces, axis=0)


def middle_kernel(b0, b1, b2, b3, col_ref):
    cs = (b0, b1, b2, b3)
    lse, mean = merge([(rolled(c[0:8, :], d, 2), rolled(c[8:16, :], d, 2)) for d, c in enumerate(cs)])
    col_ref[0:8, :] = lse
    col_ref[8:16, :] = mean
    col_ref[16:24, :] = greatest([c[16:24, :] for c in cs])


def pieces_of(value):
    left, pieces = value * DOWN, []
    for _ in range(4):
        head = left.astype(BF16).astype(F32)
        head = jnp.where(jnp.abs(head) < TINY, 0.0, head)
        pieces.append(head)
        left = (left - head) * STEP
    return pieces


def value_of(pieces):
    total = pieces[3]
    for p in (pieces[2], pieces[1], pieces[0]):
        total = p + total * (1.0 / STEP)
    return total * (1.0 / DOWN)


def encoded(first, second):
    lane = lax.broadcasted_iota(jnp.int32, (1, 512), 1) % 256
    value = jnp.where(lane % 64 < 32, first, second)
    row = jnp.zeros((1, 512), F32)
    for p, piece in enumerate(pieces_of(value)):
        row = jnp.where(lane // 64 == p, piece, row)
    return row


def tail(row, at, half):
    shape = (8, 512)
    here = lax.broadcasted_iota(jnp.int32, shape, 0) == at
    if half is not None:
        here = here & (lax.broadcasted_iota(jnp.int32, shape, 1) // 256 == half)
    return jnp.where(here, jnp.broadcast_to(row, shape), 0.0)


def total_of(v):
    return jnp.sum(jnp.sum(v, axis=0, keepdims=True), axis=1, keepdims=True)


def end_kernel(s_ref, a_ref, b0, b1, row_ref, col_ref, codes_ref, unit_ref, back_ref, scr):
    rs = [a_ref[40 * k : 40 * (k + 1), :] for k in range(16)]
    lse, mean = merge([(r[0:16, :], r[16:32, :]) for r in rs])
    scr[...] = lse + 1.0
    for k in range(4):
        for j in range(4):
            row_ref[4 * k + j : 4 * k + j + 1, :] = scr[pl.ds(row_at(k, j), 1), :]
    diagonal = total_of(sum(r[32:33, :] for r in rs)) * LN2
    text_peak = greatest([r[33:34, :] for r in rs])
    codes_ref[1:2, :] = encoded(total_of(lse) * LN2 - 2.0 * diagonal, 0.5 * LN2 * total_of(mean) - diagonal)
    swapped = [jnp.concatenate([b1[k + 4 : k + 8, :], b1[k : k + 4, :]], axis=0) for k in (0, 8)]
    lse, mean = merge([(b0[0:8, :], b0[8:16, :]), swapped])
    for k in range(8):
        col_ref[:, 128 * k : 128 * (k + 1)] = lse[k : k + 1, :] + 1.0
    image_peak = jnp.maximum(b0[16:17, :], b1[16:17, :])
    codes_ref[0:1, :] = encoded(total_of(lse) * LN2, 0.5 * LN2 * total_of(mean))
    scale = s_ref[0, 0] * LN2
    for k, top in enumerate((text_peak, image_peak)):
        unit = 4.0 / jnp.maximum(top, 1e-30)
        unit_ref[k : k + 1, :] = unit
        back = scale / unit
        back_ref[k : k + 1, :] = jnp.concatenate([back] * 4, axis=1)


def image_kernel(which, s_ref, l_ref, row_ref, col_ref, unit_ref, codes_ref, t0_ref, t1_ref, w_ref, g_ref, *scr):
    if scr:
        logits_into(scr[0], s_ref[0, 0], l_ref, (t0_ref, t1_ref))
        l_ref = scr[0]
    for j in range(4):
        at = slice(128 * j, 128 * (j + 1))
        row = row_ref[4 * which + j : 4 * which + j + 1, :]
        row = jnp.broadcast_to(row, (128, 128)).T
        for k in range(8):
            to = slice(128 * k, 128 * (k + 1))
            part = l_ref[at, to]
            w = jnp.exp2(part - row) + jnp.exp2(part - col_ref[:, to])
            if which == 0 and j == 0 and k == 0:
                w = w - jnp.where(eye(), 1.0, 0.0)
            w_ref[at, to] = w.astype(BF16)
    g = jnp.dot(w_ref[:, 0:512], t0_ref[...], preferred_element_type=F32)
    g = g + jnp.dot(w_ref[:, 512:1024], t1_ref[...], preferred_element_type=F32)
    g = g * unit_ref[0:1, 0:1]
    for k in range(4):
        g_ref[136 * k : 136 * k + 128, :] = g[128 * k : 128 * (k + 1), :]
        g_ref[136 * k + 128 : 136 * (k + 1), :] = tail(codes_ref[0:1, :], 4 * (k % 2) + which, k // 2)


def text_kernel(h, w0, w1, w2, w3, i0, i1, i2, i3, unit_ref, codes_ref, g_ref):
    at = slice(512 * h, 512 * (h + 1))
    g = None
    for w, i in zip((w0, w1, w2, w3), (i0, i1, i2, i3)):
        part = lax.dot_general(w[:, at], i[...], TN, preferred_element_type=F32)
        g = part if g is None else g + part
    g = g * unit_ref[1:2, 0:1]
    for k in range(4):
        g_ref[136 * k : 136 * k + 128, :] = g[128 * k : 128 * (k + 1), :]
        g_ref[136 * k + 128 : 136 * (k + 1), :] = tail(codes_ref[1:2, :], 2 * k + h, 0)


def texts_end_kernel(g_ref, back_ref, o_ref, tail_ref):
    o_ref[...] = (g_ref[0:128, :] * back_ref[1:2, :]).astype(BF16)
    tail_ref[...] = g_ref[128:136, :]


def images_end_kernel(g_ref, t_ref, back_ref, o_ref, loss_ref, grad_ref):
    o_ref[...] = (g_ref[0:128, :] * back_ref[0:1, :]).astype(BF16)
    rows = jnp.sum(g_ref[128:136, :] + t_ref[...], axis=0, keepdims=True)
    rows = rows[:, 0:256] + rows[:, 256:512]
    pair_total = ROWS * 128
    for v, (ref, count) in enumerate(((loss_ref, 2.0 * pair_total), (grad_ref, float(pair_total)))):
        ref[...] = value_of([rows[:, 64 * p + 32 * v : 64 * p + 32 * v + 1] for p in range(4)]) / count


def group(value, k):
    return value[136 * k : 136 * (k + 1)]


def program(images, texts, log_scale):
    s2 = jnp.reshape(jnp.exp(log_scale) * LOG2E, (1, 1))
    line = [held(images)] + everyone(images, lambda v, d: turn(v, d, True))[1:]
    line = joined(line)
    chunks = everyone(line, lambda v, d: turn(v, d, False))
    t0 = [held(texts)] + everyone(texts, along_x)[1:]
    t0 = joined(t0)
    t1 = other_core(t0)
    parts = [None] * 4
    for k in (0, 1, 3, 2):
        parts[k] = logits_of(k, s2, chunks[k], t0, t1)
    cols = call(col_kernel, out((24, 128)), *[p[0] for p in parts], *[p[1] for p in parts])
    rows = call(
        row_kernel, jax.ShapeDtypeStruct((640, 128), F32), *[p[0] for p in parts], scratch=[pltpu.VMEM((40, 128), F32)]
    )
    cols = everyone(cols, along_x)
    rows = lax.all_to_all(rows.reshape(16, 40, 128), ("y", "z"), 0, 0, tiled=True).reshape(640, 128)
    cols = call(middle_kernel, out((24, 128)), *cols)
    cols = [cols, other_core(cols)]
    row_lse, col_lse, codes, unit, back = call(
        end_kernel,
        (out((16, 128)), out((1, 1024)), out((2, 512)), out((2, 128)), out((2, 512))),
        s2, rows, *cols,
        smem=(0,),
        scratch=[pltpu.VMEM((16, 128), F32)],
    )
    ws, gs, sent = {}, {}, {}
    for k in (2, 1, 3, 0):
        ws[k], gs[k] = call(
            functools.partial(image_kernel, k),
            (out((512, 1024), BF16), out((544, 512))),
            s2, chunks[k] if k == 2 else pltpu.with_memory_space_constraint(parts[k][2], pltpu.VMEM),
            row_lse, col_lse, unit, codes, t0, t1,
            smem=(0,),
            scratch=[pltpu.VMEM((512, 1024), F32)] if k == 2 else (),
        )
        if k:
            sent[k] = turn(gs[k].astype(F16), 4 - k, False)
    g0, g1 = [
        call(
            functools.partial(text_kernel, h),
            out((544, 512)),
            *[ws[k] for k in range(4)], *chunks, unit, codes,
        )
        for h in range(2)
    ]
    swap = other_core(g1.astype(F16))
    moved = []
    for k in (2, 1, 3):
        moved.append(along_x((group(g0, k) + group(swap, k).astype(F32)).astype(F16), 4 - k))
    gt = group(g0, 0) + sum(m.astype(F32) for m in [group(swap, 0)] + moved)
    sums = [group(gs[0], k) + sum(group(m, k).astype(F32) for m in sent.values()) for k in range(4)]
    moved = []
    for k in (2, 1, 3):
        moved.append(turn(sums[k].astype(F16), 4 - k, True))
    gi = sums[0] + sum(m.astype(F32) for m in moved)
    grad_texts, gt_tail = call(
        texts_end_kernel,
        (jax.ShapeDtypeStruct((ROWS, 512), BF16), out((8, 512))),
        gt, back,
    )
    grad_images, loss, grad_scale = call(
        images_end_kernel,
        (jax.ShapeDtypeStruct((ROWS, 512), BF16),) + (jax.ShapeDtypeStruct((1, 1), F32),) * 2,
        gi, gt_tail, back,
    )
    return grad_images, grad_texts, jnp.reshape(loss, ()), jnp.reshape(grad_scale, ())


def solution(mesh):
    split = Mesh(mesh.devices.reshape(4, 4, 2, mesh.shape["group"]), ALL)
    placed = (P(ALL, None), P(ALL, None), P())
    return jax.shard_map(
        program,
        mesh=split,
        in_specs=placed,
        out_specs=(P(ALL, None), P(ALL, None), P(), P()),
        check_vma=False,
    )
```

```python
import functools

import jax
import jax.numpy as jnp
from jax import lax
from jax.experimental import pallas as pl
from jax.experimental.pallas import tpu as pltpu
from jax.sharding import Mesh
from jax.sharding import PartitionSpec as P


ALL = ("x", "y", "c", "z")
F32, BF16, F16 = jnp.float32, jnp.bfloat16, jnp.float16
LOG2E = 1.4426950408889634
LN2 = 0.6931471805599453
OFFSETS = (1, 3, 2)
ROWS = 128
DOWN = 2.0**-11
STEP = 2.0**8
TINY = 6.2e-5


def turn(value, shift, first):
    pairs = []
    for y in range(4):
        for c in range(2):
            for z in range(4):
                if (c == 0) == first:
                    to = ((y + shift) % 4, c, z)
                else:
                    to = (y, c, (z + shift) % 4)
                pairs.append(((y * 2 + c) * 4 + z, (to[0] * 2 + to[1]) * 4 + to[2]))
    return lax.ppermute(value, ("y", "c", "z"), pairs)


def along_x(value, shift):
    return lax.ppermute(value, "x", [(i, (i + shift) % 4) for i in range(4)])


def other_core(value):
    return lax.ppermute(value, "c", [(0, 1), (1, 0)])


def everyone(value, move):
    got = {0: value}
    for d in OFFSETS:
        got[d] = move(value, d)
    return [got[d] for d in range(4)]


NT = (((1,), (1,)), ((), ()))
TN = (((0,), (0,)), ((), ()))


def call(kernel, outs, *args, smem=(), scratch=()):
    return pl.pallas_call(
        kernel,
        out_shape=outs,
        in_specs=[
            pl.BlockSpec(memory_space=pltpu.SMEM if i in smem else pltpu.VMEM) for i in range(len(args))
        ],
        out_specs=jax.tree.map(lambda _: pl.BlockSpec(memory_space=pltpu.VMEM), outs),
        scratch_shapes=scratch,
        compiler_params=pltpu.CompilerParams(vmem_limit_bytes=16 << 20),
    )(*args)


def out(shape, dtype=F32):
    return pltpu.VMEM(shape, dtype)


def hold_kernel(a_ref, b_ref, a_out, b_out, sems):
    copies = [
        pltpu.make_async_copy(ref, o_ref, sems.at[k])
        for k, (ref, o_ref) in enumerate(((a_ref, a_out), (b_ref, b_out)))
    ]
    for copy in copies:
        copy.start()
    for copy in copies:
        copy.wait()


def held(a, b):
    return pl.pallas_call(
        hold_kernel,
        out_shape=(out(a.shape, BF16), out(b.shape, BF16)),
        in_specs=[pl.BlockSpec(memory_space=pl.ANY)] * 2,
        out_specs=(pl.BlockSpec(memory_space=pltpu.VMEM),) * 2,
        scratch_shapes=[pltpu.SemaphoreType.DMA((2,))],
        name="hold",
    )(a, b)


def join_kernel(*refs):
    o_ref, at = refs[-1], 0
    for a in refs[:-1]:
        o_ref[at : at + a.shape[0], :] = a[...]
        at += a.shape[0]


def half_kernel(at, a_ref, o_ref):
    o_ref[...] = a_ref[at : at + 256, :]


def half(value, at):
    return call(functools.partial(half_kernel, at), out((256, 512), BF16), value)


def joined(values):
    return call(join_kernel, out((512, 512), BF16), *values)


def places():
    y, z, on_y = lax.axis_index("y"), lax.axis_index("z"), lax.axis_index("c") == 0
    return jnp.where(on_y, y, z), jnp.where(on_y, z, y), lax.axis_index("x")


def peak(ref):
    tall = jnp.max(jnp.abs(ref[...].astype(F32)), axis=0, keepdims=True)
    return jnp.broadcast_to(jnp.max(tall, axis=1, keepdims=True), (1, 128))


def logits_into(l_ref, s2, im_ref, t_refs):
    for h, t_ref in enumerate(t_refs):
        l_ref[:, 512 * h : 512 * (h + 1)] = s2 * lax.dot_general(
            im_ref[...], t_ref[...], NT, preferred_element_type=F32
        )


def logits_kernel(first, s_ref, im_ref, t0_ref, t1_ref, rows_ref, cols_ref, l_ref, top_scr, sum_scr, mean_scr):
    s2 = s_ref[0, 0]
    logits_into(l_ref, s2, im_ref, (t0_ref, t1_ref))

    def tops(i, col_tops):
        here = pl.ds(pl.multiple_of(i * 64, 64), 64)
        row_top, new = None, []
        for k in range(8):
            part = l_ref[here, 128 * k : 128 * (k + 1)]
            row_top = part if row_top is None else jnp.maximum(row_top, part)
            new.append(jnp.maximum(col_tops[k], jnp.max(part.reshape(8, 8, 128), axis=0)))
        top_scr[here, :] = row_top
        return tuple(new)

    col_tops = lax.fori_loop(
        0, 8, tops, tuple(l_ref[0:8, 128 * k : 128 * (k + 1)] for k in range(8)), unroll=True
    )

    def sums(i, carry):
        here = pl.ds(pl.multiple_of(i * 64, 64), 64)
        row_top = top_scr[here, :]
        row_sum = row_mean = jnp.zeros((64, 128), F32)
        new = []
        for k in range(8):
            part = l_ref[here, 128 * k : 128 * (k + 1)]
            e = jnp.exp2(part - row_top)
            row_sum = row_sum + e
            row_mean = row_mean + e * part
            part = part.reshape(8, 8, 128)
            e = jnp.exp2(part - col_tops[k][None])
            new.append((carry[k][0] + jnp.sum(e, axis=0), carry[k][1] + jnp.sum(e * part, axis=0)))
        sum_scr[here, :] = row_sum
        mean_scr[here, :] = row_mean
        return tuple(new)

    zero = jnp.zeros((8, 128), F32)
    col_sums = lax.fori_loop(0, 8, sums, ((zero, zero),) * 8, unroll=True)
    for k in range(8):
        at = slice(128 * k, 128 * (k + 1))
        top = jnp.max(col_tops[k], axis=0, keepdims=True)
        e = jnp.exp2(col_tops[k] - top)
        cols_ref[0:1, at] = top
        cols_ref[1:2, at] = jnp.sum(e * col_sums[k][0], axis=0, keepdims=True)
        cols_ref[2:3, at] = jnp.sum(e * col_sums[k][1], axis=0, keepdims=True)
    for j in range(4):
        at = slice(128 * j, 128 * (j + 1))
        tops_here = top_scr[at, :].T
        top = jnp.max(tops_here, axis=0, keepdims=True)
        e = jnp.exp2(tops_here - top)
        total = jnp.sum(e * sum_scr[at, :].T, axis=0, keepdims=True)
        rows_ref[j : j + 1, :] = top + jnp.log2(total)
        rows_ref[4 + j : 5 + j, :] = jnp.sum(e * mean_scr[at, :].T, axis=0, keepdims=True) / total
    rows_ref[8:9, :] = peak(im_ref)
    if first:
        rows_ref[9:10, :] = jnp.maximum(peak(t0_ref), peak(t1_ref))
        block = l_ref[0:128, 0:128]
        rows_ref[10:11, :] = jnp.sum(jnp.where(eye(), block, 0.0), axis=0, keepdims=True)


def eye():
    shape = (128, 128)
    return lax.broadcasted_iota(jnp.int32, shape, 0) == lax.broadcasted_iota(jnp.int32, shape, 1)


def logits_of(k, s2, im, t0, t1):
    return call(
        functools.partial(logits_kernel, k == 0),
        (out((16, 128)), out((8, 1024))),
        s2, im, t0, t1,
        smem=(0,),
        scratch=[pltpu.VMEM((512, 1024), F32)] + [pltpu.VMEM((512, 128), F32)] * 3,
    )


def merge(parts):
    top = functools.reduce(jnp.maximum, [p[0] for p in parts])
    es = [jnp.exp2(p[0] - top) for p in parts]
    total = sum(es)
    mean = sum(e * p[1] for e, p in zip(es, parts)) / total
    return top + jnp.log2(total), mean


def greatest(values):
    return functools.reduce(jnp.maximum, values)


def row_at(back_second, back_first):
    first, second, _ = places()
    return lax.rem(second - back_second + 4, 4) * 4 + lax.rem(first - back_first + 4, 4)


def row_kernel(r0, r1, r2, r3, all_ref, scr):
    for k, r in enumerate((r0, r1, r2, r3)):
        for j in range(4):
            at = row_at(k, j)
            scr[pl.ds(at, 1), :] = r[j : j + 1, :]
            scr[pl.ds(16 + at, 1), :] = r[4 + j : 5 + j, :]
    scr[32:33, :] = r0[10:11, :]
    scr[33:34, :] = r0[9:10, :]
    scr[34:40, :] = jnp.zeros((6, 128), F32)
    message = scr[...]
    for k in range(16):
        all_ref[40 * k : 40 * (k + 1), :] = message


def col_kernel(r0, r1, r2, r3, c0, c1, c2, c3, col_ref):
    rs, cs = (r0, r1, r2, r3), (c0, c1, c2, c3)
    top = greatest([c[0:1, :] for c in cs])
    es = [jnp.exp2(c[0:1, :] - top) for c in cs]
    total = sum(e * c[1:2, :] for e, c in zip(es, cs))
    mean = sum(e * c[2:3, :] for e, c in zip(es, cs)) / total
    lse = top + jnp.log2(total)
    for k in range(8):
        col_ref[k : k + 1, :] = lse[:, 128 * k : 128 * (k + 1)]
        col_ref[8 + k : 9 + k, :] = mean[:, 128 * k : 128 * (k + 1)]
    col_ref[16:17, :] = greatest([r[8:9, :] for r in rs])
    col_ref[17:24, :] = jnp.zeros((7, 128), F32)


def rolled(v, d, group):
    if d == 0:
        return v
    n = v.shape[0]
    size = n // group
    quarter = size // 4
    pieces = []
    for g in range(group):
        at = g * size
        pieces += [v[at + size - d * quarter : at + size, :], v[at : at + size - d * quarter, :]]
    return jnp.concatenate(pieces, axis=0)


def middle_kernel(b0, b1, b2, b3, col_ref):
    cs = (b0, b1, b2, b3)
    lse, mean = merge([(rolled(c[0:8, :], d, 2), rolled(c[8:16, :], d, 2)) for d, c in enumerate(cs)])
    col_ref[0:8, :] = lse
    col_ref[8:16, :] = mean
    col_ref[16:24, :] = greatest([c[16:24, :] for c in cs])


def pieces_of(value):
    left, pieces = value * DOWN, []
    for _ in range(4):
        head = left.astype(BF16).astype(F32)
        head = jnp.where(jnp.abs(head) < TINY, 0.0, head)
        pieces.append(head)
        left = (left - head) * STEP
    return pieces


def value_of(pieces):
    total = pieces[3]
    for p in (pieces[2], pieces[1], pieces[0]):
        total = p + total * (1.0 / STEP)
    return total * (1.0 / DOWN)


def encoded(first, second):
    lane = lax.broadcasted_iota(jnp.int32, (1, 512), 1) % 256
    value = jnp.where(lane % 64 < 32, first, second)
    row = jnp.zeros((1, 512), F32)
    for p, piece in enumerate(pieces_of(value)):
        row = jnp.where(lane // 64 == p, piece, row)
    return row


def tail(row, at, half):
    shape = (8, 512)
    here = lax.broadcasted_iota(jnp.int32, shape, 0) == at
    if half is not None:
        here = here & (lax.broadcasted_iota(jnp.int32, shape, 1) // 256 == half)
    return jnp.where(here, jnp.broadcast_to(row, shape), 0.0)


def total_of(v):
    return jnp.sum(jnp.sum(v, axis=0, keepdims=True), axis=1, keepdims=True)


def end_kernel(s_ref, a_ref, b0, b1, row_ref, col_ref, codes_ref, unit_ref, back_ref, scr):
    rs = [a_ref[40 * k : 40 * (k + 1), :] for k in range(16)]
    lse, mean = merge([(r[0:16, :], r[16:32, :]) for r in rs])
    scr[...] = lse + 1.0
    for k in range(4):
        for j in range(4):
            row_ref[4 * k + j : 4 * k + j + 1, :] = scr[pl.ds(row_at(k, j), 1), :]
    diagonal = total_of(sum(r[32:33, :] for r in rs)) * LN2
    text_peak = greatest([r[33:34, :] for r in rs])
    codes_ref[1:2, :] = encoded(total_of(lse) * LN2 - 2.0 * diagonal, 0.5 * LN2 * total_of(mean) - diagonal)
    swapped = [jnp.concatenate([b1[k + 4 : k + 8, :], b1[k : k + 4, :]], axis=0) for k in (0, 8)]
    lse, mean = merge([(b0[0:8, :], b0[8:16, :]), swapped])
    for k in range(8):
        col_ref[:, 128 * k : 128 * (k + 1)] = lse[k : k + 1, :] + 1.0
    image_peak = jnp.maximum(b0[16:17, :], b1[16:17, :])
    codes_ref[0:1, :] = encoded(total_of(lse) * LN2, 0.5 * LN2 * total_of(mean))
    scale = s_ref[0, 0] * LN2
    for k, top in enumerate((text_peak, image_peak)):
        unit = 4.0 / jnp.maximum(top, 1e-30)
        unit_ref[k : k + 1, :] = unit
        back = scale / unit
        back_ref[k : k + 1, :] = jnp.concatenate([back] * 4, axis=1)


def image_kernel(which, s_ref, im_ref, row_ref, col_ref, unit_ref, codes_ref, t0_ref, t1_ref, w_ref, g_ref, l_ref):
    logits_into(l_ref, s_ref[0, 0], im_ref, (t0_ref, t1_ref))
    for j in range(4):
        at = slice(128 * j, 128 * (j + 1))
        row = row_ref[4 * which + j : 4 * which + j + 1, :]
        row = jnp.broadcast_to(row, (128, 128)).T
        for k in range(8):
            to = slice(128 * k, 128 * (k + 1))
            part = l_ref[at, to]
            w = jnp.exp2(part - row) + jnp.exp2(part - col_ref[:, to])
            if which == 0 and j == 0 and k == 0:
                w = w - jnp.where(eye(), 1.0, 0.0)
            w_ref[at, to] = w.astype(BF16)
    g = jnp.dot(w_ref[:, 0:512], t0_ref[...], preferred_element_type=F32)
    g = g + jnp.dot(w_ref[:, 512:1024], t1_ref[...], preferred_element_type=F32)
    g = g * unit_ref[0:1, 0:1]
    for k in range(4):
        g_ref[136 * k : 136 * k + 128, :] = g[128 * k : 128 * (k + 1), :]
        g_ref[136 * k + 128 : 136 * (k + 1), :] = tail(codes_ref[0:1, :], 4 * (k % 2) + which, k // 2)


def text_kernel(h, w0, w1, w2, w3, i0, i1, i2, i3, unit_ref, codes_ref, g_ref):
    at = slice(512 * h, 512 * (h + 1))
    g = None
    for w, i in zip((w0, w1, w2, w3), (i0, i1, i2, i3)):
        part = lax.dot_general(w[:, at], i[...], TN, preferred_element_type=F32)
        g = part if g is None else g + part
    g = g * unit_ref[1:2, 0:1]
    for k in range(4):
        g_ref[136 * k : 136 * k + 128, :] = g[128 * k : 128 * (k + 1), :]
        g_ref[136 * k + 128 : 136 * (k + 1), :] = tail(codes_ref[1:2, :], 2 * k + h, 0)


def texts_end_kernel(g_ref, back_ref, o_ref, tail_ref):
    o_ref[...] = (g_ref[0:128, :] * back_ref[1:2, :]).astype(BF16)
    tail_ref[...] = g_ref[128:136, :]


def images_end_kernel(g_ref, t_ref, back_ref, o_ref, loss_ref, grad_ref):
    o_ref[...] = (g_ref[0:128, :] * back_ref[0:1, :]).astype(BF16)
    rows = jnp.sum(g_ref[128:136, :] + t_ref[...], axis=0, keepdims=True)
    rows = rows[:, 0:256] + rows[:, 256:512]
    pair_total = ROWS * 128
    for v, (ref, count) in enumerate(((loss_ref, 2.0 * pair_total), (grad_ref, float(pair_total)))):
        ref[...] = value_of([rows[:, 64 * p + 32 * v : 64 * p + 32 * v + 1] for p in range(4)]) / count


def group(value, k):
    return value[136 * k : 136 * (k + 1)]


def program(images, texts, log_scale):
    s2 = jnp.reshape(jnp.exp(log_scale) * LOG2E, (1, 1))
    own_images, own_texts = held(images, texts)
    line = [own_images] + everyone(images, lambda v, d: turn(v, d, True))[1:]
    line = joined(line)
    chunks = [line, None, None, None]
    for d in (1, 3):
        chunks[d] = turn(line, d, False)
    halves = []
    for d in (1, 3):
        part = half(chunks[d], 256 * (d // 2))
        halves.append(turn(part, d, False))
    chunks[2] = joined(halves)
    t0 = [own_texts] + everyone(texts, along_x)[1:]
    t0 = joined(t0)
    t1 = other_core(t0)
    parts = [None] * 4
    for k in (0, 1, 3, 2):
        parts[k] = logits_of(k, s2, chunks[k], t0, t1)
    cols = call(col_kernel, out((24, 128)), *[p[0] for p in parts], *[p[1] for p in parts])
    rows = call(
        row_kernel, jax.ShapeDtypeStruct((640, 128), F32), *[p[0] for p in parts], scratch=[pltpu.VMEM((40, 128), F32)]
    )
    cols = everyone(cols, along_x)
    rows = lax.all_to_all(rows.reshape(16, 40, 128), ("y", "z"), 0, 0, tiled=True).reshape(640, 128)
    cols = call(middle_kernel, out((24, 128)), *cols)
    cols = [cols, other_core(cols)]
    row_lse, col_lse, codes, unit, back = call(
        end_kernel,
        (out((16, 128)), out((1, 1024)), out((2, 512)), out((2, 128)), out((2, 512))),
        s2, rows, *cols,
        smem=(0,),
        scratch=[pltpu.VMEM((16, 128), F32)],
    )
    ws, gs, sent = {}, {}, {}
    for k in (2, 1, 3, 0):
        ws[k], gs[k] = call(
            functools.partial(image_kernel, k),
            (out((512, 1024), BF16), out((544, 512))),
            s2, chunks[k], row_lse, col_lse, unit, codes, t0, t1,
            smem=(0,),
            scratch=[pltpu.VMEM((512, 1024), F32)],
        )
        if k:
            sent[k] = turn(gs[k].astype(F16), 4 - k, False)
    g0, g1 = [
        call(
            functools.partial(text_kernel, h),
            out((544, 512)),
            *[ws[k] for k in range(4)], *chunks, unit, codes,
        )
        for h in range(2)
    ]
    swap = other_core(g1.astype(F16))
    moved = []
    for k in (2, 1, 3):
        moved.append(along_x((group(g0, k) + group(swap, k).astype(F32)).astype(F16), 4 - k))
    gt = group(g0, 0) + sum(m.astype(F32) for m in [group(swap, 0)] + moved)
    sums = [group(gs[0], k) + sum(group(m, k).astype(F32) for m in sent.values()) for k in range(4)]
    moved = []
    for k in (2, 1, 3):
        moved.append(turn(sums[k].astype(F16), 4 - k, True))
    gi = sums[0] + sum(m.astype(F32) for m in moved)
    grad_texts, gt_tail = call(
        texts_end_kernel,
        (jax.ShapeDtypeStruct((ROWS, 512), BF16), out((8, 512))),
        gt, back,
    )
    grad_images, loss, grad_scale = call(
        images_end_kernel,
        (jax.ShapeDtypeStruct((ROWS, 512), BF16),) + (jax.ShapeDtypeStruct((1, 1), F32),) * 2,
        gi, gt_tail, back,
    )
    return grad_images, grad_texts, jnp.reshape(loss, ()), jnp.reshape(grad_scale, ())


def solution(mesh):
    split = Mesh(mesh.devices.reshape(4, 4, 2, mesh.shape["group"]), ALL)
    placed = (P(ALL, None), P(ALL, None), P())
    return jax.shard_map(
        program,
        mesh=split,
        in_specs=placed,
        out_specs=(P(ALL, None), P(ALL, None), P(), P()),
        check_vma=False,
    )
```

```python
import functools

import jax
import jax.numpy as jnp
from jax import lax
from jax.experimental import pallas as pl
from jax.experimental.pallas import tpu as pltpu
from jax.sharding import Mesh
from jax.sharding import PartitionSpec as P


ALL = ("x", "y", "c", "z")
F32, BF16, F16 = jnp.float32, jnp.bfloat16, jnp.float16
LOG2E = 1.4426950408889634
LN2 = 0.6931471805599453
OFFSETS = (1, 3, 2)
ROWS = 128
DOWN = 2.0**-11
STEP = 2.0**8
TINY = 6.2e-5


def turn(value, shift, first):
    pairs = []
    for y in range(4):
        for c in range(2):
            for z in range(4):
                if (c == 0) == first:
                    to = ((y + shift) % 4, c, z)
                else:
                    to = (y, c, (z + shift) % 4)
                pairs.append(((y * 2 + c) * 4 + z, (to[0] * 2 + to[1]) * 4 + to[2]))
    return lax.ppermute(value, ("y", "c", "z"), pairs)


def along_x(value, shift):
    return lax.ppermute(value, "x", [(i, (i + shift) % 4) for i in range(4)])


def other_core(value):
    return lax.ppermute(value, "c", [(0, 1), (1, 0)])


def everyone(value, move):
    got = {0: value}
    for d in OFFSETS:
        got[d] = move(value, d)
    return [got[d] for d in range(4)]


NT = (((1,), (1,)), ((), ()))
TN = (((0,), (0,)), ((), ()))


def call(kernel, outs, *args, smem=(), scratch=()):
    return pl.pallas_call(
        kernel,
        out_shape=outs,
        in_specs=[
            pl.BlockSpec(memory_space=pltpu.SMEM if i in smem else pltpu.VMEM) for i in range(len(args))
        ],
        out_specs=jax.tree.map(lambda _: pl.BlockSpec(memory_space=pltpu.VMEM), outs),
        scratch_shapes=scratch,
        compiler_params=pltpu.CompilerParams(vmem_limit_bytes=16 << 20),
    )(*args)


def out(shape, dtype=F32):
    return pltpu.VMEM(shape, dtype)


def hold_kernel(a_ref, b_ref, a_out, b_out, sems):
    copies = [
        pltpu.make_async_copy(ref, o_ref, sems.at[k])
        for k, (ref, o_ref) in enumerate(((a_ref, a_out), (b_ref, b_out)))
    ]
    for copy in copies:
        copy.start()
    for copy in copies:
        copy.wait()


def held(a, b):
    return pl.pallas_call(
        hold_kernel,
        out_shape=(out(a.shape, BF16), out(b.shape, BF16)),
        in_specs=[pl.BlockSpec(memory_space=pl.ANY)] * 2,
        out_specs=(pl.BlockSpec(memory_space=pltpu.VMEM),) * 2,
        scratch_shapes=[pltpu.SemaphoreType.DMA((2,))],
        name="hold",
    )(a, b)


def join_kernel(*refs):
    o_ref, at = refs[-1], 0
    for a in refs[:-1]:
        o_ref[at : at + a.shape[0], :] = a[...]
        at += a.shape[0]


def half_kernel(at, a_ref, o_ref):
    o_ref[...] = a_ref[at : at + 256, :]


def half(value, at):
    return call(functools.partial(half_kernel, at), out((256, 512), BF16), value)


def joined(values):
    return call(join_kernel, out((512, 512), BF16), *values)


def places():
    y, z, on_y = lax.axis_index("y"), lax.axis_index("z"), lax.axis_index("c") == 0
    return jnp.where(on_y, y, z), jnp.where(on_y, z, y), lax.axis_index("x")


def peak(ref):
    tall = jnp.max(jnp.abs(ref[...].astype(F32)), axis=0, keepdims=True)
    return jnp.broadcast_to(jnp.max(tall, axis=1, keepdims=True), (1, 128))


def logits_into(l_ref, s2, im_ref, t_refs):
    for h, t_ref in enumerate(t_refs):
        l_ref[:, 512 * h : 512 * (h + 1)] = s2 * lax.dot_general(
            im_ref[...], t_ref[...], NT, preferred_element_type=F32
        )


def logits_kernel(first, s_ref, im_ref, t0_ref, t1_ref, rows_ref, cols_ref, l_ref, top_scr, sum_scr, mean_scr):
    s2, count = s_ref[0, 0], im_ref.shape[0] // 64
    logits_into(l_ref, s2, im_ref, (t0_ref, t1_ref))

    def tops(i, col_tops):
        here = pl.ds(pl.multiple_of(i * 64, 64), 64)
        row_top, new = None, []
        for k in range(8):
            part = l_ref[here, 128 * k : 128 * (k + 1)]
            row_top = part if row_top is None else jnp.maximum(row_top, part)
            new.append(jnp.maximum(col_tops[k], jnp.max(part.reshape(8, 8, 128), axis=0)))
        top_scr[here, :] = row_top
        return tuple(new)

    col_tops = lax.fori_loop(
        0, count, tops, tuple(l_ref[0:8, 128 * k : 128 * (k + 1)] for k in range(8)), unroll=True
    )

    def sums(i, carry):
        here = pl.ds(pl.multiple_of(i * 64, 64), 64)
        row_top = top_scr[here, :]
        row_sum = row_mean = jnp.zeros((64, 128), F32)
        new = []
        for k in range(8):
            part = l_ref[here, 128 * k : 128 * (k + 1)]
            e = jnp.exp2(part - row_top)
            row_sum = row_sum + e
            row_mean = row_mean + e * part
            part = part.reshape(8, 8, 128)
            e = jnp.exp2(part - col_tops[k][None])
            new.append((carry[k][0] + jnp.sum(e, axis=0), carry[k][1] + jnp.sum(e * part, axis=0)))
        sum_scr[here, :] = row_sum
        mean_scr[here, :] = row_mean
        return tuple(new)

    zero = jnp.zeros((8, 128), F32)
    col_sums = lax.fori_loop(0, count, sums, ((zero, zero),) * 8, unroll=True)
    for k in range(8):
        at = slice(128 * k, 128 * (k + 1))
        top = jnp.max(col_tops[k], axis=0, keepdims=True)
        e = jnp.exp2(col_tops[k] - top)
        cols_ref[0:1, at] = top
        cols_ref[1:2, at] = jnp.sum(e * col_sums[k][0], axis=0, keepdims=True)
        cols_ref[2:3, at] = jnp.sum(e * col_sums[k][1], axis=0, keepdims=True)
    for j in range(count // 2):
        at = slice(128 * j, 128 * (j + 1))
        tops_here = top_scr[at, :].T
        top = jnp.max(tops_here, axis=0, keepdims=True)
        e = jnp.exp2(tops_here - top)
        total = jnp.sum(e * sum_scr[at, :].T, axis=0, keepdims=True)
        rows_ref[j : j + 1, :] = top + jnp.log2(total)
        rows_ref[4 + j : 5 + j, :] = jnp.sum(e * mean_scr[at, :].T, axis=0, keepdims=True) / total
    rows_ref[8:9, :] = peak(im_ref)
    if first:
        rows_ref[9:10, :] = jnp.maximum(peak(t0_ref), peak(t1_ref))
        block = l_ref[0:128, 0:128]
        rows_ref[10:11, :] = jnp.sum(jnp.where(eye(), block, 0.0), axis=0, keepdims=True)


def eye():
    shape = (128, 128)
    return lax.broadcasted_iota(jnp.int32, shape, 0) == lax.broadcasted_iota(jnp.int32, shape, 1)


def logits_of(k, s2, im, t0, t1):
    return call(
        functools.partial(logits_kernel, k == 0),
        (out((16, 128)), out((8, 1024))),
        s2, im, t0, t1,
        smem=(0,),
        scratch=[pltpu.VMEM((im.shape[0], width), F32) for width in (1024, 128, 128, 128)],
    )


def merge(parts):
    top = functools.reduce(jnp.maximum, [p[0] for p in parts])
    es = [jnp.exp2(p[0] - top) for p in parts]
    total = sum(es)
    mean = sum(e * p[1] for e, p in zip(es, parts)) / total
    return top + jnp.log2(total), mean


def greatest(values):
    return functools.reduce(jnp.maximum, values)


def row_at(back_second, back_first):
    first, second, _ = places()
    return lax.rem(second - back_second + 4, 4) * 4 + lax.rem(first - back_first + 4, 4)


def row_kernel(r0, r1, r2, r3, r4, all_ref, scr):
    for k, r, start, end in ((0, r0, 0, 4), (1, r1, 0, 4), (2, r2, 0, 2), (2, r3, 2, 4), (3, r4, 0, 4)):
        for j in range(start, end):
            at = row_at(k, j)
            scr[pl.ds(at, 1), :] = r[j - start : j - start + 1, :]
            scr[pl.ds(16 + at, 1), :] = r[4 + j - start : 5 + j - start, :]
    scr[32:33, :] = r0[10:11, :]
    scr[33:34, :] = r0[9:10, :]
    scr[34:40, :] = jnp.zeros((6, 128), F32)
    message = scr[...]
    for k in range(16):
        all_ref[40 * k : 40 * (k + 1), :] = message


def col_kernel(r0, r1, r2, r3, r4, c0, c1, c2, c3, c4, col_ref):
    rs, cs = (r0, r1, r2, r3, r4), (c0, c1, c2, c3, c4)
    top = greatest([c[0:1, :] for c in cs])
    es = [jnp.exp2(c[0:1, :] - top) for c in cs]
    total = sum(e * c[1:2, :] for e, c in zip(es, cs))
    mean = sum(e * c[2:3, :] for e, c in zip(es, cs)) / total
    lse = top + jnp.log2(total)
    for k in range(8):
        col_ref[k : k + 1, :] = lse[:, 128 * k : 128 * (k + 1)]
        col_ref[8 + k : 9 + k, :] = mean[:, 128 * k : 128 * (k + 1)]
    col_ref[16:17, :] = greatest([r[8:9, :] for r in rs])
    col_ref[17:24, :] = jnp.zeros((7, 128), F32)


def rolled(v, d, group):
    if d == 0:
        return v
    n = v.shape[0]
    size = n // group
    quarter = size // 4
    pieces = []
    for g in range(group):
        at = g * size
        pieces += [v[at + size - d * quarter : at + size, :], v[at : at + size - d * quarter, :]]
    return jnp.concatenate(pieces, axis=0)


def middle_kernel(b0, b1, b2, b3, col_ref):
    cs = (b0, b1, b2, b3)
    lse, mean = merge([(rolled(c[0:8, :], d, 2), rolled(c[8:16, :], d, 2)) for d, c in enumerate(cs)])
    col_ref[0:8, :] = lse
    col_ref[8:16, :] = mean
    col_ref[16:24, :] = greatest([c[16:24, :] for c in cs])


def pieces_of(value):
    left, pieces = value * DOWN, []
    for _ in range(4):
        head = left.astype(BF16).astype(F32)
        head = jnp.where(jnp.abs(head) < TINY, 0.0, head)
        pieces.append(head)
        left = (left - head) * STEP
    return pieces


def value_of(pieces):
    total = pieces[3]
    for p in (pieces[2], pieces[1], pieces[0]):
        total = p + total * (1.0 / STEP)
    return total * (1.0 / DOWN)


def encoded(first, second):
    lane = lax.broadcasted_iota(jnp.int32, (1, 512), 1) % 256
    value = jnp.where(lane % 64 < 32, first, second)
    row = jnp.zeros((1, 512), F32)
    for p, piece in enumerate(pieces_of(value)):
        row = jnp.where(lane // 64 == p, piece, row)
    return row


def tail(row, at, half):
    shape = (8, 512)
    here = lax.broadcasted_iota(jnp.int32, shape, 0) == at
    if half is not None:
        here = here & (lax.broadcasted_iota(jnp.int32, shape, 1) // 256 == half)
    return jnp.where(here, jnp.broadcast_to(row, shape), 0.0)


def total_of(v):
    return jnp.sum(jnp.sum(v, axis=0, keepdims=True), axis=1, keepdims=True)


def end_kernel(s_ref, a_ref, b0, b1, row_ref, col_ref, codes_ref, unit_ref, back_ref, scr):
    rs = [a_ref[40 * k : 40 * (k + 1), :] for k in range(16)]
    lse, mean = merge([(r[0:16, :], r[16:32, :]) for r in rs])
    scr[...] = lse + 1.0
    for k in range(4):
        for j in range(4):
            row_ref[4 * k + j : 4 * k + j + 1, :] = scr[pl.ds(row_at(k, j), 1), :]
    diagonal = total_of(sum(r[32:33, :] for r in rs)) * LN2
    text_peak = greatest([r[33:34, :] for r in rs])
    codes_ref[1:2, :] = encoded(total_of(lse) * LN2 - 2.0 * diagonal, 0.5 * LN2 * total_of(mean) - diagonal)
    swapped = [jnp.concatenate([b1[k + 4 : k + 8, :], b1[k : k + 4, :]], axis=0) for k in (0, 8)]
    lse, mean = merge([(b0[0:8, :], b0[8:16, :]), swapped])
    for k in range(8):
        col_ref[:, 128 * k : 128 * (k + 1)] = lse[k : k + 1, :] + 1.0
    image_peak = jnp.maximum(b0[16:17, :], b1[16:17, :])
    codes_ref[0:1, :] = encoded(total_of(lse) * LN2, 0.5 * LN2 * total_of(mean))
    scale = s_ref[0, 0] * LN2
    for k, top in enumerate((text_peak, image_peak)):
        unit = 4.0 / jnp.maximum(top, 1e-30)
        unit_ref[k : k + 1, :] = unit
        back = scale / unit
        back_ref[k : k + 1, :] = jnp.concatenate([back] * 4, axis=1)


def image_kernel(which, s_ref, im_ref, row_ref, col_ref, unit_ref, codes_ref, t0_ref, t1_ref, w_ref, g_ref, l_ref):
    logits_into(l_ref, s_ref[0, 0], im_ref, (t0_ref, t1_ref))
    for j in range(4):
        at = slice(128 * j, 128 * (j + 1))
        row = row_ref[4 * which + j : 4 * which + j + 1, :]
        row = jnp.broadcast_to(row, (128, 128)).T
        for k in range(8):
            to = slice(128 * k, 128 * (k + 1))
            part = l_ref[at, to]
            w = jnp.exp2(part - row) + jnp.exp2(part - col_ref[:, to])
            if which == 0 and j == 0 and k == 0:
                w = w - jnp.where(eye(), 1.0, 0.0)
            w_ref[at, to] = w.astype(BF16)
    g = jnp.dot(w_ref[:, 0:512], t0_ref[...], preferred_element_type=F32)
    g = g + jnp.dot(w_ref[:, 512:1024], t1_ref[...], preferred_element_type=F32)
    g = g * unit_ref[0:1, 0:1]
    for k in range(4):
        g_ref[136 * k : 136 * k + 128, :] = g[128 * k : 128 * (k + 1), :]
        g_ref[136 * k + 128 : 136 * (k + 1), :] = tail(codes_ref[0:1, :], 4 * (k % 2) + which, k // 2)


def text_kernel(h, w0, w1, w2, w3, i0, i1, i2, i3, unit_ref, codes_ref, g_ref):
    at = slice(512 * h, 512 * (h + 1))
    g = None
    for w, i in zip((w0, w1, w2, w3), (i0, i1, i2, i3)):
        part = lax.dot_general(w[:, at], i[...], TN, preferred_element_type=F32)
        g = part if g is None else g + part
    g = g * unit_ref[1:2, 0:1]
    for k in range(4):
        g_ref[136 * k : 136 * k + 128, :] = g[128 * k : 128 * (k + 1), :]
        g_ref[136 * k + 128 : 136 * (k + 1), :] = tail(codes_ref[1:2, :], 2 * k + h, 0)


def texts_end_kernel(g_ref, back_ref, o_ref, tail_ref):
    o_ref[...] = (g_ref[0:128, :] * back_ref[1:2, :]).astype(BF16)
    tail_ref[...] = g_ref[128:136, :]


def images_end_kernel(g_ref, t_ref, back_ref, o_ref, loss_ref, grad_ref):
    o_ref[...] = (g_ref[0:128, :] * back_ref[0:1, :]).astype(BF16)
    rows = jnp.sum(g_ref[128:136, :] + t_ref[...], axis=0, keepdims=True)
    rows = rows[:, 0:256] + rows[:, 256:512]
    pair_total = ROWS * 128
    for v, (ref, count) in enumerate(((loss_ref, 2.0 * pair_total), (grad_ref, float(pair_total)))):
        ref[...] = value_of([rows[:, 64 * p + 32 * v : 64 * p + 32 * v + 1] for p in range(4)]) / count


def group(value, k):
    return value[136 * k : 136 * (k + 1)]


def program(images, texts, log_scale):
    s2 = jnp.reshape(jnp.exp(log_scale) * LOG2E, (1, 1))
    own_images, own_texts = held(images, texts)
    line = [own_images] + everyone(own_images, lambda v, d: turn(v, d, True))[1:]
    line = joined(line)
    chunks = [line, None, None, None]
    for d in (1, 3):
        chunks[d] = turn(line, d, False)
    halves = []
    for d in (1, 3):
        part = half(chunks[d], 256 * (d // 2))
        halves.append(turn(part, d, False))
    chunks[2] = joined(halves)
    t0 = [own_texts] + everyone(own_texts, along_x)[1:]
    t0 = joined(t0)
    t1 = other_core(t0)
    parts = []
    for k, im in (("0", chunks[0]), ("1", chunks[1]), ("2a", halves[0]), ("2b", halves[1]), ("3", chunks[3])):
        parts.append(logits_of(0 if k == "0" else 1, s2, im, t0, t1))
    cols = call(col_kernel, out((24, 128)), *[p[0] for p in parts], *[p[1] for p in parts])
    rows = call(
        row_kernel, jax.ShapeDtypeStruct((640, 128), F32), *[p[0] for p in parts], scratch=[pltpu.VMEM((40, 128), F32)]
    )
    cols = everyone(cols, along_x)
    rows = lax.all_to_all(rows.reshape(16, 40, 128), ("y", "z"), 0, 0, tiled=True).reshape(640, 128)
    cols = call(middle_kernel, out((24, 128)), *cols)
    cols = [cols, other_core(cols)]
    row_lse, col_lse, codes, unit, back = call(
        end_kernel,
        (out((16, 128)), out((1, 1024)), out((2, 512)), out((2, 128)), out((2, 512))),
        s2, rows, *cols,
        smem=(0,),
        scratch=[pltpu.VMEM((16, 128), F32)],
    )
    ws, gs, sent = {}, {}, {}
    for k in (2, 1, 3, 0):
        ws[k], gs[k] = call(
            functools.partial(image_kernel, k),
            (out((512, 1024), BF16), out((544, 512))),
            s2, chunks[k], row_lse, col_lse, unit, codes, t0, t1,
            smem=(0,),
            scratch=[pltpu.VMEM((512, 1024), F32)],
        )
        if k:
            sent[k] = turn(gs[k].astype(F16), 4 - k, False)
    g0, g1 = [
        call(
            functools.partial(text_kernel, h),
            out((544, 512)),
            *[ws[k] for k in range(4)], *chunks, unit, codes,
        )
        for h in range(2)
    ]
    swap = other_core(g1.astype(F16))
    moved = []
    for k in (2, 1, 3):
        moved.append(along_x((group(g0, k) + group(swap, k).astype(F32)).astype(F16), 4 - k))
    gt = group(g0, 0) + sum(m.astype(F32) for m in [group(swap, 0)] + moved)
    sums = [group(gs[0], k) + sum(group(m, k).astype(F32) for m in sent.values()) for k in range(4)]
    moved = []
    for k in (2, 1, 3):
        moved.append(turn(sums[k].astype(F16), 4 - k, True))
    gi = sums[0] + sum(m.astype(F32) for m in moved)
    grad_texts, gt_tail = call(
        texts_end_kernel,
        (jax.ShapeDtypeStruct((ROWS, 512), BF16), out((8, 512))),
        gt, back,
    )
    grad_images, loss, grad_scale = call(
        images_end_kernel,
        (jax.ShapeDtypeStruct((ROWS, 512), BF16),) + (jax.ShapeDtypeStruct((1, 1), F32),) * 2,
        gi, gt_tail, back,
    )
    return grad_images, grad_texts, jnp.reshape(loss, ()), jnp.reshape(grad_scale, ())


def solution(mesh):
    split = Mesh(mesh.devices.reshape(4, 4, 2, mesh.shape["group"]), ALL)
    placed = (P(ALL, None), P(ALL, None), P())
    return jax.shard_map(
        program,
        mesh=split,
        in_specs=placed,
        out_specs=(P(ALL, None), P(ALL, None), P(), P()),
        check_vma=False,
    )
```

```python
import functools

import jax
import jax.numpy as jnp
from jax import lax
from jax.experimental import pallas as pl
from jax.experimental.pallas import tpu as pltpu
from jax.sharding import Mesh
from jax.sharding import PartitionSpec as P


ALL = ("x", "y", "c", "z")
F32, BF16, F16 = jnp.float32, jnp.bfloat16, jnp.float16
LOG2E = 1.4426950408889634
LN2 = 0.6931471805599453
OFFSETS = (1, 3, 2)
ROWS = 128
DOWN = 2.0**-11
STEP = 2.0**8
TINY = 6.2e-5


def turn(value, shift, first):
    pairs = []
    for y in range(4):
        for c in range(2):
            for z in range(4):
                if (c == 0) == first:
                    to = ((y + shift) % 4, c, z)
                else:
                    to = (y, c, (z + shift) % 4)
                pairs.append(((y * 2 + c) * 4 + z, (to[0] * 2 + to[1]) * 4 + to[2]))
    return lax.ppermute(value, ("y", "c", "z"), pairs)


def along_x(value, shift):
    return lax.ppermute(value, "x", [(i, (i + shift) % 4) for i in range(4)])


def other_core(value):
    return lax.ppermute(value, "c", [(0, 1), (1, 0)])


def everyone(value, move):
    got = {0: value}
    for d in OFFSETS:
        got[d] = move(value, d)
    return [got[d] for d in range(4)]


NT = (((1,), (1,)), ((), ()))
TN = (((0,), (0,)), ((), ()))


def call(kernel, outs, *args, smem=(), scratch=()):
    return pl.pallas_call(
        kernel,
        out_shape=outs,
        in_specs=[
            pl.BlockSpec(memory_space=pltpu.SMEM if i in smem else pltpu.VMEM) for i in range(len(args))
        ],
        out_specs=jax.tree.map(lambda _: pl.BlockSpec(memory_space=pltpu.VMEM), outs),
        scratch_shapes=scratch,
        compiler_params=pltpu.CompilerParams(vmem_limit_bytes=16 << 20),
    )(*args)


def out(shape, dtype=F32):
    return pltpu.VMEM(shape, dtype)


def hold_kernel(a_ref, b_ref, a_out, b_out, sems):
    copies = [
        pltpu.make_async_copy(ref, o_ref, sems.at[k])
        for k, (ref, o_ref) in enumerate(((a_ref, a_out), (b_ref, b_out)))
    ]
    for copy in copies:
        copy.start()
    for copy in copies:
        copy.wait()


def held(a, b):
    return pl.pallas_call(
        hold_kernel,
        out_shape=(out(a.shape, BF16), out(b.shape, BF16)),
        in_specs=[pl.BlockSpec(memory_space=pl.ANY)] * 2,
        out_specs=(pl.BlockSpec(memory_space=pltpu.VMEM),) * 2,
        scratch_shapes=[pltpu.SemaphoreType.DMA((2,))],
        name="hold",
    )(a, b)


def join_kernel(*refs):
    o_ref, at = refs[-1], 0
    for a in refs[:-1]:
        o_ref[at : at + a.shape[0], :] = a[...]
        at += a.shape[0]


def half_kernel(at, a_ref, o_ref):
    o_ref[...] = a_ref[at : at + 256, :]


def half(value, at):
    return call(functools.partial(half_kernel, at), out((256, 512), BF16), value)


def joined(values):
    return call(join_kernel, out((512, 512), BF16), *values)


def places():
    y, z, on_y = lax.axis_index("y"), lax.axis_index("z"), lax.axis_index("c") == 0
    return jnp.where(on_y, y, z), jnp.where(on_y, z, y), lax.axis_index("x")


def peak(ref):
    tall = jnp.max(jnp.abs(ref[...].astype(F32)), axis=0, keepdims=True)
    return jnp.broadcast_to(jnp.max(tall, axis=1, keepdims=True), (1, 128))


def logits_into(l_ref, s2, im_ref, t_refs):
    for h, t_ref in enumerate(t_refs):
        l_ref[:, 512 * h : 512 * (h + 1)] = s2 * lax.dot_general(
            im_ref[...], t_ref[...], NT, preferred_element_type=F32
        )


def logits_kernel(first, s_ref, im_ref, t0_ref, t1_ref, rows_ref, cols_ref, l_ref, top_scr, sum_scr, mean_scr):
    s2, count = s_ref[0, 0], im_ref.shape[0] // 64
    logits_into(l_ref, s2, im_ref, (t0_ref, t1_ref))

    def tops(i, col_tops):
        here = pl.ds(pl.multiple_of(i * 64, 64), 64)
        row_top, new = None, []
        for k in range(8):
            part = l_ref[here, 128 * k : 128 * (k + 1)]
            row_top = part if row_top is None else jnp.maximum(row_top, part)
            new.append(jnp.maximum(col_tops[k], jnp.max(part.reshape(8, 8, 128), axis=0)))
        top_scr[here, :] = row_top
        return tuple(new)

    col_tops = lax.fori_loop(
        0, count, tops, tuple(l_ref[0:8, 128 * k : 128 * (k + 1)] for k in range(8)), unroll=True
    )

    def sums(i, carry):
        here = pl.ds(pl.multiple_of(i * 64, 64), 64)
        row_top = top_scr[here, :]
        row_sum = row_mean = jnp.zeros((64, 128), F32)
        new = []
        for k in range(8):
            part = l_ref[here, 128 * k : 128 * (k + 1)]
            e = jnp.exp2(part - row_top)
            row_sum = row_sum + e
            row_mean = row_mean + e * part
            part = part.reshape(8, 8, 128)
            e = jnp.exp2(part - col_tops[k][None])
            new.append((carry[k][0] + jnp.sum(e, axis=0), carry[k][1] + jnp.sum(e * part, axis=0)))
        sum_scr[here, :] = row_sum
        mean_scr[here, :] = row_mean
        return tuple(new)

    zero = jnp.zeros((8, 128), F32)
    col_sums = lax.fori_loop(0, count, sums, ((zero, zero),) * 8, unroll=True)
    for k in range(8):
        at = slice(128 * k, 128 * (k + 1))
        top = jnp.max(col_tops[k], axis=0, keepdims=True)
        e = jnp.exp2(col_tops[k] - top)
        cols_ref[0:1, at] = top
        cols_ref[1:2, at] = jnp.sum(e * col_sums[k][0], axis=0, keepdims=True)
        cols_ref[2:3, at] = jnp.sum(e * col_sums[k][1], axis=0, keepdims=True)
    for j in range(count // 2):
        at = slice(128 * j, 128 * (j + 1))
        tops_here = top_scr[at, :].T
        top = jnp.max(tops_here, axis=0, keepdims=True)
        e = jnp.exp2(tops_here - top)
        total = jnp.sum(e * sum_scr[at, :].T, axis=0, keepdims=True)
        rows_ref[j : j + 1, :] = top + jnp.log2(total)
        rows_ref[4 + j : 5 + j, :] = jnp.sum(e * mean_scr[at, :].T, axis=0, keepdims=True) / total
    rows_ref[8:9, :] = peak(im_ref)
    if first:
        rows_ref[9:10, :] = jnp.maximum(peak(t0_ref), peak(t1_ref))
        block = l_ref[0:128, 0:128]
        rows_ref[10:11, :] = jnp.sum(jnp.where(eye(), block, 0.0), axis=0, keepdims=True)


def eye():
    shape = (128, 128)
    return lax.broadcasted_iota(jnp.int32, shape, 0) == lax.broadcasted_iota(jnp.int32, shape, 1)


def logits_of(k, s2, im, t0, t1):
    return call(
        functools.partial(logits_kernel, k == 0),
        (out((16, 128)), out((8, 1024))),
        s2, im, t0, t1,
        smem=(0,),
        scratch=[pltpu.VMEM((im.shape[0], width), F32) for width in (1024, 128, 128, 128)],
    )


def merge(parts):
    top = functools.reduce(jnp.maximum, [p[0] for p in parts])
    es = [jnp.exp2(p[0] - top) for p in parts]
    total = sum(es)
    mean = sum(e * p[1] for e, p in zip(es, parts)) / total
    return top + jnp.log2(total), mean


def greatest(values):
    return functools.reduce(jnp.maximum, values)


def row_at(back_second, back_first):
    first, second, _ = places()
    return lax.rem(second - back_second + 4, 4) * 4 + lax.rem(first - back_first + 4, 4)


def row_kernel(r0, r1, r2, r3, r4, all_ref, scr):
    for k, r, start, end in ((0, r0, 0, 4), (1, r1, 0, 4), (2, r2, 0, 2), (2, r3, 2, 4), (3, r4, 0, 4)):
        for j in range(start, end):
            at = row_at(k, j)
            scr[pl.ds(at, 1), :] = r[j - start : j - start + 1, :]
            scr[pl.ds(16 + at, 1), :] = r[4 + j - start : 5 + j - start, :]
    scr[32:33, :] = r0[10:11, :]
    scr[33:34, :] = r0[9:10, :]
    scr[34:40, :] = jnp.zeros((6, 128), F32)
    message = scr[...]
    for k in range(16):
        all_ref[40 * k : 40 * (k + 1), :] = message


def col_kernel(r0, r1, r2, r3, r4, c0, c1, c2, c3, c4, col_ref):
    rs, cs = (r0, r1, r2, r3, r4), (c0, c1, c2, c3, c4)
    top = greatest([c[0:1, :] for c in cs])
    es = [jnp.exp2(c[0:1, :] - top) for c in cs]
    total = sum(e * c[1:2, :] for e, c in zip(es, cs))
    mean = sum(e * c[2:3, :] for e, c in zip(es, cs)) / total
    lse = top + jnp.log2(total)
    for k in range(8):
        col_ref[k : k + 1, :] = lse[:, 128 * k : 128 * (k + 1)]
        col_ref[8 + k : 9 + k, :] = mean[:, 128 * k : 128 * (k + 1)]
    col_ref[16:17, :] = greatest([r[8:9, :] for r in rs])
    col_ref[17:24, :] = jnp.zeros((7, 128), F32)


def rolled(v, d, group):
    if d == 0:
        return v
    n = v.shape[0]
    size = n // group
    quarter = size // 4
    pieces = []
    for g in range(group):
        at = g * size
        pieces += [v[at + size - d * quarter : at + size, :], v[at : at + size - d * quarter, :]]
    return jnp.concatenate(pieces, axis=0)


def middle_kernel(b0, b1, col_ref):
    swapped = [jnp.concatenate([b1[k + 4 : k + 8, :], b1[k : k + 4, :]], axis=0) for k in (0, 8)]
    lse, mean = merge([(b0[0:8, :], b0[8:16, :]), swapped])
    col_ref[0:8, :] = lse
    col_ref[8:16, :] = mean
    col_ref[16:24, :] = jnp.maximum(b0[16:24, :], b1[16:24, :])


def pieces_of(value):
    left, pieces = value * DOWN, []
    for _ in range(4):
        head = left.astype(BF16).astype(F32)
        head = jnp.where(jnp.abs(head) < TINY, 0.0, head)
        pieces.append(head)
        left = (left - head) * STEP
    return pieces


def value_of(pieces):
    total = pieces[3]
    for p in (pieces[2], pieces[1], pieces[0]):
        total = p + total * (1.0 / STEP)
    return total * (1.0 / DOWN)


def encoded(first, second):
    lane = lax.broadcasted_iota(jnp.int32, (1, 512), 1) % 256
    value = jnp.where(lane % 64 < 32, first, second)
    row = jnp.zeros((1, 512), F32)
    for p, piece in enumerate(pieces_of(value)):
        row = jnp.where(lane // 64 == p, piece, row)
    return row


def tail(row, at, half):
    shape = (8, 512)
    here = lax.broadcasted_iota(jnp.int32, shape, 0) == at
    if half is not None:
        here = here & (lax.broadcasted_iota(jnp.int32, shape, 1) // 256 == half)
    return jnp.where(here, jnp.broadcast_to(row, shape), 0.0)


def total_of(v):
    return jnp.sum(jnp.sum(v, axis=0, keepdims=True), axis=1, keepdims=True)


def end_kernel(s_ref, a_ref, b0, b1, b2, b3, row_ref, col_ref, codes_ref, unit_ref, back_ref, scr):
    rs = [a_ref[40 * k : 40 * (k + 1), :] for k in range(16)]
    lse, mean = merge([(r[0:16, :], r[16:32, :]) for r in rs])
    scr[...] = lse + 1.0
    for k in range(4):
        for j in range(4):
            row_ref[4 * k + j : 4 * k + j + 1, :] = scr[pl.ds(row_at(k, j), 1), :]
    diagonal = total_of(sum(r[32:33, :] for r in rs)) * LN2
    text_peak = greatest([r[33:34, :] for r in rs])
    codes_ref[1:2, :] = encoded(total_of(lse) * LN2 - 2.0 * diagonal, 0.5 * LN2 * total_of(mean) - diagonal)
    cs = (b0, b1, b2, b3)
    lse, mean = merge([(rolled(c[0:8, :], d, 2), rolled(c[8:16, :], d, 2)) for d, c in enumerate(cs)])
    for k in range(8):
        col_ref[:, 128 * k : 128 * (k + 1)] = lse[k : k + 1, :] + 1.0
    image_peak = greatest([c[16:17, :] for c in cs])
    codes_ref[0:1, :] = encoded(total_of(lse) * LN2, 0.5 * LN2 * total_of(mean))
    scale = s_ref[0, 0] * LN2
    for k, top in enumerate((text_peak, image_peak)):
        unit = 4.0 / jnp.maximum(top, 1e-30)
        unit_ref[k : k + 1, :] = unit
        back = scale / unit
        back_ref[k : k + 1, :] = jnp.concatenate([back] * 4, axis=1)


def image_kernel(which, s_ref, im_ref, row_ref, col_ref, unit_ref, codes_ref, t0_ref, t1_ref, w_ref, g_ref, l_ref):
    logits_into(l_ref, s_ref[0, 0], im_ref, (t0_ref, t1_ref))
    for j in range(4):
        at = slice(128 * j, 128 * (j + 1))
        row = row_ref[4 * which + j : 4 * which + j + 1, :]
        row = jnp.broadcast_to(row, (128, 128)).T
        for k in range(8):
            to = slice(128 * k, 128 * (k + 1))
            part = l_ref[at, to]
            w = jnp.exp2(part - row) + jnp.exp2(part - col_ref[:, to])
            if which == 0 and j == 0 and k == 0:
                w = w - jnp.where(eye(), 1.0, 0.0)
            w_ref[at, to] = w.astype(BF16)
    g = jnp.dot(w_ref[:, 0:512], t0_ref[...], preferred_element_type=F32)
    g = g + jnp.dot(w_ref[:, 512:1024], t1_ref[...], preferred_element_type=F32)
    g = g * unit_ref[0:1, 0:1]
    for k in range(4):
        g_ref[136 * k : 136 * k + 128, :] = g[128 * k : 128 * (k + 1), :]
        g_ref[136 * k + 128 : 136 * (k + 1), :] = tail(codes_ref[0:1, :], 4 * (k % 2) + which, k // 2)


def text_kernel(h, w0, w1, w2, w3, i0, i1, i2, i3, unit_ref, codes_ref, g_ref):
    at = slice(512 * h, 512 * (h + 1))
    g = None
    for w, i in zip((w0, w1, w2, w3), (i0, i1, i2, i3)):
        part = lax.dot_general(w[:, at], i[...], TN, preferred_element_type=F32)
        g = part if g is None else g + part
    g = g * unit_ref[1:2, 0:1]
    for k in range(4):
        g_ref[136 * k : 136 * k + 128, :] = g[128 * k : 128 * (k + 1), :]
        g_ref[136 * k + 128 : 136 * (k + 1), :] = tail(codes_ref[1:2, :], 2 * k + h, 0)


def texts_end_kernel(g_ref, back_ref, o_ref, tail_ref):
    o_ref[...] = (g_ref[0:128, :] * back_ref[1:2, :]).astype(BF16)
    tail_ref[...] = g_ref[128:136, :]


def images_end_kernel(g_ref, t_ref, back_ref, o_ref, loss_ref, grad_ref):
    o_ref[...] = (g_ref[0:128, :] * back_ref[0:1, :]).astype(BF16)
    rows = jnp.sum(g_ref[128:136, :] + t_ref[...], axis=0, keepdims=True)
    rows = rows[:, 0:256] + rows[:, 256:512]
    pair_total = ROWS * 128
    for v, (ref, count) in enumerate(((loss_ref, 2.0 * pair_total), (grad_ref, float(pair_total)))):
        ref[...] = value_of([rows[:, 64 * p + 32 * v : 64 * p + 32 * v + 1] for p in range(4)]) / count


def group(value, k):
    return value[136 * k : 136 * (k + 1)]


def program(images, texts, log_scale):
    s2 = jnp.reshape(jnp.exp(log_scale) * LOG2E, (1, 1))
    own_images, own_texts = held(images, texts)
    line = [own_images] + everyone(images, lambda v, d: turn(v, d, True))[1:]
    line = joined(line)
    chunks = [line, None, None, None]
    for d in (1, 3):
        chunks[d] = turn(line, d, False)
    halves = []
    for d in (1, 3):
        part = half(chunks[d], 256 * (d // 2))
        halves.append(turn(part, d, False))
    chunks[2] = joined(halves)
    t0 = [own_texts] + everyone(texts, along_x)[1:]
    t0 = joined(t0)
    t1 = other_core(t0)
    parts = []
    for k, im in (("0", chunks[0]), ("1", chunks[1]), ("2a", halves[0]), ("2b", halves[1]), ("3", chunks[3])):
        parts.append(logits_of(0 if k == "0" else 1, s2, im, t0, t1))
    cols = call(col_kernel, out((24, 128)), *[p[0] for p in parts], *[p[1] for p in parts])
    other = other_core(cols)
    rows = call(
        row_kernel, jax.ShapeDtypeStruct((640, 128), F32), *[p[0] for p in parts], scratch=[pltpu.VMEM((40, 128), F32)]
    )
    cols = call(middle_kernel, out((24, 128)), cols, other)
    rows = lax.all_to_all(rows.reshape(16, 40, 128), ("y", "z"), 0, 0, tiled=True).reshape(640, 128)
    cols = everyone(cols, along_x)
    row_lse, col_lse, codes, unit, back = call(
        end_kernel,
        (out((16, 128)), out((1, 1024)), out((2, 512)), out((2, 128)), out((2, 512))),
        s2, rows, *cols,
        smem=(0,),
        scratch=[pltpu.VMEM((16, 128), F32)],
    )
    ws, gs, sent = {}, {}, {}
    for k in (2, 1, 3, 0):
        ws[k], gs[k] = call(
            functools.partial(image_kernel, k),
            (out((512, 1024), BF16), out((544, 512))),
            s2, chunks[k], row_lse, col_lse, unit, codes, t0, t1,
            smem=(0,),
            scratch=[pltpu.VMEM((512, 1024), F32)],
        )
        if k:
            sent[k] = turn(gs[k].astype(F16), 4 - k, False)
    g0, g1 = [
        call(
            functools.partial(text_kernel, h),
            out((544, 512)),
            *[ws[k] for k in range(4)], *chunks, unit, codes,
        )
        for h in range(2)
    ]
    swap = other_core(g1.astype(F16))
    moved = []
    for k in (2, 1, 3):
        moved.append(along_x((group(g0, k) + group(swap, k).astype(F32)).astype(F16), 4 - k))
    gt = group(g0, 0) + sum(m.astype(F32) for m in [group(swap, 0)] + moved)
    sums = [group(gs[0], k) + sum(group(m, k).astype(F32) for m in sent.values()) for k in range(4)]
    moved = []
    for k in (2, 1, 3):
        moved.append(turn(sums[k].astype(F16), 4 - k, True))
    gi = sums[0] + sum(m.astype(F32) for m in moved)
    grad_texts, gt_tail = call(
        texts_end_kernel,
        (jax.ShapeDtypeStruct((ROWS, 512), BF16), out((8, 512))),
        gt, back,
    )
    grad_images, loss, grad_scale = call(
        images_end_kernel,
        (jax.ShapeDtypeStruct((ROWS, 512), BF16),) + (jax.ShapeDtypeStruct((1, 1), F32),) * 2,
        gi, gt_tail, back,
    )
    return grad_images, grad_texts, jnp.reshape(loss, ()), jnp.reshape(grad_scale, ())


def solution(mesh):
    split = Mesh(mesh.devices.reshape(4, 4, 2, mesh.shape["group"]), ALL)
    placed = (P(ALL, None), P(ALL, None), P())
    return jax.shard_map(
        program,
        mesh=split,
        in_specs=placed,
        out_specs=(P(ALL, None), P(ALL, None), P(), P()),
        check_vma=False,
    )
```
